32 devices in a mesh: fsdp: 2 (over x), ctx: 4 (over z), tp: 4 (over y, core).
Axes of the slice: x: 2, y: 2, z: 4, core: 2. Of those that a mesh axis runs over, the one named last changes fastest.
Arguments:
- tokens: bfloat16 [4, 2048, 1024], P('fsdp', 'ctx'), may hold values from -6 to 6
- segment_ids: int32 [4, 2048], P('fsdp'), may hold values from 0 to 15, never falling along the last dimension, each value on 1 to 1024 neighbouring positions
- attn_gain: bfloat16 [1024], P('fsdp'), may hold values from 0.25 to 1.75
- w_query: bfloat16 [1024, 2048], P('fsdp', 'tp'), may hold values from -0.1875 to 0.1875
- w_key: bfloat16 [1024, 1024], P('fsdp', 'tp'), may hold values from -0.1875 to 0.1875
- w_value: bfloat16 [1024, 1024], P('fsdp', 'tp'), may hold values from -0.1875 to 0.1875
- query_gain: bfloat16 [128], P('fsdp'), may hold values from 0.099609375 to 1.8984375
- key_gain: bfloat16 [128], P('fsdp'), may hold values from 0.099609375 to 1.8984375
- w_out: bfloat16 [2048, 1024], P('tp', 'fsdp'), may hold values from -0.375 to 0.375
- ffn_gain: bfloat16 [1024], P('fsdp'), may hold values from 0.25 to 1.75
- w_gate: bfloat16 [1024, 3072], P('fsdp', 'tp'), may hold values from -0.1875 to 0.1875
- w_up: bfloat16 [1024, 3072], P('fsdp', 'tp'), may hold values from -0.1875 to 0.1875
- w_down: bfloat16 [3072, 1024], P('tp', 'fsdp'), may hold values from -0.21875 to 0.21875
- out_grad: bfloat16 [4, 2048, 1024], P('fsdp', 'ctx'), may hold values from -6 to 6
Outputs:
- layer_out: bfloat16 [4, 2048, 1024], P('fsdp', 'ctx')
- input_grad: float32 [4, 2048, 1024], P('fsdp', 'ctx')
- attn_gain_grad: float32 [1024], P('fsdp')
- w_query_grad: float32 [1024, 2048], P('fsdp', 'tp')
- w_key_grad: float32 [1024, 1024], P('fsdp', 'tp')
- w_value_grad: float32 [1024, 1024], P('fsdp', 'tp')
- query_gain_grad: float32 [128], P('fsdp')
- key_gain_grad: float32 [128], P('fsdp')
- w_out_grad: float32 [2048, 1024], P('tp', 'fsdp')
- ffn_gain_grad: float32 [1024], P('fsdp')
- w_gate_grad: float32 [1024, 3072], P('fsdp', 'tp')
- w_up_grad: float32 [1024, 3072], P('fsdp', 'tp')
- w_down_grad: float32 [3072, 1024], P('tp', 'fsdp')
The draws below stay inside these ranges and needn't reach their ends.
Inputs may be any that keep to these rules, and one draw needn't show every extreme that they name: `segment_ids`: ids never fall along a sequence, every id of 0 to 15 occurs in each sequence (so the padding segment 0 comes first), a segment has 1 to 1024 positions and some segment exactly 1024.
All inputs are finite; a program needn't handle non-finite values.
Results may differ from the reference program's by a relative error of at most 0.025.
Values may be sent and summed in bfloat16 or wider, within the bound.
No kernel may reach another device: no remote copies, remote signals or barrier semaphores. Data moves between devices by JAX's collectives and lax.ppermute only.
A program may use at most 192 MiB of HBM per device.

```python
import math
import jax
import jax.numpy as jnp
import numpy as np
from jax import lax

D = 1024
H = 16
KV = 8
HD = 128
FF = 3072
L = 2048
SEGS = 16
DOC_MOST = 1024
SEQS = 4


def block_scale(own_key, dims, cuts, low, high):
    loudness, own = 1.0, jax.random.fold_in(own_key, 6)
    for dim, parts in cuts:
        heights = jnp.exp(jax.random.uniform(jax.random.fold_in(own, dim), (parts,), jnp.float32, low / len(cuts), high / len(cuts)))
        loudness = loudness * jnp.repeat(heights, dims[dim] // parts).reshape([-1 if axis == dim else 1 for axis in range(len(dims))])
    return loudness


def profile(number_of, total, bound, slope):
    loads = [(1 << 20) // math.isqrt(standing ** slope) + 1 for standing in range(2, number_of + 1)]
    rest, holding = total - bound - (number_of - 1), [1] * (number_of - 1)
    while rest > 0:
        candidates = [i for i in range(number_of - 1) if holding[i] < bound]
        pool, left = sum([loads[i] for i in candidates]), rest
        for i in candidates:
            more = min(bound - holding[i], max(1, left * loads[i] // pool), rest)
            holding[i] = holding[i] + more
            rest = rest - more
    return np.array([bound] + holding)


def ragged_sizes(key, number_of, total, limit, slope):
    if number_of == 2:
        one = jax.random.randint(key, (), max(1, total - limit), min(limit, total - 1) + 1)
        return jnp.stack([one, total - one])
    sizes = jnp.asarray(profile(number_of, total, limit, slope), jnp.int32)
    couples = (number_of - 1) // 2
    giver, receiver = sizes[1:1 + 2 * couples:2], sizes[2:2 + 2 * couples:2]
    slack = jnp.minimum(giver - 1, limit - receiver)
    shifted = jax.random.randint(jax.random.fold_in(key, 1), (couples,), 0, 1 << 20) % (slack + 1)
    sizes = sizes.at[1:1 + 2 * couples:2].set(giver - shifted).at[2:2 + 2 * couples:2].set(receiver + shifted)
    return sizes[jax.random.permutation(jax.random.fold_in(key, 2), number_of)]


def noise(stream_key, extent, spread, limit, cuts=(), kind=jnp.bfloat16):
    factor_of = block_scale(stream_key, extent, cuts, -0.22, 0.18) if cuts else 1.0
    array = jax.random.normal(stream_key, extent, jnp.float32) * spread * factor_of
    return jnp.minimum(jnp.maximum(array, -limit), limit).astype(kind)


def setup_inputs(seed: int = 0) -> dict:
    splits = jax.random.split(jax.random.key(seed), 15)
    tokens = noise(splits[0], (SEQS, L, D), 1.0, 6.0, ((0, 2), (1, 4)))
    segment_ids = jax.vmap(lambda own: jnp.searchsorted(jnp.cumsum(ragged_sizes(own, SEGS, L, DOC_MOST, 2)), jnp.arange(L), side="right"))(jax.random.split(splits[1], SEQS)).reshape((SEQS, L)).astype(jnp.int32)
    attn_gain = jnp.clip(1.0 + 0.15 * jax.random.normal(splits[2], (D,), jnp.float32), 0.25, 1.75).astype(jnp.bfloat16)
    w_query = noise(splits[3], (D, H * HD), D ** -0.5, 0.1875, ((0, 2), (1, 4)))
    w_key = noise(splits[4], (D, KV * HD), D ** -0.5, 0.1875, ((0, 2), (1, 4)))
    w_value = noise(splits[5], (D, KV * HD), D ** -0.5, 0.1875, ((0, 2), (1, 4)))
    query_gain = jnp.clip(1.0 + 0.18 * jax.random.normal(splits[6], (HD,), jnp.float32), 0.099609375, 1.8984375).astype(jnp.bfloat16)
    key_gain = jnp.clip(1.0 + 0.18 * jax.random.normal(splits[7], (HD,), jnp.float32), 0.099609375, 1.8984375).astype(jnp.bfloat16)
    w_out = noise(splits[8], (H * HD, D), (H * HD // 8) ** -0.5, 0.375, ((0, 4), (1, 2)))
    ffn_gain = jnp.clip(1.0 + 0.15 * jax.random.normal(splits[9], (D,), jnp.float32), 0.25, 1.75).astype(jnp.bfloat16)
    w_gate = noise(splits[10], (D, FF), D ** -0.5, 0.1875, ((0, 2), (1, 4)))
    w_up = noise(splits[11], (D, FF), D ** -0.5, 0.1875, ((0, 2), (1, 4)))
    w_down = noise(splits[12], (FF, D), (FF // 4) ** -0.5, 0.21875, ((0, 4), (1, 2)))
    out_grad = noise(splits[13], (SEQS, L, D), 1.0, 6.0, ((0, 2), (1, 4)))
    return {"tokens": tokens, "segment_ids": segment_ids, "attn_gain": attn_gain, "w_query": w_query, "w_key": w_key, "w_value": w_value, "query_gain": query_gain, "key_gain": key_gain, "w_out": w_out, "ffn_gain": ffn_gain, "w_gate": w_gate, "w_up": w_up, "w_down": w_down, "out_grad": out_grad}


epsilon = 1e-06
rope_base = 1000000.0
masked_score = -1e+30

@jax.custom_vjp
def low(v):
    return lax.optimization_barrier(v.astype(jnp.bfloat16)).astype(jnp.float32)

@jax.custom_vjp
def low_back(v):
    return v

def low_keep(v):
    return (low(v), None)

def low_pass(kept, grad):
    return (grad,)

def back_keep(v):
    return (v, None)

def back_low(kept, grad):
    return (low(grad),)
low.defvjp(low_keep, low_pass)
low_back.defvjp(back_keep, back_low)

def positions(segment_row):
    index_row = jnp.arange(segment_row.shape[0], dtype=jnp.int32)
    previous = jnp.concatenate([segment_row[:1] - 1, segment_row[:-1]])
    starts = jnp.where(segment_row != previous, index_row, 0).astype(jnp.int32)
    return index_row - lax.cummax(starts, axis=0)

def angles(position):
    half_size = HD // 2
    frequency = rope_base ** (-(jnp.arange(half_size, dtype=jnp.float32) * 2.0 / HD))
    turned = position.astype(jnp.float32)[:, None] * frequency[None, :]
    return (jnp.cos(turned), jnp.sin(turned))

def rotate(values, cosine, sine):
    half_size = values.shape[-1] // 2
    first = values[..., :half_size]
    second = values[..., half_size:]
    return jnp.concatenate([first * cosine - second * sine, second * cosine + first * sine], -1)

def norm_rows(values, gain):
    return values * lax.rsqrt(lax.optimization_barrier(jnp.mean(values * values, -1, keepdims=True)) + epsilon) * gain

def big_dot(left, right):
    return jnp.dot(left, right, preferred_element_type=jnp.float32, precision=lax.Precision.HIGHEST)

def seq_forward(params, rows, segment_row):
    attn_gain, w_query, w_key, w_value, query_gain, key_gain, w_out, ffn_gain, w_gate, w_up, w_down = params
    length = rows.shape[0]
    position = positions(segment_row)
    valid = (segment_row != 0).astype(jnp.float32)[:, None]
    cosine, sine = angles(position)
    cosine = cosine[:, None, :]
    sine = sine[:, None, :]
    normed = low(norm_rows(rows, attn_gain))
    query_pre = low_back(big_dot(normed, w_query)).reshape(length, H, HD)
    key_pre = low_back(big_dot(normed, w_key)).reshape(length, KV, HD)
    value_pre = low_back(big_dot(normed, w_value)).reshape(length, KV, HD)
    queries = low(rotate(norm_rows(query_pre, query_gain), cosine, sine))
    keys = low(rotate(norm_rows(key_pre, key_gain), cosine, sine))
    values = low(value_pre)
    group_size = H // KV
    keys_all = jnp.repeat(keys, group_size, axis=1)
    values_all = jnp.repeat(values, group_size, axis=1)
    scores = low_back(jnp.einsum('qhd,khd->hqk', queries, keys_all, precision=lax.Precision.HIGHEST) * HD ** (-0.5))
    index_row = jnp.arange(length, dtype=jnp.int32)
    allowed = (segment_row[:, None] == segment_row[None, :]) & (index_row[None, :] <= index_row[:, None]) & (segment_row[None, :] != 0)
    masked = jnp.where(allowed[None], scores, masked_score)
    top_score = lax.optimization_barrier(jnp.max(masked, -1, keepdims=True))
    weights = jnp.where(allowed[None], jnp.exp(masked - top_score), 0.0)
    total = lax.optimization_barrier(jnp.sum(weights, -1, keepdims=True))
    total_safe = jnp.where(segment_row[None, :, None] != 0, total, 1.0)
    probs = low(weights / total_safe)
    mixed = jnp.einsum('hqk,khd->qhd', probs, values_all, precision=lax.Precision.HIGHEST) * valid[:, :, None]
    mixed = low(low_back(mixed)).reshape(length, H * HD)
    branch = low_back(big_dot(mixed, w_out))
    resid = rows + valid * branch
    normed_two = low(norm_rows(resid, ffn_gain))
    gate = low_back(big_dot(normed_two, w_gate))
    upper = low_back(big_dot(normed_two, w_up))
    active = low(jax.nn.silu(gate) * upper)
    return resid + valid * low_back(big_dot(active, w_down))

def reference(tokens, segment_ids, attn_gain, w_query, w_key, w_value, query_gain, key_gain, w_out, ffn_gain, w_gate, w_up, w_down, out_grad):
    params = (attn_gain.astype(jnp.float32), w_query.astype(jnp.float32), w_key.astype(jnp.float32), w_value.astype(jnp.float32), query_gain.astype(jnp.float32), key_gain.astype(jnp.float32), w_out.astype(jnp.float32), ffn_gain.astype(jnp.float32), w_gate.astype(jnp.float32), w_up.astype(jnp.float32), w_down.astype(jnp.float32))
    checked = jax.checkpoint(seq_forward)

    def forward(weights, inputs):

        def one_sequence(pair):
            return checked(weights, pair[0], pair[1])
        return lax.map(one_sequence, (inputs, segment_ids))
    outputs, pull = jax.vjp(forward, params, tokens.astype(jnp.float32))
    param_grads, input_grad = pull(out_grad.astype(jnp.float32))
    return (outputs.astype(jnp.bfloat16), input_grad, param_grads[0], param_grads[1], param_grads[2], param_grads[3], param_grads[4], param_grads[5], param_grads[6], param_grads[7], param_grads[8], param_grads[9], param_grads[10])
```

```python
import functools
import math

import jax
import jax.numpy as jnp
from jax import lax
from jax.experimental import pallas as pl
from jax.experimental.pallas import tpu as pltpu
from jax.sharding import PartitionSpec as P

epsilon = 1e-06
rope_base = 1000000.0
longest_segment = 1024
f32 = jnp.float32
bf16 = jnp.bfloat16

NN = (((1,), (0,)), ((), ()))
NT = (((1,), (1,)), ((), ()))
TN = (((0,), (0,)), ((), ()))


def dot(left, right, dims=NN):
    return lax.dot_general(left, right, dims, preferred_element_type=f32)


def inv_scale(values):
    return lax.rsqrt(jnp.mean(values * values, -1, keepdims=True) + epsilon)


def norm_back(values, scale, gain, grad):
    scaled = grad * gain
    return scale * scaled - values * (scale * scale * scale) * jnp.mean(
        scaled * values, -1, keepdims=True
    )


def rows_of(index, size):
    return pl.ds(pl.multiple_of(index * size, size), size)


def whole(shape):
    return pl.BlockSpec(shape, lambda *_: (0,) * len(shape))


def columns(parts):
    width = parts[0]
    return [(i * width, (i + 1) * width) for i in range(len(parts))]


def call(kernel, name, grid, ins, outs, scratch, flops, moved, scalars, *args, aliases=None):
    return pl.pallas_call(
        kernel,
        name=name,
        out_shape=[o[0] for o in outs],
        grid_spec=pltpu.PrefetchScalarGridSpec(
            num_scalar_prefetch=1,
            grid=grid,
            in_specs=ins,
            out_specs=[o[1] for o in outs],
            scratch_shapes=scratch,
        ),
        input_output_aliases=aliases or {},
        compiler_params=pltpu.CompilerParams(dimension_semantics=("arbitrary",) * len(grid)),
        cost_estimate=pl.CostEstimate(flops=int(flops), bytes_accessed=int(moved), transcendentals=0),
    )(scalars, *args)


def qkv_kernel(heads, kv_heads, size, np_, ids, tok, gain, cos, sin, qg, kg, *rest):
    weights, (normed, q_out, kv_out, pre_out) = rest[:np_], rest[np_:]
    x = tok[...].astype(f32)
    low = (x * inv_scale(x) * gain[...]).astype(bf16)
    normed[...] = low
    width = low.shape[1] // np_
    acc = dot(low[:, :width], weights[0][...])
    for i in range(1, np_):
        acc = acc + dot(low[:, i * width : (i + 1) * width], weights[i][...])
    total = heads + kv_heads
    pre_out[...] = acc[:, : total * size]
    c, s = cos[...], sin[...]
    for h in range(total):
        u = acc[:, h * size : (h + 1) * size]
        g = qg[...] if h < heads else kg[...]
        u = u * inv_scale(u) * g
        rot = (u * c + pltpu.roll(u, size // 2, 1) * s).astype(bf16)
        if h < heads:
            q_out[:, h * size : (h + 1) * size] = rot
        else:
            kv_out[:, (h - heads) * size : (h - heads + 1) * size] = rot
    kv_out[:, kv_heads * size :] = acc[:, total * size :].astype(bf16)


def allowed_block(key_base, start, row_base, block, rows):
    key_index = key_base + lax.broadcasted_iota(jnp.int32, (block, rows), 0)
    row_index = row_base + lax.broadcasted_iota(jnp.int32, (block, rows), 1)
    return (key_index >= start) & (key_index <= row_index)


def attend_kernel(cfg, ids, q, start, *rest):
    heads, kv_heads, size, np_, back, block, scale2 = cfg
    chunks = rest[: back + 1]
    w_out = rest[back + 1 : back + 1 + np_]
    own, oth, mixed_out, lse_out, kv, acc, total = rest[back + 1 + np_ :]
    t = pl.program_id(0)
    core = ids[1]
    rows = q.shape[0]
    length = chunks[0].shape[0]
    group = heads // kv_heads

    @pl.when(t == 0)
    def _():
        for i in range(back + 1):
            kv[i * length : (i + 1) * length, :] = chunks[i][...]

    acc[...] = jnp.zeros_like(acc)
    total[...] = jnp.zeros_like(total)
    row_base = back * length + t * rows
    start_row = start[...]

    def step(kb, carry):
        at = pl.ds(pl.multiple_of(kb * block, block), block)
        allow = allowed_block(kb * block, start_row, row_base, block, rows)
        for g in range(kv_heads):
            k = kv[at, g * size : (g + 1) * size]
            v = kv[at, (kv_heads + g) * size : (kv_heads + g + 1) * size]
            for h in range(g * group, (g + 1) * group):
                s = dot(k, q[:, h * size : (h + 1) * size], NT)
                e = jnp.where(allow, jnp.exp2(s * scale2), 0.0)
                total[h : h + 1, :] += jnp.sum(e, 0, keepdims=True)
                acc[h * size : (h + 1) * size, :] += dot(v, e.astype(bf16), TN)
        return carry

    lax.fori_loop(ids[2 + t], (row_base + rows) // block, step, 0)
    sums = total[...]
    sums = jnp.where(sums > 0.0, sums, 1.0)
    lse_out[...] = jnp.log2(sums)
    inverse = 1.0 / sums
    for h in range(heads):
        part = (acc[h * size : (h + 1) * size, :] * inverse[h : h + 1, :]).astype(bf16)
        mixed_out[h * size : (h + 1) * size, :] = part
    mixed = mixed_out[...]
    width = w_out[0].shape[1]
    for i in range(np_):
        part = dot(mixed, w_out[i][...], TN).astype(bf16)

        @pl.when(t == core)
        def _():
            own[:, i * width : (i + 1) * width] = part

        @pl.when(t != core)
        def _():
            oth[:, i * width : (i + 1) * width] = part


def ffn_kernel(np_, ids, tok, b_own, b_oth, valid, gain, grad, *rest):
    gate_w, up_w, down_w = rest[:np_], rest[np_ : 2 * np_], rest[2 * np_ : 3 * np_]
    n2_out, act_out, gg_out, gu_out, own, oth, gain_out, hat, acc = rest[3 * np_ :]
    f = pl.program_id(0)
    core = ids[1]
    half = b_own.shape[0]

    @pl.when(f == 0)
    def _():
        for ref, tile in ((b_own, core), (b_oth, 1 - core)):
            at = rows_of(tile, half)
            resid = tok[at, :].astype(f32) + valid[at, :1] * ref[...].astype(f32)
            normal = resid * inv_scale(resid)
            hat[at, :] = normal
            n2_out[at, :] = (normal * gain[...]).astype(bf16)
        acc[...] = jnp.zeros_like(acc)

    width = tok.shape[1] // np_
    parts = [(i * width, (i + 1) * width) for i in range(np_)]
    gate = up = active_grad = None
    for i, (a, b) in enumerate(parts):
        x = n2_out[:, a:b]
        g, u, d = dot(x, gate_w[i][...]), dot(x, up_w[i][...]), dot(grad[:, a:b], down_w[i][...], NT)
        gate, up, active_grad = (g, u, d) if i == 0 else (gate + g, up + u, active_grad + d)
    sigma = jax.nn.sigmoid(gate)
    silu = gate * sigma
    act_out[...] = (silu * up).astype(bf16)
    gg = (active_grad * up * sigma * (1.0 + gate * (1.0 - sigma))).astype(bf16)
    gu = (active_grad * silu).astype(bf16)
    gg_out[...] = gg
    gu_out[...] = gu
    for i, (a, b) in enumerate(parts):
        acc[:, a:b] += dot(gg, gate_w[i][...], NT) + dot(gu, up_w[i][...], NT)

    @pl.when(f == pl.num_programs(0) - 1)
    def _():
        own[...] = acc[rows_of(core, half), :].astype(bf16)
        oth[...] = acc[rows_of(1 - core, half), :].astype(bf16)
        gain_out[...] = jnp.sum(acc[...] * hat[...], 0, keepdims=True)


def picked(ids, own, oth, t):
    return jnp.where(ids[1] == t, own[...].astype(f32), oth[...].astype(f32))


def attend_back_kernel(cfg, ids, tok, b_own, b_oth, t_own, t_oth, valid, gain, grad, mixed, lse, q, start, pre, cos, sin, qg, *rest):
    heads, kv_heads, size, np_, back, block, scale2 = cfg
    chunks = rest[: back + 1]
    w_out = rest[back + 1 : back + 1 + np_]
    outs = rest[back + 1 + np_ :]
    resid_out, branch_out, gq_out, gain_out = outs[:4]
    far = outs[4 : 4 + back + 1]
    kv, dkv, dq, dout = outs[4 + back + 1 :]
    t = pl.program_id(0)
    rows = q.shape[0]
    length = chunks[0].shape[0]
    group = heads // kv_heads
    scale = size**-0.5

    @pl.when(t == 0)
    def _():
        for i in range(back + 1):
            kv[i * length : (i + 1) * length, :] = chunks[i][...]
        dkv[...] = jnp.zeros_like(dkv)
        gain_out[...] = jnp.zeros_like(gain_out)

    resid = tok[...].astype(f32) + valid[:, :1] * picked(ids, b_own, b_oth, t)
    resid_grad = grad[...].astype(f32) + norm_back(
        resid, inv_scale(resid), gain[...], picked(ids, t_own, t_oth, t)
    )
    resid_out[...] = resid_grad
    low = (valid[:, :1] * resid_grad).astype(bf16)
    branch_out[...] = low
    width = low.shape[1] // np_
    mixed_grad = dot(w_out[0][...], low[:, :width], NT)
    for i in range(1, np_):
        mixed_grad = mixed_grad + dot(w_out[i][...], low[:, i * width : (i + 1) * width], NT)
    dout[...] = mixed_grad.astype(bf16)
    delta = [
        jnp.sum(
            dout[h * size : (h + 1) * size, :].astype(f32) * mixed[h * size : (h + 1) * size, :].astype(f32),
            0,
            keepdims=True,
        )
        for h in range(heads)
    ]
    dq[...] = jnp.zeros_like(dq)
    row_base = back * length + t * rows
    start_row = start[...]

    def step(kb, carry):
        at = pl.ds(pl.multiple_of(kb * block, block), block)
        allow = allowed_block(kb * block, start_row, row_base, block, rows)
        for g in range(kv_heads):
            k = kv[at, g * size : (g + 1) * size]
            v = kv[at, (kv_heads + g) * size : (kv_heads + g + 1) * size]
            dk = dv = None
            for h in range(g * group, (g + 1) * group):
                qh = q[:, h * size : (h + 1) * size]
                do = dout[h * size : (h + 1) * size, :]
                s = dot(k, qh, NT)
                p = jnp.where(allow, jnp.exp2(s * scale2 - lse[h : h + 1, :]), 0.0)
                dp = dot(v, do)
                ds = (p * (dp - delta[h])).astype(bf16)
                one_v = dot(p.astype(bf16), do, NT)
                one_k = dot(ds, qh)
                dk, dv = (one_k, one_v) if dk is None else (dk + one_k, dv + one_v)
                dq[h * size : (h + 1) * size, :] += dot(k, ds, TN)
            dkv[at, g * size : (g + 1) * size] += dk * scale
            dkv[at, (kv_heads + g) * size : (kv_heads + g + 1) * size] += dv
        return carry

    lax.fori_loop(ids[2 + t], (row_base + rows) // block, step, 0)
    c, s_ = cos[...], sin[...]
    for h in range(heads):
        u = dq[h * size : (h + 1) * size, :].T * scale
        u = u * c - pltpu.roll(u, size // 2, 1) * s_
        v = pre[:, h * size : (h + 1) * size]
        r = inv_scale(v)
        gain_out[...] += jnp.sum(u * (v * r), 0, keepdims=True)
        gq_out[:, h * size : (h + 1) * size] = norm_back(v, r, qg[...], u).astype(bf16)

    @pl.when(t == pl.num_programs(0) - 1)
    def _():
        for i in range(back + 1):
            far[i][...] = dkv[i * length : (i + 1) * length, :].astype(far[i].dtype)


def input_back_kernel(cfg, ids, tok, gain, gq, near, came, pre, cos, sin, kg, *rest):
    heads, kv_heads, size, np_ = cfg
    weights = rest[:np_]
    gkv_out, own, oth, k_gain, a_gain = rest[np_:]
    t = pl.program_id(0)
    core = ids[1]

    @pl.when(t == 0)
    def _():
        k_gain[...] = jnp.zeros_like(k_gain)
        a_gain[...] = jnp.zeros_like(a_gain)

    dkv = near[...] + came[...].astype(f32)
    c, s_ = cos[...], sin[...]
    for h in range(kv_heads):
        u = dkv[:, h * size : (h + 1) * size]
        u = u * c - pltpu.roll(u, size // 2, 1) * s_
        v = pre[:, (heads + h) * size : (heads + h + 1) * size]
        r = inv_scale(v)
        k_gain[...] += jnp.sum(u * (v * r), 0, keepdims=True)
        gkv_out[:, h * size : (h + 1) * size] = norm_back(v, r, kg[...], u).astype(bf16)
    gkv_out[:, kv_heads * size :] = dkv[:, kv_heads * size :].astype(bf16)
    split = heads * size
    x = tok[...].astype(f32)
    normal = x * inv_scale(x)
    width = x.shape[1] // np_
    for i in range(np_):
        at = slice(i * width, (i + 1) * width)
        part = dot(gq[...], weights[i][:, :split], NT) + dot(gkv_out[...], weights[i][:, split:], NT)
        a_gain[:, at] += jnp.sum(part * normal[:, at], 0, keepdims=True)
        low = part.astype(bf16)

        @pl.when(t == core)
        def _():
            own[:, at] = low

        @pl.when(t != core)
        def _():
            oth[:, at] = low


def place(out, values, fs, np_):
    width = values.shape[1] // np_
    if np_ == 1:
        out[...] = values
        return
    for i in range(2):
        at = pl.ds(pl.multiple_of((fs if i == 0 else 1 - fs) * width, 128), width)
        out[:, at] = values[:, i * width : (i + 1) * width]


def layer_kernel(np_, ids, tok, b_own, b_oth, f_own, f_oth, valid, *rest):
    out = rest[-1]
    t = pl.program_id(0)
    v = valid[:, :1]
    resid = tok[...].astype(f32) + v * picked(ids, b_own, b_oth, t)
    place(out, (resid + v * picked(ids, f_own, f_oth, t)).astype(bf16), ids[0], np_)


def input_kernel(np_, ids, tok, resid_grad, g_own, g_oth, gain, *rest):
    out = rest[-1]
    t = pl.program_id(0)
    x = tok[...].astype(f32)
    grad = resid_grad[...] + norm_back(x, inv_scale(x), gain[...], picked(ids, g_own, g_oth, t))
    place(out, grad, ids[0], np_)


def product_kernel(pairs, tiles, split, left_t, ids, *rest):
    outs = rest[2 * pairs :]
    m = pl.program_id(0)
    total = None
    for i in range(pairs):
        one = dot(rest[2 * i][...], rest[2 * i + 1][...], NN if left_t else TN)
        total = one if total is None else total + one
    low = total.astype(bf16)
    if split is None:
        outs[0][...] = low
    elif split == 1:
        width = low.shape[1] // 2
        outs[0][...] = low[:, :width]
        outs[1][...] = low[:, width:]
    else:

        @pl.when(m < tiles // 2)
        def _():
            outs[0][...] = low

        @pl.when(m >= tiles // 2)
        def _():
            outs[1][...] = low


def product(name, ids, lefts, rights, split, tile, left_t=False):
    pairs = len(lefts)
    m = lefts[0].shape[0 if left_t else 1]
    k = lefts[0].shape[1 if left_t else 0]
    n = rights[0].shape[1]
    tiles = m // tile
    ins, args = [], []
    for left, right in zip(lefts, rights):
        if left_t:
            ins.append(pl.BlockSpec((tile, k), lambda i, *_: (i, 0)))
        else:
            ins.append(pl.BlockSpec((k, tile), lambda i, *_: (0, i)))
        ins.append(whole(right.shape))
        args += [left, right]
    if split is None:
        outs = [(jax.ShapeDtypeStruct((m, n), bf16), pl.BlockSpec((tile, n), lambda i, *_: (i, 0)))]
    elif split == 1:
        one = (jax.ShapeDtypeStruct((m, n // 2), bf16), pl.BlockSpec((tile, n // 2), lambda i, *_: (i, 0)))
        outs = [one, one]
    else:
        half = tiles // 2
        shape = jax.ShapeDtypeStruct((m // 2, n), bf16)
        outs = [
            (shape, pl.BlockSpec((tile, n), lambda i, *_: (jnp.minimum(i, half - 1), 0))),
            (shape, pl.BlockSpec((tile, n), lambda i, *_: (jnp.maximum(i - half, 0), 0))),
        ]
    return call(
        functools.partial(product_kernel, pairs, tiles, split, left_t),
        name, (tiles,), ins, outs, [],
        2 * pairs * m * k * n, 2 * (pairs * k * (m + n) + m * n), ids, *args,
    )


def swap(values, axis, bit, size):
    return lax.ppermute(values, axis, [(i, i ^ bit) for i in range(size)])


def plus(a, b):
    return (a.astype(f32) + b.astype(f32)).astype(bf16)


def sum_tp(own, oth, size):
    total = plus(own, swap(oth, "tp", 1, size))
    bit = 2
    while bit < size:
        total = plus(total, swap(total, "tp", bit, size))
        bit *= 2
    return total, swap(total, "tp", 1, size)


def sum_line(values, axis, size):
    index = lax.axis_index(axis)
    middle = size // 2
    total = values
    for i in range(middle - 1):
        came = lax.ppermute(total, axis, [(i, i + 1), (size - 1 - i, size - 2 - i)])
        total = plus(total, came)
    if size > 1:
        total = plus(total, lax.ppermute(total, axis, [(middle - 1, middle), (middle, middle - 1)]))
    for i in reversed(range(middle - 1)):
        came = lax.ppermute(total, axis, [(i + 1, i), (size - 2 - i, size - 1 - i)])
        total = jnp.where((index == i) | (index == size - 1 - i), came, total)
    return total


def sum_small(values, axis, size):
    bit = 1
    while bit < size:
        values = values + swap(values, axis, bit, size)
        bit *= 2
    return values


def body(
    n_fs, n_ctx, n_tp,
    tokens, segment_ids, attn_gain, w_query, w_key, w_value, query_gain, key_gain,
    w_out, ffn_gain, w_gate, w_up, w_down, out_grad,
):
    seqs, length, model = tokens.shape
    paired = n_fs == 2
    np_ = 2 if paired else 1
    fs = lax.axis_index("fsdp")
    ctx = lax.axis_index("ctx")
    core = lax.axis_index("tp") % 2
    size = query_gain.shape[0] * n_fs
    heads = w_query.shape[1] // size
    kv_heads = w_key.shape[1] // size
    hidden = w_gate.shape[1]
    q_width, kv_width = heads * size, kv_heads * size
    rows = length // 2
    block = rows
    back = min(n_ctx - 1, -(-(longest_segment - 1) // length))
    scale2 = size**-0.5 * math.log2(math.e)

    w_qkv = jnp.concatenate([w_query, w_key, w_value], 1)

    def gather(weight, axis):
        if paired:
            return [weight, swap(weight, "fsdp", 1, 2)]
        return [lax.all_gather(weight, "fsdp", axis=axis, tiled=True)]

    gains = jnp.concatenate([attn_gain, ffn_gain, query_gain, key_gain])[None, :]
    if paired:
        both = [gains, swap(gains, "fsdp", 1, 2)]
    else:
        every = lax.all_gather(gains, "fsdp", axis=0, tiled=True)
        both = [every[i : i + 1] for i in range(n_fs)]
    part = attn_gain.shape[0]
    small = query_gain.shape[0]
    gain_one = jnp.concatenate([b[:, :part] for b in both], 1).astype(f32)
    gain_two = jnp.concatenate([b[:, part : 2 * part] for b in both], 1).astype(f32)

    def natural(first):
        own_first = jnp.concatenate([b[:, first : first + small] for b in both], 1)
        if paired:
            own_first = jnp.where(fs == 0, own_first, jnp.roll(own_first, small, 1))
        return own_first.astype(f32)

    qg, kg = natural(2 * part), natural(2 * part + small)
    qkv_w = gather(w_qkv, 0)
    out_w = gather(w_out, 1)
    down_w = gather(w_down, 1)
    gate_w = gather(w_gate, 0)
    up_w = gather(w_up, 0)

    def reorder(values):
        if not paired:
            return values
        half = model // 2
        return jnp.where(fs == 0, values, jnp.concatenate([values[..., half:], values[..., :half]], -1))

    index = ctx * length + jnp.arange(length, dtype=jnp.int32)
    row_seg = lax.dynamic_slice_in_dim(segment_ids, ctx * length, length, 1)
    first = jnp.sum((segment_ids[:, None, :] < row_seg[:, :, None]).astype(jnp.int32), -1)
    position = index[None, :] - first
    live = row_seg != 0
    valid = jnp.broadcast_to(live.astype(f32)[:, :, None], (seqs, length, 128))
    window = (back + 1) * length
    start = jnp.where(live, jnp.maximum(first - (ctx - back) * length, 0), window + 1)
    lowest = jnp.min(start.reshape(seqs, 2, rows), -1) // block
    frequency = rope_base ** (-(jnp.arange(size // 2, dtype=f32) * 2.0 / size))
    turned = position.astype(f32)[:, :, None] * frequency
    cosine, sine = jnp.cos(turned), jnp.sin(turned)
    cos = jnp.concatenate([cosine, cosine], -1)
    sin = jnp.concatenate([-sine, sine], -1)
    tok = reorder(tokens)
    grad = reorder(out_grad)
    low_grad = jnp.where(live[:, :, None], grad, jnp.zeros((), bf16))
    start = start[:, None, :]

    def scalars(s):
        return jnp.concatenate([jnp.stack([fs, core]).astype(jnp.int32), lowest[s]])

    ids = [scalars(s) for s in range(seqs)]
    cfg = (heads, kv_heads, size, np_, back, block, scale2)

    def tiled(width):
        return pl.BlockSpec((rows, width), lambda i, *_: (i, 0))

    def tiled_t(height):
        return pl.BlockSpec((height, rows), lambda i, *_: (0, i))

    def shape(*dims, dtype=bf16):
        return jax.ShapeDtypeStruct(dims, dtype)

    half_pair = [(shape(rows, model), whole((rows, model)))] * 2

    normed, queries, kv, pre = [], [], [], []
    for s in range(seqs):
        n, q, one, p = call(
            functools.partial(qkv_kernel, heads, kv_heads, size, np_),
            "qkv", (2,),
            [tiled(model), whole((1, model)), tiled(size), tiled(size), whole((1, size)), whole((1, size))]
            + [whole(w.shape) for w in qkv_w],
            [
                (shape(length, model), tiled(model)),
                (shape(length, q_width), tiled(q_width)),
                (shape(length, 2 * kv_width), tiled(2 * kv_width)),
                (shape(length, q_width + kv_width, dtype=f32), tiled(q_width + kv_width)),
            ],
            [],
            2 * length * model * (q_width + 2 * kv_width), 8 * length * model, ids[s],
            tok[s], gain_one, cos[s], sin[s], qg, kg, *qkv_w,
        )
        chunks = [one]
        for _ in range(back):
            chunks.insert(0, lax.ppermute(chunks[0], "ctx", [(i, i + 1) for i in range(n_ctx - 1)]))
        normed.append(n)
        queries.append(q)
        kv.append(chunks)
        pre.append(p)

    mixed, lse, branch = [], [], []
    for s in range(seqs):
        own, oth, m, l = call(
            functools.partial(attend_kernel, cfg),
            "attend", (2,),
            [tiled(q_width), pl.BlockSpec((1, rows), lambda i, *_: (0, i))]
            + [whole((length, 2 * kv_width))] * (back + 1)
            + [whole(w.shape) for w in out_w],
            half_pair
            + [
                (shape(q_width, length), tiled_t(q_width)),
                (shape(8 * -(-heads // 8), length, dtype=f32), tiled_t(8 * -(-heads // 8))),
            ],
            [
                pltpu.VMEM((window, 2 * kv_width), bf16),
                pltpu.VMEM((q_width, rows), f32),
                pltpu.VMEM((8 * -(-heads // 8), rows), f32),
            ],
            4 * length * length * q_width * 4, 8 * length * model, ids[s],
            queries[s], start[s], *kv[s], *out_w,
        )
        mixed.append(m)
        lse.append(l)
        branch.append(sum_tp(own, oth, n_tp))

    tile = 256
    steps = hidden // tile
    normed_two, active, grad_gate, grad_up, grad_two, ffn_gains = [], [], [], [], [], []
    for s in range(seqs):
        col = pl.BlockSpec((length, tile), lambda i, *_: (0, i))
        w_in = [pl.BlockSpec((w.shape[0], tile), lambda i, *_: (0, i)) for w in gate_w]
        w_dn = [pl.BlockSpec((tile, w.shape[1]), lambda i, *_: (i, 0)) for w in down_w]
        n2, act, gg, gu, own, oth, fg = call(
            functools.partial(ffn_kernel, np_),
            "ffn", (steps,),
            [whole((length, model)), whole((rows, model)), whole((rows, model)), whole((length, 128)),
             whole((1, model)), whole((length, model))] + w_in + w_in + w_dn,
            [
                (shape(length, model), whole((length, model))),
                (shape(length, hidden), col),
                (shape(length, hidden), col),
                (shape(length, hidden), col),
            ]
            + half_pair
            + [(shape(1, model, dtype=f32), whole((1, model)))],
            [pltpu.VMEM((length, model), f32), pltpu.VMEM((length, model), f32)],
            10 * length * model * hidden, 8 * length * model, ids[s],
            tok[s], *branch[s], valid[s], gain_two, low_grad[s], *gate_w, *up_w, *down_w,
        )
        normed_two.append(n2)
        active.append(act)
        grad_gate.append(gg)
        grad_up.append(gu)
        grad_two.append(sum_tp(own, oth, n_tp))
        ffn_gains.append(fg)

    rows_split, cols_split = (0, 1) if paired else (None, None)
    gate_parts = product("gate_grad", ids[0], normed_two, grad_gate, rows_split, 256)
    up_parts = product("up_grad", ids[0], normed_two, grad_up, rows_split, 256)
    down_parts = product("down_grad", ids[0], active, [low_grad[s] for s in range(seqs)], cols_split, 256)

    layer_out = None
    for s in range(seqs):
        parts = jnp.dot(active[s], jnp.concatenate(down_w, 1), preferred_element_type=f32).astype(bf16)
        parts = jnp.where(core == 0, parts, jnp.roll(parts, rows, 0))
        ffn = sum_tp(parts[:rows], parts[rows:], n_tp)
        extra = [] if layer_out is None else [layer_out]
        layer_out = call(
            functools.partial(layer_kernel, np_),
            "layer_out", (2,),
            [tiled(model)] + [whole((rows, model))] * 4 + [tiled(128)]
            + [pl.BlockSpec(memory_space=pl.ANY)] * len(extra),
            [(shape(seqs, length, model), pl.BlockSpec((None, rows, model), lambda i, *_, s=s: (s, i, 0)))],
            [],
            0, 10 * length * model, ids[s],
            tok[s], *branch[s], *ffn, valid[s], *extra,
            aliases={7: 0} if extra else None,
        )[0]

    resid_grad, grad_branch, grad_query, near, q_gains, came = [], [], [], [], [], []
    down_perm = [(i + 1, i) for i in range(n_ctx - 1)]
    for s in range(seqs):
        far_shapes = [(shape(length, 2 * kv_width), whole((length, 2 * kv_width)))] * back
        rg, gb, gq, qgain, *far, dkv = call(
            functools.partial(attend_back_kernel, cfg),
            "attend_back", (2,),
            [tiled(model)] + [whole((rows, model))] * 4 + [tiled(128), whole((1, model)), tiled(model),
             tiled_t(q_width), tiled_t(lse[s].shape[0]), tiled(q_width), pl.BlockSpec((1, rows), lambda i, *_: (0, i)),
             tiled(q_width + kv_width), tiled(size), tiled(size), whole((1, size))]
            + [whole((length, 2 * kv_width))] * (back + 1)
            + [whole(w.shape) for w in out_w],
            [
                (shape(length, model, dtype=f32), tiled(model)),
                (shape(length, model), tiled(model)),
                (shape(length, q_width), tiled(q_width)),
                (shape(1, size, dtype=f32), whole((1, size))),
            ]
            + far_shapes
            + [(shape(length, 2 * kv_width, dtype=f32), whole((length, 2 * kv_width)))],
            [
                pltpu.VMEM((window, 2 * kv_width), bf16),
                pltpu.VMEM((window, 2 * kv_width), f32),
                pltpu.VMEM((q_width, rows), f32),
                pltpu.VMEM((q_width, rows), bf16),
            ],
            10 * length * length * q_width * 4, 16 * length * model, ids[s],
            tok[s], *branch[s], *grad_two[s], valid[s], gain_two, grad[s], mixed[s], lse[s], queries[s],
            start[s], pre[s], cos[s], sin[s], qg, *kv[s], *out_w,
        )
        moving = None
        for one in far:
            moving = lax.ppermute(one if moving is None else plus(one, moving), "ctx", down_perm)
        resid_grad.append(rg)
        grad_branch.append(gb)
        grad_query.append(gq)
        q_gains.append(qgain)
        near.append(dkv)
        came.append(moving if moving is not None else jnp.zeros_like(dkv, bf16))

    out_parts = product("out_grad", ids[0], mixed, grad_branch, cols_split, 256, left_t=True)
    query_parts = product("query_grad", ids[0], normed, grad_query, rows_split, 256)

    grad_kv, k_gains, a_gains, grad_one = [], [], [], []
    for s in range(seqs):
        gkv, own, oth, kgain, again = call(
            functools.partial(input_back_kernel, (heads, kv_heads, size, np_)),
            "input_back", (2,),
            [tiled(model), whole((1, model)), tiled(q_width), tiled(2 * kv_width), tiled(2 * kv_width),
             tiled(q_width + kv_width), tiled(size), tiled(size), whole((1, size))]
            + [whole(w.shape) for w in qkv_w],
            [(shape(length, 2 * kv_width), tiled(2 * kv_width))]
            + half_pair
            + [(shape(1, size, dtype=f32), whole((1, size))), (shape(1, model, dtype=f32), whole((1, model)))],
            [],
            2 * length * model * (q_width + 2 * kv_width), 8 * length * model, ids[s],
            tok[s], gain_one, grad_query[s], near[s], came[s], pre[s], cos[s], sin[s], kg, *qkv_w,
        )
        grad_kv.append(gkv)
        k_gains.append(kgain)
        a_gains.append(again)
        grad_one.append(sum_tp(own, oth, n_tp))

    kv_parts = product("kv_grad", ids[0], normed, grad_kv, rows_split, 256)

    input_grad = None
    for s in range(seqs):
        extra = [] if input_grad is None else [input_grad]
        input_grad = call(
            functools.partial(input_kernel, np_),
            "input_grad", (2,),
            [tiled(model), tiled(model)] + [whole((rows, model))] * 2 + [whole((1, model))]
            + [pl.BlockSpec(memory_space=pl.ANY)] * len(extra),
            [(shape(seqs, length, model, dtype=f32), pl.BlockSpec((None, rows, model), lambda i, *_, s=s: (s, i, 0)))],
            [],
            0, 14 * length * model, ids[s],
            tok[s], resid_grad[s], *grad_one[s], gain_one, *extra,
            aliases={6: 0} if extra else None,
        )[0]

    def owned(parts, axis):
        if paired:
            return plus(parts[0], swap(parts[1], "fsdp", 1, 2))
        return lax.psum_scatter(parts[0], "fsdp", scatter_dimension=axis, tiled=True)

    gate_sum = sum_line(owned(gate_parts, 0), "ctx", n_ctx)
    up_sum = sum_line(owned(up_parts, 0), "ctx", n_ctx)
    down_sum = sum_line(owned(down_parts, 1), "ctx", n_ctx)
    out_sum = sum_line(owned(out_parts, 1), "ctx", n_ctx)
    query_sum = sum_line(owned(query_parts, 0), "ctx", n_ctx)
    kv_sum = sum_line(owned(kv_parts, 0), "ctx", n_ctx)

    def order(values):
        if not paired:
            return values
        return jnp.where(fs == 0, values, jnp.roll(values, model // 2, 1))

    gains_grad = jnp.concatenate(
        [order(sum(a_gains)), order(sum(ffn_gains)), sum(q_gains), sum(k_gains)], 1
    )
    for axis, count in (("tp", n_tp), ("fsdp", n_fs), ("ctx", n_ctx)):
        gains_grad = sum_small(gains_grad, axis, count)
    gains_grad = gains_grad[0]

    def mine(first, width):
        return lax.dynamic_slice_in_dim(gains_grad, first + fs * (width // n_fs), width // n_fs, 0)

    return (
        layer_out,
        input_grad,
        mine(0, model),
        query_sum.astype(f32),
        kv_sum[:, :kv_width].astype(f32),
        kv_sum[:, kv_width:].astype(f32),
        mine(2 * model, size),
        mine(2 * model + size, size),
        out_sum.astype(f32),
        mine(model, model),
        gate_sum.astype(f32),
        up_sum.astype(f32),
        down_sum.astype(f32),
    )


def solution(mesh):
    n_fs, n_ctx, n_tp = mesh.shape["fsdp"], mesh.shape["ctx"], mesh.shape["tp"]
    placed = (
        P("fsdp", "ctx", None),
        P("fsdp", None),
        P("fsdp"),
        P("fsdp", "tp"),
        P("fsdp", "tp"),
        P("fsdp", "tp"),
        P("fsdp"),
        P("fsdp"),
        P("tp", "fsdp"),
        P("fsdp"),
        P("fsdp", "tp"),
        P("fsdp", "tp"),
        P("tp", "fsdp"),
        P("fsdp", "ctx", None),
    )
    return jax.shard_map(
        functools.partial(body, n_fs, n_ctx, n_tp),
        mesh=mesh,
        in_specs=placed,
        out_specs=(
            P("fsdp", "ctx", None),
            P("fsdp", "ctx", None),
            P("fsdp"),
            P("fsdp", "tp"),
            P("fsdp", "tp"),
            P("fsdp", "tp"),
            P("fsdp"),
            P("fsdp"),
            P("tp", "fsdp"),
            P("fsdp"),
            P("fsdp", "tp"),
            P("fsdp", "tp"),
            P("tp", "fsdp"),
        ),
        check_vma=False,
    )
```

```python
import functools
import math

import jax
import jax.numpy as jnp
from jax import lax
from jax.experimental import pallas as pl
from jax.experimental.pallas import tpu as pltpu
from jax.sharding import PartitionSpec as P

epsilon = 1e-06
rope_base = 1000000.0
longest_segment = 1024
f32 = jnp.float32
bf16 = jnp.bfloat16

cost = dict(
    keys=4.6, query=4.5, attend_own=6.0, attend=8.0, ffn=12.5, down=4.8, layer_out=4.0,
    attend_back=18.0, input_back=7.2, input_grad=4.5, gate_up_grad=12.0, down_grad=6.0,
    out_grad=4.6, query_grad=5.7, kv_grad=5.7,
)

NN = (((1,), (0,)), ((), ()))
NT = (((1,), (1,)), ((), ()))
TN = (((0,), (0,)), ((), ()))


def dot(left, right, dims=NN):
    return lax.dot_general(left, right, dims, preferred_element_type=f32)


def inv_scale(values):
    return lax.rsqrt(jnp.mean(values * values, -1, keepdims=True) + epsilon)


def norm_back(values, scale, gain, grad):
    scaled = grad * gain
    return scale * scaled - values * (scale * scale * scale) * jnp.mean(
        scaled * values, -1, keepdims=True
    )


def rows_of(index, size):
    return pl.ds(pl.multiple_of(index * size, size), size)


def ordered(ref, fs, np_):
    if np_ == 1:
        return ref[...]
    half = ref.shape[-1] // 2
    first = ref[:, pl.ds(pl.multiple_of(fs * half, 128), half)]
    other = ref[:, pl.ds(pl.multiple_of((1 - fs) * half, 128), half)]
    return jnp.concatenate([first, other], 1)


def whole(shape):
    return pl.BlockSpec(shape, lambda *_: (0,) * len(shape))


def columns(parts):
    width = parts[0]
    return [(i * width, (i + 1) * width) for i in range(len(parts))]


def call(kernel, name, grid, ins, outs, scratch, flops, moved, scalars, *args, aliases=None):
    return pl.pallas_call(
        kernel,
        name=name,
        out_shape=[o[0] for o in outs],
        grid_spec=pltpu.PrefetchScalarGridSpec(
            num_scalar_prefetch=1,
            grid=grid,
            in_specs=ins,
            out_specs=[o[1] for o in outs],
            scratch_shapes=scratch,
        ),
        input_output_aliases=aliases or {},
        compiler_params=pltpu.CompilerParams(dimension_semantics=("arbitrary",) * len(grid)),
        cost_estimate=pl.CostEstimate(flops=1, bytes_accessed=1, transcendentals=0),
    )(scalars, *args)


def project(low, weights, np_):
    width = low.shape[1] // np_
    acc = None
    for i in range(np_):
        one = dot(low[:, i * width : (i + 1) * width], weights[i][...])
        acc = one if acc is None else acc + one
    return acc


def turn(acc, count, size, g, c, s, out):
    for h in range(count):
        u = acc[:, h * size : (h + 1) * size]
        u = u * inv_scale(u) * g
        out[:, h * size : (h + 1) * size] = (u * c + pltpu.roll(u, size // 2, 1) * s).astype(bf16)


def kv_kernel(kv_heads, size, np_, ids, tok, gain, cos, sin, kg, *rest):
    weights, (normed, kv_out, pre_out) = rest[:np_], rest[np_:]
    x = ordered(tok, ids[0], np_).astype(f32)
    low = (x * inv_scale(x) * gain[...]).astype(bf16)
    normed[...] = low
    acc = project(low, weights, np_)
    pre_out[...] = acc[:, : kv_heads * size]
    turn(acc, kv_heads, size, kg[...], cos[...], sin[...], kv_out)
    kv_out[:, kv_heads * size :] = acc[:, kv_heads * size :].astype(bf16)


def query_kernel(heads, size, np_, ids, normed, cos, sin, qg, *rest):
    weights, (q_out, pre_out) = rest[:np_], rest[np_:]
    acc = project(normed[...], weights, np_)
    pre_out[...] = acc
    turn(acc, heads, size, qg[...], cos[...], sin[...], q_out)


def allowed_block(key_base, start, row_base, block, rows):
    key_index = key_base + lax.broadcasted_iota(jnp.int32, (block, rows), 0)
    row_index = row_base + lax.broadcasted_iota(jnp.int32, (block, rows), 1)
    return (key_index >= start) & (key_index <= row_index)


def attend_blocks(cfg, low, high, base, kv, q, start_row, row_base, acc, total):
    heads, kv_heads, size, block, scale2 = cfg
    group = heads // kv_heads
    rows = q.shape[0]

    def step(kb, carry):
        at = pl.ds(pl.multiple_of((kb - base) * block, block), block)
        allow = allowed_block(kb * block, start_row, row_base, block, rows)
        for g in range(kv_heads):
            k = kv[at, g * size : (g + 1) * size]
            v = kv[at, (kv_heads + g) * size : (kv_heads + g + 1) * size]
            for h in range(g * group, (g + 1) * group):
                s = dot(k, q[:, h * size : (h + 1) * size], NT)
                e = jnp.where(allow, jnp.exp2(s * scale2), 0.0)
                total[h : h + 1, :] += jnp.sum(e, 0, keepdims=True)
                acc[h * size : (h + 1) * size, :] += dot(v, e.astype(bf16), TN)
        return carry

    lax.fori_loop(low, high, step, 0)


def attend_own_kernel(cfg, back, ids, q, start, kv, acc, total):
    t = pl.program_id(0)
    rows = q.shape[0]
    base = back * kv.shape[0]
    acc[...] = jnp.zeros_like(acc)
    total[...] = jnp.zeros_like(total)
    first = base // cfg[3]
    attend_blocks(
        cfg, jnp.maximum(ids[2 + t], first), (base + (t + 1) * rows) // cfg[3], first,
        kv, q, start[...], base + t * rows, acc, total,
    )


def attend_kernel(cfg, np_, back, ids, q, start, acc_in, total_in, *rest):
    heads, _, size, block, _ = cfg
    chunks = rest[:back]
    w_out = rest[back : back + np_]
    own, oth, mixed_out, lse_out, kv, acc, total = rest[back + np_ :]
    t = pl.program_id(0)
    core = ids[1]
    rows = q.shape[0]
    length = chunks[0].shape[0]

    @pl.when(t == 0)
    def _():
        for i in range(back):
            kv[i * length : (i + 1) * length, :] = chunks[i][...]

    acc[...] = acc_in[...]
    total[...] = total_in[...]
    attend_blocks(
        cfg, ids[2 + t], back * length // block, 0, kv, q, start[...], back * length + t * rows, acc, total
    )
    sums = total[...]
    sums = jnp.where(sums > 0.0, sums, 1.0)
    lse_out[...] = jnp.log2(sums)
    inverse = 1.0 / sums
    for h in range(heads):
        part = (acc[h * size : (h + 1) * size, :] * inverse[h : h + 1, :]).astype(bf16)
        mixed_out[h * size : (h + 1) * size, :] = part
    mixed = mixed_out[...]
    width = w_out[0].shape[1]
    for i in range(np_):
        part = dot(mixed, w_out[i][...], TN).astype(bf16)

        @pl.when(t == core)
        def _():
            own[:, i * width : (i + 1) * width] = part

        @pl.when(t != core)
        def _():
            oth[:, i * width : (i + 1) * width] = part


def ffn_kernel(np_, ids, tok, b_own, b_oth, valid, gain, grad, *rest):
    gate_w, up_w, down_w = rest[:np_], rest[np_ : 2 * np_], rest[2 * np_ : 3 * np_]
    n2_out, act_out, gg_out, gu_out, own, oth, gain_out, hat, acc = rest[3 * np_ :]
    f = pl.program_id(0)
    core = ids[1]
    half = b_own.shape[0]

    @pl.when(f == 0)
    def _():
        for ref, tile in ((b_own, core), (b_oth, 1 - core)):
            at = rows_of(tile, half)
            tokens = ordered(tok.at[at], ids[0], np_).astype(f32)
            resid = tokens + valid[at, :1] * ref[...].astype(f32)
            normal = resid * inv_scale(resid)
            hat[at, :] = normal
            n2_out[at, :] = (normal * gain[...]).astype(bf16)
        acc[...] = jnp.zeros_like(acc)

    width = tok.shape[1] // np_
    parts = [(i * width, (i + 1) * width) for i in range(np_)]
    gate = up = active_grad = None
    for i, (a, b) in enumerate(parts):
        x = n2_out[:, a:b]
        g, u, d = dot(x, gate_w[i][...]), dot(x, up_w[i][...]), dot(grad[:, a:b], down_w[i][...], NT)
        gate, up, active_grad = (g, u, d) if i == 0 else (gate + g, up + u, active_grad + d)
    sigma = jax.nn.sigmoid(gate)
    silu = gate * sigma
    act_out[...] = (silu * up).astype(bf16)
    gg = (active_grad * up * sigma * (1.0 + gate * (1.0 - sigma))).astype(bf16)
    gu = (active_grad * silu).astype(bf16)
    gg_out[...] = gg
    gu_out[...] = gu
    for i, (a, b) in enumerate(parts):
        acc[:, a:b] += dot(gg, gate_w[i][...], NT) + dot(gu, up_w[i][...], NT)

    @pl.when(f == pl.num_programs(0) - 1)
    def _():
        own[...] = acc[rows_of(core, half), :].astype(bf16)
        oth[...] = acc[rows_of(1 - core, half), :].astype(bf16)
        gain_out[...] = jnp.sum(acc[...] * hat[...], 0, keepdims=True)


def down_kernel(np_, ids, act, *rest):
    weights, (own, oth) = rest[:np_], rest[-2:]
    t = pl.program_id(0)
    width = weights[0].shape[1]
    for i in range(np_):
        part = dot(act[...], weights[i][...]).astype(bf16)

        @pl.when(t == ids[1])
        def _():
            own[:, i * width : (i + 1) * width] = part

        @pl.when(t != ids[1])
        def _():
            oth[:, i * width : (i + 1) * width] = part


def picked(ids, own, oth, t):
    return jnp.where(ids[1] == t, own[...].astype(f32), oth[...].astype(f32))


def attend_back_kernel(cfg, ids, tok, b_own, b_oth, t_own, t_oth, valid, gain, grad, mixed, lse, q, start, pre, cos, sin, qg, *rest):
    heads, kv_heads, size, np_, back, block, scale2 = cfg
    chunks = rest[: back + 1]
    w_out = rest[back + 1 : back + 1 + np_]
    outs = rest[back + 1 + np_ :]
    resid_out, branch_out, gq_out, gain_out = outs[:4]
    far = outs[4 : 4 + back + 1]
    kv, dkv, dq, dout = outs[4 + back + 1 :]
    t = pl.program_id(0)
    rows = q.shape[0]
    length = chunks[0].shape[0]
    group = heads // kv_heads
    scale = size**-0.5

    @pl.when(t == 0)
    def _():
        for i in range(back + 1):
            kv[i * length : (i + 1) * length, :] = chunks[i][...]
        dkv[...] = jnp.zeros_like(dkv)
        gain_out[...] = jnp.zeros_like(gain_out)

    resid = ordered(tok, ids[0], np_).astype(f32) + valid[:, :1] * picked(ids, b_own, b_oth, t)
    resid_grad = ordered(grad, ids[0], np_).astype(f32) + norm_back(
        resid, inv_scale(resid), gain[...], picked(ids, t_own, t_oth, t)
    )
    resid_out[...] = resid_grad
    low = (valid[:, :1] * resid_grad).astype(bf16)
    branch_out[...] = low
    width = low.shape[1] // np_
    mixed_grad = dot(w_out[0][...], low[:, :width], NT)
    for i in range(1, np_):
        mixed_grad = mixed_grad + dot(w_out[i][...], low[:, i * width : (i + 1) * width], NT)
    dout[...] = mixed_grad.astype(bf16)
    delta = [
        jnp.sum(
            dout[h * size : (h + 1) * size, :].astype(f32) * mixed[h * size : (h + 1) * size, :].astype(f32),
            0,
            keepdims=True,
        )
        for h in range(heads)
    ]
    dq[...] = jnp.zeros_like(dq)
    row_base = back * length + t * rows
    start_row = start[...]

    def step(kb, carry):
        at = pl.ds(pl.multiple_of(kb * block, block), block)
        allow = allowed_block(kb * block, start_row, row_base, block, rows)
        for g in range(kv_heads):
            k = kv[at, g * size : (g + 1) * size]
            v = kv[at, (kv_heads + g) * size : (kv_heads + g + 1) * size]
            dk = dv = None
            for h in range(g * group, (g + 1) * group):
                qh = q[:, h * size : (h + 1) * size]
                do = dout[h * size : (h + 1) * size, :]
                s = dot(k, qh, NT)
                p = jnp.where(allow, jnp.exp2(s * scale2 - lse[h : h + 1, :]), 0.0)
                dp = dot(v, do)
                ds = (p * (dp - delta[h])).astype(bf16)
                one_v = dot(p.astype(bf16), do, NT)
                one_k = dot(ds, qh)
                dk, dv = (one_k, one_v) if dk is None else (dk + one_k, dv + one_v)
                dq[h * size : (h + 1) * size, :] += dot(k, ds, TN)
            dkv[at, g * size : (g + 1) * size] += dk * scale
            dkv[at, (kv_heads + g) * size : (kv_heads + g + 1) * size] += dv
        return carry

    lax.fori_loop(ids[2 + t], (row_base + rows) // block, step, 0)
    c, s_ = cos[...], sin[...]
    for h in range(heads):
        u = dq[h * size : (h + 1) * size, :].T * scale
        u = u * c - pltpu.roll(u, size // 2, 1) * s_
        v = pre[:, h * size : (h + 1) * size]
        r = inv_scale(v)
        gain_out[...] += jnp.sum(u * (v * r), 0, keepdims=True)
        gq_out[:, h * size : (h + 1) * size] = norm_back(v, r, qg[...], u).astype(bf16)

    @pl.when(t == pl.num_programs(0) - 1)
    def _():
        for i in range(back + 1):
            far[i][...] = dkv[i * length : (i + 1) * length, :].astype(far[i].dtype)


def input_back_kernel(cfg, ids, tok, gain, gq, near, came, pre, cos, sin, kg, *rest):
    heads, kv_heads, size, np_ = cfg
    weights = rest[: 2 * np_]
    gkv_out, own, oth, k_gain, a_gain = rest[-5:]
    t = pl.program_id(0)
    core = ids[1]

    @pl.when(t == 0)
    def _():
        k_gain[...] = jnp.zeros_like(k_gain)
        a_gain[...] = jnp.zeros_like(a_gain)

    dkv = near[...] + came[...].astype(f32)
    c, s_ = cos[...], sin[...]
    for h in range(kv_heads):
        u = dkv[:, h * size : (h + 1) * size]
        u = u * c - pltpu.roll(u, size // 2, 1) * s_
        v = pre[:, h * size : (h + 1) * size]
        r = inv_scale(v)
        k_gain[...] += jnp.sum(u * (v * r), 0, keepdims=True)
        gkv_out[:, h * size : (h + 1) * size] = norm_back(v, r, kg[...], u).astype(bf16)
    gkv_out[:, kv_heads * size :] = dkv[:, kv_heads * size :].astype(bf16)
    x = ordered(tok, ids[0], np_).astype(f32)
    normal = x * inv_scale(x)
    width = x.shape[1] // np_
    for i in range(np_):
        at = slice(i * width, (i + 1) * width)
        part = dot(gq[...], weights[i][...], NT)
        part = part + dot(gkv_out[...], weights[np_ + i][...], NT)
        a_gain[:, at] += jnp.sum(part * normal[:, at], 0, keepdims=True)
        low = part.astype(bf16)

        @pl.when(t == core)
        def _():
            own[:, at] = low

        @pl.when(t != core)
        def _():
            oth[:, at] = low


def place(out, values, fs, np_):
    width = values.shape[1] // np_
    if np_ == 1:
        out[...] = values
        return
    for i in range(2):
        at = pl.ds(pl.multiple_of((fs if i == 0 else 1 - fs) * width, 128), width)
        out[:, at] = values[:, i * width : (i + 1) * width]


def layer_kernel(np_, fine, ids, tok, b_own, b_oth, f_own, f_oth, valid, *rest):
    out = rest[-1]
    t = pl.program_id(0) // fine
    v = valid[:, :1]
    resid = ordered(tok, ids[0], np_).astype(f32) + v * picked(ids, b_own, b_oth, t)
    place(out, (resid + v * picked(ids, f_own, f_oth, t)).astype(bf16), ids[0], np_)


def input_kernel(np_, fine, ids, tok, resid_grad, g_own, g_oth, gain, *rest):
    out = rest[-1]
    t = pl.program_id(0) // fine
    x = ordered(tok, ids[0], np_).astype(f32)
    grad = resid_grad[...] + norm_back(x, inv_scale(x), gain[...], picked(ids, g_own, g_oth, t))
    place(out, grad, ids[0], np_)


def product_kernel(pairs, groups, tiles, split, left_t, tail, ids, *rest):
    count = 1 if split is None else 2
    outs = rest[-count:]
    m = pl.program_id(0)

    def low():
        columns = []
        for j in range(groups):
            total = None
            for i in range(pairs):
                one = dot(rest[i][...], rest[pairs * (1 + j) + i][...], NN if left_t else TN)
                total = one if total is None else total + one
            columns.append(total.astype(bf16))
        return columns[0] if groups == 1 else jnp.concatenate(columns, 1)

    if split is None:
        outs[0][...] = low()
    elif split == 1:
        value = low()
        width = value.shape[1] // 2
        outs[0][...] = value[:, :width]
        outs[1][...] = value[:, width:]
    else:

        @pl.when(m < tiles // 2)
        def _():
            outs[0][...] = low()

        @pl.when((m >= tiles // 2) & (m < tiles))
        def _():
            outs[1][...] = low()

    if tail:

        @pl.when(m == tiles)
        def _():
            at = pairs * (1 + groups)
            for i in range(2):
                outs[i][: rest[at + i].shape[0], :] = rest[at + i][...]


def product(name, ids, lefts, rights, split, tile, left_t=False, at=0, height=None, into=None, tail=None):
    pairs, groups = len(lefts), len(rights)
    m = lefts[0].shape[0 if left_t else 1]
    k = lefts[0].shape[1 if left_t else 0]
    n = sum(r[0].shape[1] for r in rights)
    tiles = m // tile
    ins, args = [], []
    for left in lefts:
        if left_t:
            ins.append(pl.BlockSpec((tile, k), lambda i, *_: (jnp.minimum(i, tiles - 1), 0)))
        else:
            ins.append(pl.BlockSpec((k, tile), lambda i, *_: (0, jnp.minimum(i, tiles - 1))))
        args.append(left)
    for group in rights:
        for right in group:
            ins.append(whole(right.shape))
            args.append(right)
    if split is None:
        shape = jax.ShapeDtypeStruct((height or m, n), bf16)
        outs = [(shape, pl.BlockSpec((tile, n), lambda i, *_: (i + at, 0)))]
    elif split == 1:
        shape = jax.ShapeDtypeStruct((height or m, n // 2), bf16)
        outs = [(shape, pl.BlockSpec((tile, n // 2), lambda i, *_: (i + at, 0)))] * 2
    else:
        half = tiles // 2
        shape = jax.ShapeDtypeStruct((height or m // 2, n), bf16)
        last = at + half if tail is not None else at + half - 1

        def own(i, *_):
            return (jnp.where(i < half, i + at, jnp.where(i < tiles, half - 1 + at, last)), 0)

        def other(i, *_):
            return (jnp.where(i < tiles, jnp.maximum(i - half, 0) + at, last), 0)

        outs = [(shape, pl.BlockSpec((tile, n), own)), (shape, pl.BlockSpec((tile, n), other))]
    if tail is not None:
        ins += [whole(v.shape) for v in tail]
        args += list(tail)
    aliases = None
    if into is not None:
        aliases = {1 + len(ins) + i: i for i in range(len(into))}
        ins += [pl.BlockSpec(memory_space=pl.ANY)] * len(into)
        args += list(into)
    return call(
        functools.partial(product_kernel, pairs, groups, tiles, split, left_t, tail is not None),
        name, (tiles + (tail is not None),), ins, outs, [], 0, 0, ids, *args, aliases=aliases,
    )


def swap(values, axis, bit, size):
    return lax.ppermute(values, axis, [(i, i ^ bit) for i in range(size)])


def plus(a, b):
    return a + b


class Line:
    def __init__(self):
        self.last = None
        self.waited = ()

    def __call__(self, fn, *args):
        if self.last is not None:
            args, _, _ = lax.optimization_barrier((args, self.last, self.waited))
        outs = fn(*args)
        self.last, self.waited = jax.tree.leaves(outs)[0], ()
        return outs

    def wait(self, *values):
        self.waited += values

    def after(self, value):
        return lax.optimization_barrier((value, self.last, self.waited))[0]


class Steps:
    def __init__(self, steps):
        self.steps, self.value = steps, None

    def __call__(self, count=1):
        for _ in range(count):
            self.value = next(self.steps)
        return self.value


def sum_tp(line, own, oth, size):
    total = line(plus, own, swap(line.after(oth), "tp", 1, size))
    yield total
    bit = 2
    while bit < size:
        total = line(plus, total, swap(total, "tp", bit, size))
        bit *= 2
        if bit < size:
            yield total
    yield total, swap(total, "tp", 1, size)


def sum_line(line, total, axis, size):
    index = lax.axis_index(axis)
    middle = size // 2
    for i in range(middle - 1):
        came = lax.ppermute(total, axis, [(i, i + 1), (size - 1 - i, size - 2 - i)])
        total = line(plus, total, came)
        yield total
    total = line(plus, total, lax.ppermute(total, axis, [(middle - 1, middle), (middle, middle - 1)]))
    yield total
    for i in reversed(range(middle - 1)):
        came = lax.ppermute(total, axis, [(i + 1, i), (size - 2 - i, size - 1 - i)])
        total = jnp.where((index == i) | (index == size - 1 - i), came, total)
    yield total


def sum_small(values, axis, size):
    bit = 1
    while bit < size:
        values = values + swap(values, axis, bit, size)
        bit *= 2
    return values


def body(
    n_fs, n_ctx, n_tp,
    tokens, segment_ids, attn_gain, w_query, w_key, w_value, query_gain, key_gain,
    w_out, ffn_gain, w_gate, w_up, w_down, out_grad,
):
    seqs, length, model = tokens.shape
    paired = n_fs == 2
    np_ = 2 if paired else 1
    fs = lax.axis_index("fsdp")
    ctx = lax.axis_index("ctx")
    core = lax.axis_index("tp") % 2
    size = query_gain.shape[0] * n_fs
    heads = w_query.shape[1] // size
    kv_heads = w_key.shape[1] // size
    hidden = w_gate.shape[1]
    q_width, kv_width = heads * size, kv_heads * size
    rows = length // 2
    block = rows
    back = min(n_ctx - 1, -(-(longest_segment - 1) // length))
    scale2 = size**-0.5 * math.log2(math.e)

    def gather(weight, axis):
        if paired:
            return [weight, swap(weight, "fsdp", 1, 2)]
        return [lax.all_gather(weight, "fsdp", axis=axis, tiled=True)]

    kv_w = gather(jnp.concatenate([w_key, w_value], 1), 0)
    query_w = gather(w_query, 0)
    out_w = gather(w_out, 1)
    gate_w = gather(w_gate, 0)
    up_w = gather(w_up, 0)
    down_w = gather(w_down, 1)

    part, small = attn_gain.shape[0], query_gain.shape[0]
    padding = part - 2 * small
    gains = jnp.concatenate([query_gain, key_gain] + ([jnp.zeros((padding,), bf16)] if padding > 0 else []))
    gains = jnp.stack([attn_gain, ffn_gain, gains[:part]]) if padding >= 0 else None
    if paired:
        gains, kv_w[0] = lax.optimization_barrier((gains, kv_w[0]))
    both = [gains, swap(gains, "fsdp", 1, 2)] if paired else None
    if paired:
        wide = jnp.concatenate(both, 1).astype(f32)
        gain_one, gain_two = wide[:1], wide[1:2]

    def natural(first, values):
        if not paired:
            return lax.all_gather(values, "fsdp", axis=0, tiled=True)[None, :].astype(f32)
        own_first = jnp.concatenate([b[2:, first : first + small] for b in both], 1)
        return jnp.where(fs == 0, own_first, jnp.roll(own_first, small, 1)).astype(f32)

    if not paired:
        gain_one, gain_two = natural(0, attn_gain), natural(0, ffn_gain)
    qg, kg = natural(0, query_gain), natural(small, key_gain)

    def reorder(values):
        if not paired:
            return values
        half = model // 2
        return jnp.where(fs == 0, values, jnp.concatenate([values[..., half:], values[..., :half]], -1))

    index = ctx * length + jnp.arange(length, dtype=jnp.int32)
    row_seg = lax.dynamic_slice_in_dim(segment_ids, ctx * length, length, 1)
    first = jnp.sum((segment_ids[:, None, :] < row_seg[:, :, None]).astype(jnp.int32), -1)
    position = index[None, :] - first
    live = row_seg != 0
    valid = jnp.broadcast_to(live.astype(f32)[:, :, None], (seqs, length, 128))
    window = (back + 1) * length
    start = jnp.where(live, jnp.maximum(first - (ctx - back) * length, 0), window + 1)
    lowest = jnp.min(start.reshape(seqs, 2, rows), -1) // block
    frequency = rope_base ** (-(jnp.arange(size // 2, dtype=f32) * 2.0 / size))
    turned = position.astype(f32)[:, :, None] * frequency
    cosine, sine = jnp.cos(turned), jnp.sin(turned)
    cos = jnp.concatenate([cosine, cosine], -1)
    sin = jnp.concatenate([-sine, sine], -1)
    low_grad = jnp.where(live[:, :, None], reorder(out_grad), jnp.zeros((), bf16))
    start = start[:, None, :]

    def scalars(s):
        return jnp.concatenate([jnp.stack([fs, core]).astype(jnp.int32), lowest[s]])

    ids = [scalars(s) for s in range(seqs)]
    cfg = (heads, kv_heads, size, np_, back, block, scale2)
    cfg_forward = (heads, kv_heads, size, block, scale2)

    def tiled(width):
        return pl.BlockSpec((rows, width), lambda i, *_: (i, 0))

    def tiled_t(height):
        return pl.BlockSpec((height, rows), lambda i, *_: (0, i))

    def of(s, width, tile=rows):
        return pl.BlockSpec((None, tile, width), lambda i, *_: (s, i, 0))

    def all_of(s, width):
        return pl.BlockSpec((None, length, width), lambda *_: (s, 0, 0))

    def lanes(s):
        return pl.BlockSpec((None, 1, rows), lambda i, *_: (s, 0, i))

    def shape(*dims, dtype=bf16):
        return jax.ShapeDtypeStruct(dims, dtype)

    half_pair = [(shape(rows, model), whole((rows, model)))] * 2

    line = Line()
    up_perm = [(i, i + 1) for i in range(n_ctx - 1)]
    down_perm = [(i + 1, i) for i in range(n_ctx - 1)]
    kv_shape = (length, 2 * kv_width)
    sums = 8 * -(-heads // 8)

    def kernel(name, body_, grid, ins, outs, scratch, s, *args, aliases=None):
        return line(
            functools.partial(call, body_, name, grid, ins, outs, scratch, 0, 0, ids[s], aliases=aliases), *args
        )

    normed, own_kv, pre_k, queries, pre_q = [], [], [], [], []

    def keys(s):
        n, k, p = kernel(
            "keys", functools.partial(kv_kernel, kv_heads, size, np_), (2,),
            [of(s, model), whole((1, model)), of(s, size), of(s, size), whole((1, size))]
            + [whole(w.shape) for w in kv_w],
            [
                (shape(length, model), tiled(model)),
                (shape(*kv_shape), tiled(2 * kv_width)),
                (shape(length, kv_width, dtype=f32), tiled(kv_width)),
            ],
            [], s, tokens, gain_one, cos, sin, kg, *kv_w,
        )
        normed.append(n)
        own_kv.append(k)
        pre_k.append(p)

    def query(s):
        q, p = kernel(
            "query", functools.partial(query_kernel, heads, size, np_), (2,),
            [tiled(model), of(s, size), of(s, size), whole((1, size))] + [whole(w.shape) for w in query_w],
            [
                (shape(length, q_width), tiled(q_width)),
                (shape(length, q_width, dtype=f32), tiled(q_width)),
            ],
            [], s, normed[s], cos, sin, qg, *query_w,
        )
        queries.append(q)
        pre_q.append(p)

    kv = []

    def spread(s):
        chunks = [line.after(own_kv[s])]
        chunks.insert(0, lax.ppermute(chunks[0], "ctx", up_perm))
        kv.append(chunks)

    def forward(s):
        for _ in range(back - 1):
            kv[s].insert(0, lax.ppermute(line.after(kv[s][0]), "ctx", up_perm))

    sums_own, mixed, lse, branch = [], [], [], []

    def attend_own(s):
        sums_own.append(
            kernel(
                "attend_own", functools.partial(attend_own_kernel, cfg_forward, back), (2,),
                [tiled(q_width), lanes(s), whole(kv_shape)],
                [
                    (shape(q_width, length, dtype=f32), tiled_t(q_width)),
                    (shape(sums, length, dtype=f32), tiled_t(sums)),
                ],
                [], s, queries[s], start, own_kv[s],
            )
        )

    def attend(s):
        own, oth, m, l = kernel(
            "attend", functools.partial(attend_kernel, cfg_forward, np_, back), (2,),
            [tiled(q_width), lanes(s), tiled_t(q_width), tiled_t(sums)]
            + [whole(kv_shape)] * back + [whole(w.shape) for w in out_w],
            half_pair
            + [
                (shape(q_width, length), tiled_t(q_width)),
                (shape(sums, length, dtype=f32), tiled_t(sums)),
            ],
            [
                pltpu.VMEM((back * length, 2 * kv_width), bf16),
                pltpu.VMEM((q_width, rows), f32),
                pltpu.VMEM((sums, rows), f32),
            ],
            s, queries[s], start, *sums_own[s], *kv[s][:back], *out_w,
        )
        mixed.append(m)
        lse.append(l)
        branch.append(Steps(sum_tp(line, own, oth, n_tp)))

    tile = 256
    steps = hidden // tile
    normed_two, active, grad_gate, grad_up, grad_two, ffn_gains = [], [], [], [], [], []

    def ffn(s):
        col = pl.BlockSpec((length, tile), lambda i, *_: (0, i))
        w_in = [pl.BlockSpec((w.shape[0], tile), lambda i, *_: (0, i)) for w in gate_w]
        w_dn = [pl.BlockSpec((tile, w.shape[1]), lambda i, *_: (i, 0)) for w in down_w]
        n2, act, gg, gu, own, oth, fg = kernel(
            "ffn", functools.partial(ffn_kernel, np_), (steps,),
            [all_of(s, model), whole((rows, model)), whole((rows, model)), all_of(s, 128),
             whole((1, model)), all_of(s, model)] + w_in + w_in + w_dn,
            [
                (shape(length, model), whole((length, model))),
                (shape(length, hidden), col),
                (shape(length, hidden), col),
                (shape(length, hidden), col),
            ]
            + half_pair
            + [(shape(1, model, dtype=f32), whole((1, model)))],
            [pltpu.VMEM((length, model), f32), pltpu.VMEM((length, model), f32)],
            s, tokens, *branch[s].value, valid, gain_two, low_grad, *gate_w, *up_w, *down_w,
        )
        normed_two.append(n2)
        active.append(act)
        grad_gate.append(gg)
        grad_up.append(gu)
        grad_two.append(Steps(sum_tp(line, own, oth, n_tp)))
        ffn_gains.append(fg)

    both_pair = [
        (shape(seqs * rows, model), lambda s: pl.BlockSpec((rows, model), lambda *_: (s, 0))),
    ] * 2

    def pair_of(s):
        return [(one, spec(s)) for one, spec in both_pair]

    layers = []

    def down(s):
        first = 2 + len(down_w)
        into = list(layers)
        layers[:] = kernel(
            "down", functools.partial(down_kernel, np_), (2,),
            [tiled(hidden)] + [whole((hidden, w.shape[1])) for w in down_w] + [pl.BlockSpec(memory_space=pl.ANY)] * len(into),
            pair_of(s), [], s, active[s], *down_w, *into,
            aliases={first: 0, first + 1: 1} if into else None,
        )
        if s == seqs - 1:
            layers[:] = [Steps(sum_tp(line, *layers, n_tp))]

    fine = 1
    small_rows = rows // fine

    def halves(s):
        return [pl.BlockSpec((small_rows, model), lambda i, *_: (s * fine + i % fine, 0))] * 2

    finished = {}

    def output(name, body_, s, ins, dtype, *args):
        extra = [finished[name]] if name in finished else []
        finished[name] = kernel(
            name, functools.partial(body_, np_, fine), (2 * fine,),
            [of(s, model, small_rows)] + ins + [pl.BlockSpec(memory_space=pl.ANY)] * len(extra),
            [(shape(seqs, length, model, dtype=dtype), of(s, model, small_rows))],
            [], s, tokens, *args, *extra,
            aliases={2 + len(ins): 0} if extra else None,
        )[0]

    def layer_output(s):
        output(
            "layer_out", layer_kernel, s, halves(0) + halves(s) + [of(s, 128, small_rows)], bf16,
            *branch[s].value, *layers[0].value, valid,
        )

    resid_grad, grad_branch, grad_query, near, q_gains, came = [], [], [], [], [], []

    def bring(far):
        moving = None
        for one in far:
            one = line.after(one) if moving is None else line(plus, one, moving)
            moving = lax.ppermute(one, "ctx", down_perm)
            yield moving

    def attend_back(s):
        far_shapes = [(shape(*kv_shape), whole(kv_shape))] * back
        rg, gb, gq, qgain, *far, dkv = kernel(
            "attend_back", functools.partial(attend_back_kernel, cfg), (2,),
            [of(s, model)] + [whole((rows, model))] * 4 + [of(s, 128), whole((1, model)), of(s, model),
             tiled_t(q_width), tiled_t(sums), tiled(q_width), lanes(s),
             tiled(q_width), of(s, size), of(s, size), whole((1, size))]
            + [whole(kv_shape)] * (back + 1)
            + [whole(w.shape) for w in out_w],
            [
                (shape(length, model, dtype=f32), tiled(model)),
                (shape(length, model), tiled(model)),
                (shape(length, q_width), tiled(q_width)),
                (shape(1, size, dtype=f32), whole((1, size))),
            ]
            + far_shapes
            + [(shape(*kv_shape, dtype=f32), whole(kv_shape))],
            [
                pltpu.VMEM((window, 2 * kv_width), bf16),
                pltpu.VMEM((window, 2 * kv_width), f32),
                pltpu.VMEM((q_width, rows), f32),
                pltpu.VMEM((q_width, rows), bf16),
            ],
            s, tokens, *branch[s].value, *grad_two[s].value, valid, gain_two, out_grad, mixed[s], lse[s], queries[s],
            start, pre_q[s], cos, sin, qg, *kv[s], *out_w,
        )
        came.append(Steps(bring(far)))
        resid_grad.append(rg)
        grad_branch.append(gb)
        grad_query.append(gq)
        q_gains.append(qgain)
        near.append(dkv)

    grad_kv, k_gains, a_gains, grad_one = [], [], [], []
    qkv_w = query_w + kv_w

    def input_back(s):
        into = list(grad_one)
        first = 11 + len(qkv_w)
        gkv, own, oth, kgain, again = kernel(
            "input_back", functools.partial(input_back_kernel, (heads, kv_heads, size, np_)), (2,),
            [of(s, model), whole((1, model)), tiled(q_width), tiled(2 * kv_width), tiled(2 * kv_width),
             tiled(kv_width), of(s, size), of(s, size), whole((1, size))]
            + [whole(w.shape) for w in qkv_w] + [pl.BlockSpec(memory_space=pl.ANY)] * len(into),
            [(shape(*kv_shape), tiled(2 * kv_width))]
            + pair_of(s)
            + [(shape(1, size, dtype=f32), whole((1, size))), (shape(1, model, dtype=f32), whole((1, model)))],
            [], s, tokens, gain_one, grad_query[s], near[s], came[s].value, pre_k[s], cos, sin, kg, *qkv_w, *into,
            aliases={first - 1: 1, first: 2} if into else None,
        )
        grad_kv.append(gkv)
        k_gains.append(kgain)
        a_gains.append(again)
        grad_one[:] = [own, oth]
        if s == seqs - 1:
            grad_one[:] = [Steps(sum_tp(line, own, oth, n_tp))]

    def input_output(s):
        output(
            "input_grad", input_kernel, s, [pl.BlockSpec((small_rows, model), lambda i, *_: (i, 0))]
            + halves(s) + [whole((1, model))], f32,
            resid_grad[s], *grad_one[0].value, gain_one,
        )

    rows_split, cols_split = (0, 1) if paired else (None, None)

    def reduced(parts, axis):
        if paired:
            total = line(plus, parts[0], swap(parts[1], "fsdp", 1, 2))
        else:
            total = lax.psum_scatter(parts[0], "fsdp", scatter_dimension=axis, tiled=True)
        yield total
        yield from sum_line(line, total, "ctx", n_ctx)

    def weight(name, lefts, rights, split, left_t=False, **place_):
        def run(lefts, rights, place_):
            return product(name, ids[0], lefts, rights, split, 256, left_t, **place_)

        if not paired:
            place_ = {}
        numbers = {k: v for k, v in place_.items() if k in ("at", "height")}
        arrays = {k: v for k, v in place_.items() if k not in numbers and v is not None}
        return line(lambda l, r, x: run(l, r, {**numbers, **x}), list(lefts), [list(r) for r in rights], arrays)

    gain_width = 2 * kv_width
    gain_rows = 16 * -(-(2 * part + 2 * small) // (16 * gain_width))

    def gain_sum():
        values = jnp.concatenate([sum(a_gains), sum(ffn_gains), sum(q_gains), sum(k_gains)], 1)
        bit = 1
        while bit < n_tp:
            values = line(jnp.add, values, swap(values, "tp", bit, n_tp))
            bit *= 2
            yield values
        yield values

    def gain_parts(values):
        def one(own):
            pieces = [values[:, (0 if own else part) :][:, :part], values[:, model + (0 if own else part) :][:, :part]]
            for at in (2 * model, 2 * model + size):
                low, high = values[:, at : at + small], values[:, at + small : at + size]
                pieces.append(jnp.where((fs == 0) == own, low, high))
            row = jnp.concatenate(pieces, 1)
            row = jnp.pad(row, ((0, 0), (0, gain_rows * gain_width - row.shape[1])))
            return row.reshape(gain_rows, gain_width).astype(bf16)

        return [one(True), one(False)]

    sums_of, parts_of = {}, {}

    def make(name):
        if name == "gate_up":
            parts_of[name] = weight("gate_up_grad", normed_two, [grad_gate, grad_up], rows_split)
        elif name == "down":
            parts_of[name] = weight(
                "down_grad", active, [[low_grad[s] for s in range(seqs)]], cols_split, height=hidden + q_width
            )
        elif name == "out":
            parts_of[name] = weight(
                "out_grad", mixed, [grad_branch], cols_split, True,
                at=hidden // 256, height=hidden + q_width, into=parts_of["down"],
            )
        elif name == "query":
            parts_of[name] = weight("query_grad", normed, [grad_query], rows_split)
        else:
            parts_of[name] = weight(
                "kv_grad", normed, [grad_kv], rows_split, height=model // 2 + gain_rows, tail=gain_parts(sums_of["gains"].value) if paired else None,
            )

    def send(*names):
        axis = 1 if names[0] in ("down", "out") else 0
        if paired:
            sums_of[names[0]] = Steps(reduced(parts_of[names[-1]], axis))
        else:
            steps = [reduced(parts_of[n], axis) for n in names]
            sums_of[names[0]] = Steps(zip(*steps))

    keys(0)
    line.wait(query_w[-1])
    spread(0)
    keys(1)
    spread(1)
    forward(0)
    query(0)
    query(1)
    attend_own(0)
    attend_own(1)
    forward(1)
    line.wait(gate_w[-1])
    attend(0)
    line.wait(up_w[-1])
    branch[0]()
    attend(1)
    branch[0]()
    branch[1]()
    ffn(0)
    branch[1]()
    grad_two[0]()
    ffn(1)
    grad_two[0]()
    grad_two[1]()
    make("gate_up")
    send("gate_up")
    attend_back(0)
    grad_two[1]()
    came[0]()
    make("down")
    came[0]()
    attend_back(1)
    line.wait(came[0].value)
    came[1]()
    make("out")
    send("down", "out")
    came[1]()
    sums_of["gate_up"]()
    make("query")
    send("query")
    input_back(0)
    input_back(1)
    sums_of["down"]()
    sums_of["query"]()
    grad_one[0]()
    sums_of["gains"] = Steps(gain_sum())
    sums_of["gains"]()
    sums_of["gate_up"]()
    sums_of["gains"]()
    make("kv")
    send("kv")
    down(0)
    down(1)
    sums_of["kv"]()
    sums_of["down"]()
    grad_one[0]()
    layers[0]()
    input_output(0)
    sums_of["gate_up"]()
    input_output(1)
    sums_of["query"]()
    sums_of["kv"]()
    layers[0]()
    sums_of["down"]()
    layer_output(0)
    sums_of["query"]()
    sums_of["kv"]()
    layer_output(1)
    gate_up, down_out, query_sum, kv_total = (sums_of[name]() for name in ("gate_up", "down", "query", "kv"))
    if paired:
        gate_sum, up_sum = gate_up[:, :hidden], gate_up[:, hidden:]
        down_sum, out_sum = down_out[:hidden], down_out[hidden:]
        kv_total, gain_total = kv_total[: model // 2], kv_total[model // 2 :]
    else:
        gate_sum, up_sum = gate_up[0][:, :hidden], gate_up[0][:, hidden:]
        (down_sum, out_sum), (query_sum,), (kv_total,) = down_out, query_sum, kv_total
    if paired:
        mine_all = gain_total.reshape(1, -1)[0].astype(f32)
        gain_out = []
        at = 0
        for width in (part, part, small, small):
            gain_out.append(mine_all[at : at + width])
            at += width
    else:
        values = sums_of["gains"].value
        for axis, count in (("fsdp", n_fs), ("ctx", n_ctx)):
            values = sum_small(values, axis, count)
        gain_out = []
        for at, width in ((0, model), (model, model), (2 * model, size), (2 * model + size, size)):
            gain_out.append(lax.dynamic_slice_in_dim(values[0], at + fs * (width // n_fs), width // n_fs, 0))
    attn_out, ffn_out, query_out, key_out = gain_out

    return (
        finished["layer_out"],
        finished["input_grad"],
        attn_out,
        query_sum.astype(f32),
        kv_total[:, :kv_width].astype(f32),
        kv_total[:, kv_width:].astype(f32),
        query_out,
        key_out,
        out_sum.astype(f32),
        ffn_out,
        gate_sum.astype(f32),
        up_sum.astype(f32),
        down_sum.astype(f32),
    )


def solution(mesh):
    n_fs, n_ctx, n_tp = mesh.shape["fsdp"], mesh.shape["ctx"], mesh.shape["tp"]
    placed = (
        P("fsdp", "ctx", None),
        P("fsdp", None),
        P("fsdp"),
        P("fsdp", "tp"),
        P("fsdp", "tp"),
        P("fsdp", "tp"),
        P("fsdp"),
        P("fsdp"),
        P("tp", "fsdp"),
        P("fsdp"),
        P("fsdp", "tp"),
        P("fsdp", "tp"),
        P("tp", "fsdp"),
        P("fsdp", "ctx", None),
    )
    return jax.shard_map(
        functools.partial(body, n_fs, n_ctx, n_tp),
        mesh=mesh,
        in_specs=placed,
        out_specs=(
            P("fsdp", "ctx", None),
            P("fsdp", "ctx", None),
            P("fsdp"),
            P("fsdp", "tp"),
            P("fsdp", "tp"),
            P("fsdp", "tp"),
            P("fsdp"),
            P("fsdp"),
            P("tp", "fsdp"),
            P("fsdp"),
            P("fsdp", "tp"),
            P("fsdp", "tp"),
            P("tp", "fsdp"),
        ),
        check_vma=False,
    )
```

```python
import functools
import math

import jax
import jax.numpy as jnp
from jax import lax
from jax.experimental import pallas as pl
from jax.experimental.pallas import tpu as pltpu
from jax.sharding import PartitionSpec as P

epsilon = 1e-06
rope_base = 1000000.0
longest_segment = 1024
f32 = jnp.float32
bf16 = jnp.bfloat16

NN = (((1,), (0,)), ((), ()))
NT = (((1,), (1,)), ((), ()))
TN = (((0,), (0,)), ((), ()))


def dot(left, right, dims=NN):
    return lax.dot_general(left, right, dims, preferred_element_type=f32)


def inv_scale(values):
    return lax.rsqrt(jnp.mean(values * values, -1, keepdims=True) + epsilon)


def norm_back(values, scale, gain, grad):
    scaled = grad * gain
    return scale * scaled - values * (scale * scale * scale) * jnp.mean(
        scaled * values, -1, keepdims=True
    )


def rows_of(index, size):
    return pl.ds(pl.multiple_of(index * size, size), size)


def ordered(ref, fs, np_):
    if np_ == 1:
        return ref[...]
    half = ref.shape[-1] // 2
    first = ref[:, pl.ds(pl.multiple_of(fs * half, 128), half)]
    other = ref[:, pl.ds(pl.multiple_of((1 - fs) * half, 128), half)]
    return jnp.concatenate([first, other], 1)


def whole(shape):
    return pl.BlockSpec(shape, lambda *_: (0,) * len(shape))


def columns(parts):
    width = parts[0]
    return [(i * width, (i + 1) * width) for i in range(len(parts))]


def call(kernel, name, grid, ins, outs, scratch, scalars, *args, aliases=None, waits=()):
    skip = len(waits)

    def body_(ids, *refs):
        kernel(ids, *refs[skip:])

    return pl.pallas_call(
        body_,
        name=name,
        out_shape=[o[0] for o in outs],
        grid_spec=pltpu.PrefetchScalarGridSpec(
            num_scalar_prefetch=1,
            grid=grid,
            in_specs=[pl.BlockSpec(memory_space=pl.ANY)] * skip + ins,
            out_specs=[o[1] for o in outs],
            scratch_shapes=scratch,
        ),
        input_output_aliases={k + skip: v for k, v in (aliases or {}).items()},
        compiler_params=pltpu.CompilerParams(dimension_semantics=("arbitrary",) * len(grid)),
        cost_estimate=pl.CostEstimate(flops=1, bytes_accessed=1, transcendentals=0),
    )(scalars, *waits, *args)


def project(low, weights, np_):
    width = low.shape[1] // np_
    acc = None
    for i in range(np_):
        one = dot(low[:, i * width : (i + 1) * width], weights[i][...])
        acc = one if acc is None else acc + one
    return acc


def turn(acc, count, size, g, c, s, out):
    for h in range(count):
        u = acc[:, h * size : (h + 1) * size]
        u = u * inv_scale(u) * g
        out[:, h * size : (h + 1) * size] = (u * c + pltpu.roll(u, size // 2, 1) * s).astype(bf16)


def kv_kernel(kv_heads, size, np_, passed, ids, tok, gain, cos, sin, kg, *rest):
    weights, (normed, kv_out, pre_out) = rest[:np_], rest[np_ + passed : np_ + passed + 3]
    x = ordered(tok, ids[0], np_).astype(f32)
    low = (x * inv_scale(x) * gain[...]).astype(bf16)
    normed[...] = low
    acc = project(low, weights, np_)
    pre_out[...] = acc[:, : kv_heads * size]
    turn(acc, kv_heads, size, kg[...], cos[...], sin[...], kv_out)
    kv_out[:, kv_heads * size :] = acc[:, kv_heads * size :].astype(bf16)


def query_kernel(heads, size, np_, ids, normed, cos, sin, qg, *rest):
    weights, (q_out, pre_out) = rest[:np_], rest[np_:]
    acc = project(normed[...], weights, np_)
    pre_out[...] = acc
    turn(acc, heads, size, qg[...], cos[...], sin[...], q_out)


def allowed_block(key_base, start, row_base, block, rows):
    key_index = key_base + lax.broadcasted_iota(jnp.int32, (block, rows), 0)
    row_index = row_base + lax.broadcasted_iota(jnp.int32, (block, rows), 1)
    return (key_index >= start) & (key_index <= row_index)


def attend_blocks(cfg, low, high, base, kv, q, start_row, row_base, acc, total):
    heads, kv_heads, size, block, scale2 = cfg
    group = heads // kv_heads
    rows = q.shape[0]

    def step(kb, carry):
        at = pl.ds(pl.multiple_of((kb - base) * block, block), block)
        allow = allowed_block(kb * block, start_row, row_base, block, rows)
        for g in range(kv_heads):
            k = kv[at, g * size : (g + 1) * size]
            v = kv[at, (kv_heads + g) * size : (kv_heads + g + 1) * size]
            for h in range(g * group, (g + 1) * group):
                s = dot(k, q[:, h * size : (h + 1) * size], NT)
                e = jnp.where(allow, jnp.exp2(s * scale2), 0.0)
                total[h : h + 1, :] += jnp.sum(e, 0, keepdims=True)
                acc[h * size : (h + 1) * size, :] += dot(v, e.astype(bf16), TN)
        return carry

    lax.fori_loop(low, high, step, 0)


def attend_own_kernel(cfg, back, ids, q, start, kv, acc, total):
    t = pl.program_id(0)
    rows = q.shape[0]
    base = back * kv.shape[0]
    acc[...] = jnp.zeros_like(acc)
    total[...] = jnp.zeros_like(total)
    first = base // cfg[3]
    attend_blocks(
        cfg, jnp.maximum(ids[2 + t], first), (base + (t + 1) * rows) // cfg[3], first,
        kv, q, start[...], base + t * rows, acc, total,
    )


def attend_kernel(cfg, np_, back, out_at, ids, q, start, acc_in, total_in, *rest):
    heads, _, size, block, _ = cfg
    chunks = rest[:back]
    w_out = rest[back : back + np_]
    own, oth, mixed_out, lse_out, kv, acc, total = rest[back + np_ :]
    t = pl.program_id(0)
    core = ids[1]
    rows = q.shape[0]
    length = chunks[0].shape[0]

    @pl.when(t == 0)
    def _():
        for i in range(back):
            kv[i * length : (i + 1) * length, :] = chunks[i][...]

    acc[...] = acc_in[...]
    total[...] = total_in[...]
    attend_blocks(
        cfg, ids[2 + t], back * length // block, 0, kv, q, start[...], back * length + t * rows, acc, total
    )
    sums = total[...]
    sums = jnp.where(sums > 0.0, sums, 1.0)
    lse_out[...] = jnp.log2(sums)
    inverse = 1.0 / sums
    for h in range(heads):
        part = (acc[h * size : (h + 1) * size, :] * inverse[h : h + 1, :]).astype(bf16)
        mixed_out[h * size : (h + 1) * size, :] = part
    mixed = mixed_out[...]
    width = w_out[0].shape[1]
    for i in range(np_):
        part = dot(mixed, w_out[i][out_at:, :], TN).astype(bf16)

        @pl.when(t == core)
        def _():
            own[:, i * width : (i + 1) * width] = part

        @pl.when(t != core)
        def _():
            oth[:, i * width : (i + 1) * width] = part


def ffn_kernel(np_, ids, tok, b_own, b_oth, valid, gain, grad, *rest):
    gate_w, up_w, down_w = rest[:np_], rest[np_ : 2 * np_], rest[2 * np_ : 3 * np_]
    n2_out, act_out, gg_out, gu_out, own, oth, gain_out, hat, acc = rest[3 * np_ :]
    f = pl.program_id(0)
    core = ids[1]
    half = b_own.shape[0]

    @pl.when(f == 0)
    def _():
        for ref, tile in ((b_own, core), (b_oth, 1 - core)):
            at = rows_of(tile, half)
            tokens = ordered(tok.at[at], ids[0], np_).astype(f32)
            resid = tokens + valid[at, :1] * ref[...].astype(f32)
            normal = resid * inv_scale(resid)
            hat[at, :] = normal
            n2_out[at, :] = (normal * gain[...]).astype(bf16)
        acc[...] = jnp.zeros_like(acc)

    width = tok.shape[1] // np_
    parts = [(i * width, (i + 1) * width) for i in range(np_)]
    gate = up = active_grad = None
    for i, (a, b) in enumerate(parts):
        x = n2_out[:, a:b]
        g, u, d = dot(x, gate_w[i][...]), dot(x, up_w[i][...]), dot(grad[:, a:b], down_w[i][...], NT)
        gate, up, active_grad = (g, u, d) if i == 0 else (gate + g, up + u, active_grad + d)
    sigma = jax.nn.sigmoid(gate)
    silu = gate * sigma
    act_out[...] = (silu * up).astype(bf16)
    gg = (active_grad * up * sigma * (1.0 + gate * (1.0 - sigma))).astype(bf16)
    gu = (active_grad * silu).astype(bf16)
    gg_out[...] = gg
    gu_out[...] = gu
    for i, (a, b) in enumerate(parts):
        acc[:, a:b] += dot(gg, gate_w[i][...], NT) + dot(gu, up_w[i][...], NT)

    @pl.when(f == pl.num_programs(0) - 1)
    def _():
        own[...] = acc[rows_of(core, half), :].astype(bf16)
        oth[...] = acc[rows_of(1 - core, half), :].astype(bf16)
        gain_out[...] = jnp.sum(acc[...] * hat[...], 0, keepdims=True)


def down_kernel(np_, ids, act, *rest):
    weights, (own, oth) = rest[:np_], rest[-2:]
    t = pl.program_id(0)
    width = weights[0].shape[1]
    for i in range(np_):
        part = dot(act[...], weights[i][...]).astype(bf16)

        @pl.when(t == ids[1])
        def _():
            own[:, i * width : (i + 1) * width] = part

        @pl.when(t != ids[1])
        def _():
            oth[:, i * width : (i + 1) * width] = part


def picked(ids, own, oth, t):
    return jnp.where(ids[1] == t, own[...].astype(f32), oth[...].astype(f32))


def attend_back_kernel(cfg, out_at, ids, tok, b_own, b_oth, t_own, t_oth, valid, gain, grad, mixed, lse, q, start, pre, cos, sin, qg, *rest):
    heads, kv_heads, size, np_, back, block, scale2 = cfg
    chunks = rest[: back + 1]
    w_out = rest[back + 1 : back + 1 + np_]
    outs = rest[back + 1 + np_ :]
    resid_out, branch_out, gq_out, gain_out = outs[:4]
    far = outs[4 : 4 + back + 1]
    kv, dkv, dq, dout = outs[4 + back + 1 :]
    t = pl.program_id(0)
    rows = q.shape[0]
    length = chunks[0].shape[0]
    group = heads // kv_heads
    scale = size**-0.5

    @pl.when(t == 0)
    def _():
        for i in range(back + 1):
            kv[i * length : (i + 1) * length, :] = chunks[i][...]
        dkv[...] = jnp.zeros_like(dkv)
        gain_out[...] = jnp.zeros_like(gain_out)

    resid = ordered(tok, ids[0], np_).astype(f32) + valid[:, :1] * picked(ids, b_own, b_oth, t)
    resid_grad = ordered(grad, ids[0], np_).astype(f32) + norm_back(
        resid, inv_scale(resid), gain[...], picked(ids, t_own, t_oth, t)
    )
    resid_out[...] = resid_grad
    low = (valid[:, :1] * resid_grad).astype(bf16)
    branch_out[...] = low
    width = low.shape[1] // np_
    mixed_grad = dot(w_out[0][out_at:, :], low[:, :width], NT)
    for i in range(1, np_):
        mixed_grad = mixed_grad + dot(w_out[i][out_at:, :], low[:, i * width : (i + 1) * width], NT)
    dout[...] = mixed_grad.astype(bf16)
    delta = [
        jnp.sum(
            dout[h * size : (h + 1) * size, :].astype(f32) * mixed[h * size : (h + 1) * size, :].astype(f32),
            0,
            keepdims=True,
        )
        for h in range(heads)
    ]
    dq[...] = jnp.zeros_like(dq)
    row_base = back * length + t * rows
    start_row = start[...]

    def step(kb, carry):
        at = pl.ds(pl.multiple_of(kb * block, block), block)
        allow = allowed_block(kb * block, start_row, row_base, block, rows)
        for g in range(kv_heads):
            k = kv[at, g * size : (g + 1) * size]
            v = kv[at, (kv_heads + g) * size : (kv_heads + g + 1) * size]
            dk = dv = None
            for h in range(g * group, (g + 1) * group):
                qh = q[:, h * size : (h + 1) * size]
                do = dout[h * size : (h + 1) * size, :]
                s = dot(k, qh, NT)
                p = jnp.where(allow, jnp.exp2(s * scale2 - lse[h : h + 1, :]), 0.0)
                dp = dot(v, do)
                ds = (p * (dp - delta[h])).astype(bf16)
                one_v = dot(p.astype(bf16), do, NT)
                one_k = dot(ds, qh)
                dk, dv = (one_k, one_v) if dk is None else (dk + one_k, dv + one_v)
                dq[h * size : (h + 1) * size, :] += dot(k, ds, TN)
            dkv[at, g * size : (g + 1) * size] += dk * scale
            dkv[at, (kv_heads + g) * size : (kv_heads + g + 1) * size] += dv
        return carry

    lax.fori_loop(ids[2 + t], (row_base + rows) // block, step, 0)
    c, s_ = cos[...], sin[...]
    for h in range(heads):
        u = dq[h * size : (h + 1) * size, :].T * scale
        u = u * c - pltpu.roll(u, size // 2, 1) * s_
        v = pre[:, h * size : (h + 1) * size]
        r = inv_scale(v)
        gain_out[...] += jnp.sum(u * (v * r), 0, keepdims=True)
        gq_out[:, h * size : (h + 1) * size] = norm_back(v, r, qg[...], u).astype(bf16)

    @pl.when(t == pl.num_programs(0) - 1)
    def _():
        for i in range(back + 1):
            far[i][...] = dkv[i * length : (i + 1) * length, :].astype(far[i].dtype)


def input_back_kernel(cfg, ids, tok, gain, gq, near, came, pre, cos, sin, kg, *rest):
    heads, kv_heads, size, np_ = cfg
    weights = rest[: 2 * np_]
    gkv_out, own, oth, k_gain, a_gain = rest[-5:]
    t = pl.program_id(0)
    core = ids[1]

    @pl.when(t == 0)
    def _():
        k_gain[...] = jnp.zeros_like(k_gain)
        a_gain[...] = jnp.zeros_like(a_gain)

    dkv = near[...] + came[...].astype(f32)
    c, s_ = cos[...], sin[...]
    for h in range(kv_heads):
        u = dkv[:, h * size : (h + 1) * size]
        u = u * c - pltpu.roll(u, size // 2, 1) * s_
        v = pre[:, h * size : (h + 1) * size]
        r = inv_scale(v)
        k_gain[...] += jnp.sum(u * (v * r), 0, keepdims=True)
        gkv_out[:, h * size : (h + 1) * size] = norm_back(v, r, kg[...], u).astype(bf16)
    gkv_out[:, kv_heads * size :] = dkv[:, kv_heads * size :].astype(bf16)
    x = ordered(tok, ids[0], np_).astype(f32)
    normal = x * inv_scale(x)
    width = x.shape[1] // np_
    for i in range(np_):
        at = slice(i * width, (i + 1) * width)
        part = dot(gq[...], weights[i][...], NT)
        part = part + dot(gkv_out[...], weights[np_ + i][...], NT)
        a_gain[:, at] += jnp.sum(part * normal[:, at], 0, keepdims=True)
        low = part.astype(bf16)

        @pl.when(t == core)
        def _():
            own[:, at] = low

        @pl.when(t != core)
        def _():
            oth[:, at] = low


def place(out, values, fs, np_):
    width = values.shape[1] // np_
    if np_ == 1:
        out[...] = values
        return
    for i in range(2):
        at = pl.ds(pl.multiple_of((fs if i == 0 else 1 - fs) * width, 128), width)
        out[:, at] = values[:, i * width : (i + 1) * width]


def layer_kernel(np_, fine, ids, tok, b_own, b_oth, f_own, f_oth, valid, *rest):
    out = rest[-1]
    t = pl.program_id(0) // fine
    v = valid[:, :1]
    resid = ordered(tok, ids[0], np_).astype(f32) + v * picked(ids, b_own, b_oth, t)
    place(out, (resid + v * picked(ids, f_own, f_oth, t)).astype(bf16), ids[0], np_)


def input_kernel(np_, fine, ids, tok, resid_grad, g_own, g_oth, gain, *rest):
    out = rest[-1]
    t = pl.program_id(0) // fine
    x = ordered(tok, ids[0], np_).astype(f32)
    grad = resid_grad[...] + norm_back(x, inv_scale(x), gain[...], picked(ids, g_own, g_oth, t))
    place(out, grad, ids[0], np_)


def product_kernel(pairs, groups, tiles, split, left_t, tail, ids, *rest):
    count = 1 if split is None else 2
    outs = rest[-count:]
    m = pl.program_id(0)

    def low():
        columns = []
        for j in range(groups):
            total = None
            for i in range(pairs):
                one = dot(rest[i][...], rest[pairs * (1 + j) + i][...], NN if left_t else TN)
                total = one if total is None else total + one
            columns.append(total.astype(bf16))
        return columns[0] if groups == 1 else jnp.concatenate(columns, 1)

    if split is None:
        outs[0][...] = low()
    elif split == 1:
        value = low()
        width = value.shape[1] // 2
        outs[0][...] = value[:, :width]
        outs[1][...] = value[:, width:]
    else:

        @pl.when(m < tiles // 2)
        def _():
            outs[0][...] = low()

        @pl.when((m >= tiles // 2) & (m < tiles))
        def _():
            outs[1][...] = low()

    if tail:

        @pl.when(m == tiles)
        def _():
            at = pairs * (1 + groups)
            for i in range(2):
                outs[i][: rest[at + i].shape[0], :] = rest[at + i][...]


def product(name, ids, lefts, rights, split, tile, left_t=False, at=0, height=None, into=None, tail=None, waits=()):
    pairs, groups = len(lefts), len(rights)
    m = lefts[0].shape[0 if left_t else 1]
    k = lefts[0].shape[1 if left_t else 0]
    n = sum(r[0].shape[1] for r in rights)
    tiles = m // tile
    ins, args = [], []
    for left in lefts:
        if left_t:
            ins.append(pl.BlockSpec((tile, k), lambda i, *_: (jnp.minimum(i, tiles - 1), 0)))
        else:
            ins.append(pl.BlockSpec((k, tile), lambda i, *_: (0, jnp.minimum(i, tiles - 1))))
        args.append(left)
    for group in rights:
        for right in group:
            ins.append(whole(right.shape))
            args.append(right)
    if split is None:
        shape = jax.ShapeDtypeStruct((height or m, n), bf16)
        outs = [(shape, pl.BlockSpec((tile, n), lambda i, *_: (i + at, 0)))]
    elif split == 1:
        shape = jax.ShapeDtypeStruct((height or m, n // 2), bf16)
        outs = [(shape, pl.BlockSpec((tile, n // 2), lambda i, *_: (i + at, 0)))] * 2
    else:
        half = tiles // 2
        shape = jax.ShapeDtypeStruct((height or m // 2, n), bf16)
        last = at + half if tail is not None else at + half - 1

        def own(i, *_):
            return (jnp.where(i < half, i + at, jnp.where(i < tiles, half - 1 + at, last)), 0)

        def other(i, *_):
            return (jnp.where(i < tiles, jnp.maximum(i - half, 0) + at, last), 0)

        outs = [(shape, pl.BlockSpec((tile, n), own)), (shape, pl.BlockSpec((tile, n), other))]
    if tail is not None:
        ins += [whole(v.shape) for v in tail]
        args += list(tail)
    aliases = None
    if into is not None:
        aliases = {1 + len(ins) + i: i for i in range(len(into))}
        ins += [pl.BlockSpec(memory_space=pl.ANY)] * len(into)
        args += list(into)
    return call(
        functools.partial(product_kernel, pairs, groups, tiles, split, left_t, tail is not None),
        name, (tiles + (tail is not None),), ins, outs, [], ids, *args, aliases=aliases, waits=waits,
    )


def swap(values, axis, bit, size):
    return lax.ppermute(values, axis, [(i, i ^ bit) for i in range(size)])


def plus(a, b):
    return a + b


class Line:
    def __init__(self):
        self.last = None
        self.waited = ()

    def __call__(self, fn, *args):
        if self.last is not None:
            args, _ = lax.optimization_barrier((args, self.last))
        outs = fn(*args)
        self.last = jax.tree.leaves(outs)[0]
        return outs

    def wait(self, *values):
        self.waited += values

    def take(self):
        values, self.waited = self.waited, ()
        return values

    def after(self, value):
        return lax.optimization_barrier((value, self.last, self.waited))[0]


class Steps:
    def __init__(self, steps):
        self.steps, self.value = steps, None

    def __call__(self, count=1):
        for _ in range(count):
            self.value = next(self.steps)
        return self.value


def sum_tp(line, own, oth, size):
    total = line(plus, own, swap(line.after(oth), "tp", 1, size))
    yield total
    bit = 2
    while bit < size:
        total = line(plus, total, swap(total, "tp", bit, size))
        bit *= 2
        if bit < size:
            yield total
    yield total, swap(total, "tp", 1, size)


def sum_line(line, total, axis, size):
    index = lax.axis_index(axis)
    middle = size // 2
    for i in range(middle - 1):
        came = lax.ppermute(total, axis, [(i, i + 1), (size - 1 - i, size - 2 - i)])
        total = line(plus, total, came)
        yield total
    total = line(plus, total, lax.ppermute(total, axis, [(middle - 1, middle), (middle, middle - 1)]))
    yield total
    for i in reversed(range(middle - 1)):
        came = lax.ppermute(total, axis, [(i + 1, i), (size - 2 - i, size - 1 - i)])
        total = jnp.where((index == i) | (index == size - 1 - i), came, total)
    yield total


def sum_small(values, axis, size):
    bit = 1
    while bit < size:
        values = values + swap(values, axis, bit, size)
        bit *= 2
    return values


def body(
    n_fs, n_ctx, n_tp,
    tokens, segment_ids, attn_gain, w_query, w_key, w_value, query_gain, key_gain,
    w_out, ffn_gain, w_gate, w_up, w_down, out_grad,
):
    seqs, length, model = tokens.shape
    paired = n_fs == 2
    np_ = 2 if paired else 1
    fs = lax.axis_index("fsdp")
    ctx = lax.axis_index("ctx")
    core = lax.axis_index("tp") % 2
    size = query_gain.shape[0] * n_fs
    heads = w_query.shape[1] // size
    kv_heads = w_key.shape[1] // size
    hidden = w_gate.shape[1]
    q_width, kv_width = heads * size, kv_heads * size
    rows = length // 2
    block = rows
    back = min(n_ctx - 1, -(-(longest_segment - 1) // length))
    scale2 = size**-0.5 * math.log2(math.e)

    def gather(weight, axis):
        if paired:
            return [weight, swap(weight, "fsdp", 1, 2)]
        return [lax.all_gather(weight, "fsdp", axis=axis, tiled=True)]

    kv_w = gather(jnp.concatenate([w_key, w_value], 1), 0)
    query_w = gather(w_query, 0)
    gate_w = gather(w_gate, 0)
    up_w = gather(w_up, 0)
    down_out = [jnp.concatenate([w_down, w_out], 0)] if paired else []
    out_at = hidden if paired else 0

    part, small = attn_gain.shape[0], query_gain.shape[0]
    padding = part - 2 * small
    gains = jnp.concatenate([query_gain, key_gain] + ([jnp.zeros((padding,), bf16)] if padding > 0 else []))
    gains = jnp.stack([attn_gain, ffn_gain, gains[:part]]) if padding >= 0 else None
    if paired:
        gains, kv_w[0] = lax.optimization_barrier((gains, kv_w[0]))
    both = [gains, swap(gains, "fsdp", 1, 2)] if paired else None
    if paired:
        wide = jnp.concatenate(both, 1).astype(f32)
        gain_one, gain_two = wide[:1], wide[1:2]

    def natural(first, values):
        if not paired:
            return lax.all_gather(values, "fsdp", axis=0, tiled=True)[None, :].astype(f32)
        own_first = jnp.concatenate([b[2:, first : first + small] for b in both], 1)
        return jnp.where(fs == 0, own_first, jnp.roll(own_first, small, 1)).astype(f32)

    if not paired:
        gain_one, gain_two = natural(0, attn_gain), natural(0, ffn_gain)
    qg, kg = natural(0, query_gain), natural(small, key_gain)

    def reorder(values):
        if not paired:
            return values
        half = model // 2
        return jnp.where(fs == 0, values, jnp.concatenate([values[..., half:], values[..., :half]], -1))

    index = ctx * length + jnp.arange(length, dtype=jnp.int32)
    row_seg = lax.dynamic_slice_in_dim(segment_ids, ctx * length, length, 1)
    first = jnp.sum((segment_ids[:, None, :] < row_seg[:, :, None]).astype(jnp.int32), -1)
    position = index[None, :] - first
    live = row_seg != 0
    valid = jnp.broadcast_to(live.astype(f32)[:, :, None], (seqs, length, 128))
    window = (back + 1) * length
    start = jnp.where(live, jnp.maximum(first - (ctx - back) * length, 0), window + 1)
    lowest = jnp.min(start.reshape(seqs, 2, rows), -1) // block
    frequency = rope_base ** (-(jnp.arange(size // 2, dtype=f32) * 2.0 / size))
    turned = position.astype(f32)[:, :, None] * frequency
    cosine, sine = jnp.cos(turned), jnp.sin(turned)
    cos = jnp.concatenate([cosine, cosine], -1)
    sin = jnp.concatenate([-sine, sine], -1)
    low_grad = jnp.where(live[:, :, None], reorder(out_grad), jnp.zeros((), bf16))
    start = start[:, None, :]

    def scalars(s):
        return jnp.concatenate([jnp.stack([fs, core]).astype(jnp.int32), lowest[s]])

    ids = [scalars(s) for s in range(seqs)]
    cfg = (heads, kv_heads, size, np_, back, block, scale2)
    cfg_forward = (heads, kv_heads, size, block, scale2)

    def tiled(width):
        return pl.BlockSpec((rows, width), lambda i, *_: (i, 0))

    def tiled_t(height):
        return pl.BlockSpec((height, rows), lambda i, *_: (0, i))

    def of(s, width, tile=rows):
        return pl.BlockSpec((None, tile, width), lambda i, *_: (s, i, 0))

    def all_of(s, width):
        return pl.BlockSpec((None, length, width), lambda *_: (s, 0, 0))

    def lanes(s):
        return pl.BlockSpec((None, 1, rows), lambda i, *_: (s, 0, i))

    def shape(*dims, dtype=bf16):
        return jax.ShapeDtypeStruct(dims, dtype)

    half_pair = [(shape(rows, model), whole((rows, model)))] * 2

    line = Line()
    up_perm = [(i, i + 1) for i in range(n_ctx - 1)]
    down_perm = [(i + 1, i) for i in range(n_ctx - 1)]
    kv_shape = (length, 2 * kv_width)
    sums = 8 * -(-heads // 8)

    def kernel(name, body_, grid, ins, outs, scratch, s, *args, aliases=None):
        count = len(args)

        def run(*all_args):
            return call(
                body_, name, grid, ins, outs, scratch, ids[s], *all_args[:count],
                aliases=aliases, waits=all_args[count:],
            )

        return line(run, *args, *line.take())

    normed, own_kv, pre_k, queries, pre_q = [], [], [], [], []

    def keys(s, through=()):
        first = 6 + len(kv_w)
        n, k, p, *through = kernel(
            "keys", functools.partial(kv_kernel, kv_heads, size, np_, len(through)), (2,),
            [of(s, model), whole((1, model)), of(s, size), of(s, size), whole((1, size))]
            + [whole(w.shape) for w in kv_w] + [pl.BlockSpec(memory_space=pl.ANY)] * len(through),
            [
                (shape(length, model), tiled(model)),
                (shape(*kv_shape), tiled(2 * kv_width)),
                (shape(length, kv_width, dtype=f32), tiled(kv_width)),
            ]
            + [(shape(*v.shape), pl.BlockSpec(memory_space=pl.ANY)) for v in through],
            [], s, tokens, gain_one, cos, sin, kg, *kv_w, *through,
            aliases={first + i: 3 + i for i in range(len(through))},
        )
        normed.append(n)
        own_kv.append(k)
        pre_k.append(p)
        return through

    def query(s):
        q, p = kernel(
            "query", functools.partial(query_kernel, heads, size, np_), (2,),
            [tiled(model), of(s, size), of(s, size), whole((1, size))] + [whole(w.shape) for w in query_w],
            [
                (shape(length, q_width), tiled(q_width)),
                (shape(length, q_width, dtype=f32), tiled(q_width)),
            ],
            [], s, normed[s], cos, sin, qg, *query_w,
        )
        queries.append(q)
        pre_q.append(p)

    kv = []

    def spread(s):
        chunks = [line.after(own_kv[s])]
        chunks.insert(0, lax.ppermute(chunks[0], "ctx", up_perm))
        kv.append(chunks)

    def forward(s):
        for _ in range(back - 1):
            kv[s].insert(0, lax.ppermute(line.after(kv[s][0]), "ctx", up_perm))

    sums_own, mixed, lse, branch = [], [], [], []

    def attend_own(s):
        sums_own.append(
            kernel(
                "attend_own", functools.partial(attend_own_kernel, cfg_forward, back), (2,),
                [tiled(q_width), lanes(s), whole(kv_shape)],
                [
                    (shape(q_width, length, dtype=f32), tiled_t(q_width)),
                    (shape(sums, length, dtype=f32), tiled_t(sums)),
                ],
                [], s, queries[s], start, own_kv[s],
            )
        )

    def attend(s):
        own, oth, m, l = kernel(
            "attend", functools.partial(attend_kernel, cfg_forward, np_, back, out_at), (2,),
            [tiled(q_width), lanes(s), tiled_t(q_width), tiled_t(sums)]
            + [whole(kv_shape)] * back + [whole(w.shape) for w in out_w],
            half_pair
            + [
                (shape(q_width, length), tiled_t(q_width)),
                (shape(sums, length, dtype=f32), tiled_t(sums)),
            ],
            [
                pltpu.VMEM((back * length, 2 * kv_width), bf16),
                pltpu.VMEM((q_width, rows), f32),
                pltpu.VMEM((sums, rows), f32),
            ],
            s, queries[s], start, *sums_own[s], *kv[s][:back], *out_w,
        )
        mixed.append(m)
        lse.append(l)
        branch.append(Steps(sum_tp(line, own, oth, n_tp)))

    tile = 256
    steps = hidden // tile
    normed_two, active, grad_gate, grad_up, grad_two, ffn_gains = [], [], [], [], [], []

    def ffn(s):
        col = pl.BlockSpec((length, tile), lambda i, *_: (0, i))
        w_in = [pl.BlockSpec((w.shape[0], tile), lambda i, *_: (0, i)) for w in gate_w]
        w_dn = [pl.BlockSpec((tile, w.shape[1]), lambda i, *_: (i, 0)) for w in down_w]
        n2, act, gg, gu, own, oth, fg = kernel(
            "ffn", functools.partial(ffn_kernel, np_), (steps,),
            [all_of(s, model), whole((rows, model)), whole((rows, model)), all_of(s, 128),
             whole((1, model)), all_of(s, model)] + w_in + w_in + w_dn,
            [
                (shape(length, model), whole((length, model))),
                (shape(length, hidden), col),
                (shape(length, hidden), col),
                (shape(length, hidden), col),
            ]
            + half_pair
            + [(shape(1, model, dtype=f32), whole((1, model)))],
            [pltpu.VMEM((length, model), f32), pltpu.VMEM((length, model), f32)],
            s, tokens, *branch[s].value, valid, gain_two, low_grad, *gate_w, *up_w, *down_w,
        )
        normed_two.append(n2)
        active.append(act)
        grad_gate.append(gg)
        grad_up.append(gu)
        grad_two.append(Steps(sum_tp(line, own, oth, n_tp)))
        ffn_gains.append(fg)

    both_pair = [
        (shape(seqs * rows, model), lambda s: pl.BlockSpec((rows, model), lambda *_: (s, 0))),
    ] * 2

    def pair_of(s):
        return [(one, spec(s)) for one, spec in both_pair]

    layers = []

    def down(s):
        first = 2 + len(down_w)
        into = list(layers)
        layers[:] = kernel(
            "down", functools.partial(down_kernel, np_), (2,),
            [tiled(hidden)] + [whole((hidden, w.shape[1])) for w in down_w] + [pl.BlockSpec(memory_space=pl.ANY)] * len(into),
            pair_of(s), [], s, active[s], *down_w, *into,
            aliases={first: 0, first + 1: 1} if into else None,
        )
        if s == seqs - 1:
            layers[:] = [Steps(sum_tp(line, *layers, n_tp))]

    fine = 1
    small_rows = rows // fine

    def halves(s):
        return [pl.BlockSpec((small_rows, model), lambda i, *_: (s * fine + i % fine, 0))] * 2

    finished = {}

    def output(name, body_, s, ins, dtype, *args):
        extra = [finished[name]] if name in finished else []
        finished[name] = kernel(
            name, functools.partial(body_, np_, fine), (2 * fine,),
            [of(s, model, small_rows)] + ins + [pl.BlockSpec(memory_space=pl.ANY)] * len(extra),
            [(shape(seqs, length, model, dtype=dtype), of(s, model, small_rows))],
            [], s, tokens, *args, *extra,
            aliases={2 + len(ins): 0} if extra else None,
        )[0]

    def layer_output(s):
        output(
            "layer_out", layer_kernel, s, halves(0) + halves(s) + [of(s, 128, small_rows)], bf16,
            *branch[s].value, *layers[0].value, valid,
        )

    resid_grad, grad_branch, grad_query, near, q_gains, came = [], [], [], [], [], []

    def bring(far):
        moving = None
        for one in far:
            one = line.after(one) if moving is None else line(plus, one, moving)
            moving = lax.ppermute(one, "ctx", down_perm)
            yield moving

    def attend_back(s):
        far_shapes = [(shape(*kv_shape), whole(kv_shape))] * back
        rg, gb, gq, qgain, *far, dkv = kernel(
            "attend_back", functools.partial(attend_back_kernel, cfg, out_at), (2,),
            [of(s, model)] + [whole((rows, model))] * 4 + [of(s, 128), whole((1, model)), of(s, model),
             tiled_t(q_width), tiled_t(sums), tiled(q_width), lanes(s),
             tiled(q_width), of(s, size), of(s, size), whole((1, size))]
            + [whole(kv_shape)] * (back + 1)
            + [whole(w.shape) for w in out_w],
            [
                (shape(length, model, dtype=f32), tiled(model)),
                (shape(length, model), tiled(model)),
                (shape(length, q_width), tiled(q_width)),
                (shape(1, size, dtype=f32), whole((1, size))),
            ]
            + far_shapes
            + [(shape(*kv_shape, dtype=f32), whole(kv_shape))],
            [
                pltpu.VMEM((window, 2 * kv_width), bf16),
                pltpu.VMEM((window, 2 * kv_width), f32),
                pltpu.VMEM((q_width, rows), f32),
                pltpu.VMEM((q_width, rows), bf16),
            ],
            s, tokens, *branch[s].value, *grad_two[s].value, valid, gain_two, out_grad, mixed[s], lse[s], queries[s],
            start, pre_q[s], cos, sin, qg, *kv[s], *out_w,
        )
        came.append(Steps(bring(far)))
        resid_grad.append(rg)
        grad_branch.append(gb)
        grad_query.append(gq)
        q_gains.append(qgain)
        near.append(dkv)

    grad_kv, k_gains, a_gains, grad_one = [], [], [], []
    qkv_w = query_w + kv_w

    def input_back(s):
        into = list(grad_one)
        first = 11 + len(qkv_w)
        gkv, own, oth, kgain, again = kernel(
            "input_back", functools.partial(input_back_kernel, (heads, kv_heads, size, np_)), (2,),
            [of(s, model), whole((1, model)), tiled(q_width), tiled(2 * kv_width), tiled(2 * kv_width),
             tiled(kv_width), of(s, size), of(s, size), whole((1, size))]
            + [whole(w.shape) for w in qkv_w] + [pl.BlockSpec(memory_space=pl.ANY)] * len(into),
            [(shape(*kv_shape), tiled(2 * kv_width))]
            + pair_of(s)
            + [(shape(1, size, dtype=f32), whole((1, size))), (shape(1, model, dtype=f32), whole((1, model)))],
            [], s, tokens, gain_one, grad_query[s], near[s], came[s].value, pre_k[s], cos, sin, kg, *qkv_w, *into,
            aliases={first - 1: 1, first: 2} if into else None,
        )
        grad_kv.append(gkv)
        k_gains.append(kgain)
        a_gains.append(again)
        grad_one[:] = [own, oth]
        if s == seqs - 1:
            grad_one[:] = [Steps(sum_tp(line, own, oth, n_tp))]

    def input_output(s):
        output(
            "input_grad", input_kernel, s, [pl.BlockSpec((small_rows, model), lambda i, *_: (i, 0))]
            + halves(s) + [whole((1, model))], f32,
            resid_grad[s], *grad_one[0].value, gain_one,
        )

    rows_split, cols_split = (0, 1) if paired else (None, None)

    def reduced(parts, axis):
        if paired:
            total = line(plus, parts[0], swap(parts[1], "fsdp", 1, 2))
        else:
            total = lax.psum_scatter(parts[0], "fsdp", scatter_dimension=axis, tiled=True)
        yield total
        yield from sum_line(line, total, "ctx", n_ctx)

    def weight(name, lefts, rights, split, left_t=False, **place_):
        def run(lefts, rights, place_):
            return product(name, ids[0], lefts, rights, split, 256, left_t, **place_)

        if not paired:
            place_ = {}
        numbers = {k: v for k, v in place_.items() if k in ("at", "height")}
        arrays = {k: v for k, v in place_.items() if k not in numbers and v is not None}
        arrays["waits"] = line.take()
        return line(lambda l, r, x: run(l, r, {**numbers, **x}), list(lefts), [list(r) for r in rights], arrays)

    gain_width = 2 * kv_width
    gain_rows = 16 * -(-(2 * part + 2 * small) // (16 * gain_width))

    def gain_sum():
        values = jnp.concatenate([sum(a_gains), sum(ffn_gains), sum(q_gains), sum(k_gains)], 1)
        bit = 1
        while bit < n_tp:
            values = line(jnp.add, values, swap(values, "tp", bit, n_tp))
            bit *= 2
            yield values
        yield values

    def gain_parts(values):
        def one(own):
            pieces = [values[:, (0 if own else part) :][:, :part], values[:, model + (0 if own else part) :][:, :part]]
            for at in (2 * model, 2 * model + size):
                low, high = values[:, at : at + small], values[:, at + small : at + size]
                pieces.append(jnp.where((fs == 0) == own, low, high))
            row = jnp.concatenate(pieces, 1)
            row = jnp.pad(row, ((0, 0), (0, gain_rows * gain_width - row.shape[1])))
            return row.reshape(gain_rows, gain_width).astype(bf16)

        return [one(True), one(False)]

    sums_of, parts_of = {}, {}

    def make(name):
        if name == "gate_up":
            parts_of[name] = weight("gate_up_grad", normed_two, [grad_gate, grad_up], rows_split)
        elif name == "down":
            parts_of[name] = weight(
                "down_grad", active, [[low_grad[s] for s in range(seqs)]], cols_split, height=hidden + q_width
            )
        elif name == "out":
            parts_of[name] = weight(
                "out_grad", mixed, [grad_branch], cols_split, True,
                at=hidden // 256, height=hidden + q_width, into=parts_of["down"],
            )
        elif name == "query":
            parts_of[name] = weight("query_grad", normed, [grad_query], rows_split)
        else:
            parts_of[name] = weight(
                "kv_grad", normed, [grad_kv], rows_split, height=model // 2 + gain_rows, tail=gain_parts(sums_of["gains"].value) if paired else None,
            )

    def send(*names):
        axis = 1 if names[0] in ("down", "out") else 0
        if paired:
            sums_of[names[0]] = Steps(reduced(parts_of[names[-1]], axis))
        else:
            steps = [reduced(parts_of[n], axis) for n in names]
            sums_of[names[0]] = Steps(zip(*steps))

    down_out = keys(0, down_out)
    if paired:
        down_w = out_w = gather(down_out[0], 1)
    else:
        down_w, out_w = gather(w_down, 1), gather(w_out, 1)
    line.wait(query_w[-1])
    spread(0)
    keys(1)
    spread(1)
    forward(0)
    query(0)
    query(1)
    attend_own(0)
    attend_own(1)
    forward(1)
    attend(0)
    line.wait(gate_w[-1], up_w[-1])
    branch[0]()
    attend(1)
    branch[0]()
    branch[1]()
    ffn(0)
    branch[1]()
    grad_two[0]()
    ffn(1)
    grad_two[0]()
    grad_two[1]()
    attend_back(0)
    came[0]()
    make("gate_up")
    send("gate_up")
    grad_two[1]()
    down(0)
    came[0]()
    attend_back(1)
    line.wait(came[0].value)
    came[1]()
    make("down")
    make("out")
    send("down", "out")
    make("query")
    send("query")
    came[1]()
    down(1)
    input_back(0)
    sums_of["gate_up"]()
    input_back(1)
    sums_of["down"]()
    sums_of["query"]()
    sums_of["gains"] = Steps(gain_sum())
    sums_of["gains"]()
    sums_of["gains"]()
    make("kv")
    send("kv")
    grad_one[0]()
    sums_of["gate_up"]()
    layers[0]()
    sums_of["kv"]()
    sums_of["down"]()
    sums_of["query"]()
    grad_one[0]()
    sums_of["gate_up"]()
    input_output(0)
    sums_of["kv"]()
    layers[0]()
    input_output(1)
    sums_of["down"]()
    layer_output(0)
    sums_of["query"]()
    sums_of["kv"]()
    layer_output(1)
    gate_up, down_and_out, query_sum, kv_total = (sums_of[name]() for name in ("gate_up", "down", "query", "kv"))
    if paired:
        gate_sum, up_sum = gate_up[:, :hidden], gate_up[:, hidden:]
        down_sum, out_sum = down_and_out[:hidden], down_and_out[hidden:]
        kv_total, gain_total = kv_total[: model // 2], kv_total[model // 2 :]
    else:
        gate_sum, up_sum = gate_up[0][:, :hidden], gate_up[0][:, hidden:]
        (down_sum, out_sum), (query_sum,), (kv_total,) = down_and_out, query_sum, kv_total
    if paired:
        mine_all = gain_total.reshape(1, -1)[0].astype(f32)
        gain_out = []
        at = 0
        for width in (part, part, small, small):
            gain_out.append(mine_all[at : at + width])
            at += width
    else:
        values = sums_of["gains"].value
        for axis, count in (("fsdp", n_fs), ("ctx", n_ctx)):
            values = sum_small(values, axis, count)
        gain_out = []
        for at, width in ((0, model), (model, model), (2 * model, size), (2 * model + size, size)):
            gain_out.append(lax.dynamic_slice_in_dim(values[0], at + fs * (width // n_fs), width // n_fs, 0))
    attn_out, ffn_out, query_out, key_out = gain_out

    return (
        finished["layer_out"],
        finished["input_grad"],
        attn_out,
        query_sum.astype(f32),
        kv_total[:, :kv_width].astype(f32),
        kv_total[:, kv_width:].astype(f32),
        query_out,
        key_out,
        out_sum.astype(f32),
        ffn_out,
        gate_sum.astype(f32),
        up_sum.astype(f32),
        down_sum.astype(f32),
    )


def solution(mesh):
    n_fs, n_ctx, n_tp = mesh.shape["fsdp"], mesh.shape["ctx"], mesh.shape["tp"]
    placed = (
        P("fsdp", "ctx", None),
        P("fsdp", None),
        P("fsdp"),
        P("fsdp", "tp"),
        P("fsdp", "tp"),
        P("fsdp", "tp"),
        P("fsdp"),
        P("fsdp"),
        P("tp", "fsdp"),
        P("fsdp"),
        P("fsdp", "tp"),
        P("fsdp", "tp"),
        P("tp", "fsdp"),
        P("fsdp", "ctx", None),
    )
    return jax.shard_map(
        functools.partial(body, n_fs, n_ctx, n_tp),
        mesh=mesh,
        in_specs=placed,
        out_specs=(
            P("fsdp", "ctx", None),
            P("fsdp", "ctx", None),
            P("fsdp"),
            P("fsdp", "tp"),
            P("fsdp", "tp"),
            P("fsdp", "tp"),
            P("fsdp"),
            P("fsdp"),
            P("tp", "fsdp"),
            P("fsdp"),
            P("fsdp", "tp"),
            P("fsdp", "tp"),
            P("tp", "fsdp"),
        ),
        check_vma=False,
    )
```

```python
import functools
import math

import jax
import jax.numpy as jnp
from jax import lax
from jax.experimental import pallas as pl
from jax.experimental.pallas import tpu as pltpu
from jax.sharding import PartitionSpec as P

epsilon = 1e-06
rope_base = 1000000.0
longest_segment = 1024
f32 = jnp.float32
bf16 = jnp.bfloat16

NN = (((1,), (0,)), ((), ()))
NT = (((1,), (1,)), ((), ()))
TN = (((0,), (0,)), ((), ()))


def dot(left, right, dims=NN):
    return lax.dot_general(left, right, dims, preferred_element_type=f32)


def inv_scale(values):
    return lax.rsqrt(jnp.mean(values * values, -1, keepdims=True) + epsilon)


def norm_back(values, scale, gain, grad):
    scaled = grad * gain
    return scale * scaled - values * (scale * scale * scale) * jnp.mean(
        scaled * values, -1, keepdims=True
    )


def rows_of(index, size):
    return pl.ds(pl.multiple_of(index * size, size), size)


def ordered(ref, fs, np_):
    if np_ == 1:
        return ref[...]
    half = ref.shape[-1] // 2
    first = ref[:, pl.ds(pl.multiple_of(fs * half, 128), half)]
    other = ref[:, pl.ds(pl.multiple_of((1 - fs) * half, 128), half)]
    return jnp.concatenate([first, other], 1)


def whole(shape):
    return pl.BlockSpec(shape, lambda *_: (0,) * len(shape))


def columns(parts):
    width = parts[0]
    return [(i * width, (i + 1) * width) for i in range(len(parts))]


def call(kernel, name, grid, ins, outs, scratch, scalars, *args, aliases=None, waits=()):
    skip = len(waits)

    def body_(ids, *refs):
        kernel(ids, *refs[skip:])

    return pl.pallas_call(
        body_,
        name=name,
        out_shape=[o[0] for o in outs],
        grid_spec=pltpu.PrefetchScalarGridSpec(
            num_scalar_prefetch=1,
            grid=grid,
            in_specs=[pl.BlockSpec(memory_space=pl.ANY)] * skip + ins,
            out_specs=[o[1] for o in outs],
            scratch_shapes=scratch,
        ),
        input_output_aliases={k + skip: v for k, v in (aliases or {}).items()},
        compiler_params=pltpu.CompilerParams(dimension_semantics=("arbitrary",) * len(grid)),
        cost_estimate=pl.CostEstimate(flops=1, bytes_accessed=1, transcendentals=0),
    )(scalars, *waits, *args)


def project(low, weights, np_):
    width = low.shape[1] // np_
    acc = None
    for i in range(np_):
        one = dot(low[:, i * width : (i + 1) * width], weights[i][...])
        acc = one if acc is None else acc + one
    return acc


def turn(acc, count, size, g, c, s, out):
    for h in range(count):
        u = acc[:, h * size : (h + 1) * size]
        u = u * inv_scale(u) * g
        out[:, h * size : (h + 1) * size] = (u * c + pltpu.roll(u, size // 2, 1) * s).astype(bf16)


def kv_kernel(kv_heads, size, np_, passed, ids, tok, gain, cos, sin, kg, *rest):
    weights, (normed, kv_out, pre_out) = rest[:np_], rest[np_ + passed : np_ + passed + 3]
    x = ordered(tok, ids[0], np_).astype(f32)
    low = (x * inv_scale(x) * gain[...]).astype(bf16)
    normed[...] = low
    acc = project(low, weights, np_)
    pre_out[...] = acc[:, : kv_heads * size]
    turn(acc, kv_heads, size, kg[...], cos[...], sin[...], kv_out)
    kv_out[:, kv_heads * size :] = acc[:, kv_heads * size :].astype(bf16)


def query_kernel(heads, size, np_, ids, normed, cos, sin, qg, *rest):
    weights, (q_out, pre_out) = rest[:np_], rest[np_:]
    acc = project(normed[...], weights, np_)
    pre_out[...] = acc
    turn(acc, heads, size, qg[...], cos[...], sin[...], q_out)


def allowed_block(key_base, start, row_base, block, rows):
    key_index = key_base + lax.broadcasted_iota(jnp.int32, (block, rows), 0)
    row_index = row_base + lax.broadcasted_iota(jnp.int32, (block, rows), 1)
    return (key_index >= start) & (key_index <= row_index)


def attend_blocks(cfg, low, high, base, kv, q, start_row, row_base, acc, total):
    heads, kv_heads, size, block, scale2 = cfg
    group = heads // kv_heads
    rows = q.shape[0]

    def step(kb, carry):
        at = pl.ds(pl.multiple_of((kb - base) * block, block), block)
        allow = allowed_block(kb * block, start_row, row_base, block, rows)
        for g in range(kv_heads):
            k = kv[at, g * size : (g + 1) * size]
            v = kv[at, (kv_heads + g) * size : (kv_heads + g + 1) * size]
            for h in range(g * group, (g + 1) * group):
                s = dot(k, q[:, h * size : (h + 1) * size], NT)
                e = jnp.where(allow, jnp.exp2(s * scale2), 0.0)
                total[h : h + 1, :] += jnp.sum(e, 0, keepdims=True)
                acc[h * size : (h + 1) * size, :] += dot(v, e.astype(bf16), TN)
        return carry

    lax.fori_loop(low, high, step, 0)


def attend_own_kernel(cfg, back, ids, q, start, kv, acc, total):
    t = pl.program_id(0)
    rows = q.shape[0]
    base = back * kv.shape[0]
    acc[...] = jnp.zeros_like(acc)
    total[...] = jnp.zeros_like(total)
    first = base // cfg[3]
    attend_blocks(
        cfg, jnp.maximum(ids[2 + t], first), (base + (t + 1) * rows) // cfg[3], first,
        kv, q, start[...], base + t * rows, acc, total,
    )


def attend_kernel(cfg, np_, back, out_at, ids, q, start, acc_in, total_in, *rest):
    heads, _, size, block, _ = cfg
    chunks = rest[:back]
    w_out = rest[back : back + np_]
    own, oth, mixed_out, lse_out, kv, acc, total = rest[back + np_ :]
    t = pl.program_id(0)
    core = ids[1]
    rows = q.shape[0]
    length = chunks[0].shape[0]

    @pl.when(t == 0)
    def _():
        for i in range(back):
            kv[i * length : (i + 1) * length, :] = chunks[i][...]

    acc[...] = acc_in[...]
    total[...] = total_in[...]
    attend_blocks(
        cfg, ids[2 + t], back * length // block, 0, kv, q, start[...], back * length + t * rows, acc, total
    )
    sums = total[...]
    sums = jnp.where(sums > 0.0, sums, 1.0)
    lse_out[...] = jnp.log2(sums)
    inverse = 1.0 / sums
    for h in range(heads):
        part = (acc[h * size : (h + 1) * size, :] * inverse[h : h + 1, :]).astype(bf16)
        mixed_out[h * size : (h + 1) * size, :] = part
    mixed = mixed_out[...]
    width = w_out[0].shape[1]
    for i in range(np_):
        part = dot(mixed, w_out[i][out_at:, :], TN).astype(bf16)

        @pl.when(t == core)
        def _():
            own[:, i * width : (i + 1) * width] = part

        @pl.when(t != core)
        def _():
            oth[:, i * width : (i + 1) * width] = part


def ffn_kernel(np_, ids, tok, b_own, b_oth, valid, gain, grad, *rest):
    gate_w, up_w, down_w = rest[:np_], rest[np_ : 2 * np_], rest[2 * np_ : 3 * np_]
    n2_out, act_out, gg_out, gu_out, own, oth, gain_out, hat, acc = rest[3 * np_ :]
    f = pl.program_id(0)
    core = ids[1]
    half = b_own.shape[0]

    @pl.when(f == 0)
    def _():
        for ref, tile in ((b_own, core), (b_oth, 1 - core)):
            at = rows_of(tile, half)
            tokens = ordered(tok.at[at], ids[0], np_).astype(f32)
            resid = tokens + valid[at, :1] * ref[...].astype(f32)
            normal = resid * inv_scale(resid)
            hat[at, :] = normal
            n2_out[at, :] = (normal * gain[...]).astype(bf16)
        acc[...] = jnp.zeros_like(acc)

    width = tok.shape[1] // np_
    parts = [(i * width, (i + 1) * width) for i in range(np_)]
    gate = up = active_grad = None
    for i, (a, b) in enumerate(parts):
        x = n2_out[:, a:b]
        g, u, d = dot(x, gate_w[i][...]), dot(x, up_w[i][...]), dot(grad[:, a:b], down_w[i][...], NT)
        gate, up, active_grad = (g, u, d) if i == 0 else (gate + g, up + u, active_grad + d)
    sigma = jax.nn.sigmoid(gate)
    silu = gate * sigma
    act_out[...] = (silu * up).astype(bf16)
    gg = (active_grad * up * sigma * (1.0 + gate * (1.0 - sigma))).astype(bf16)
    gu = (active_grad * silu).astype(bf16)
    gg_out[...] = gg
    gu_out[...] = gu
    for i, (a, b) in enumerate(parts):
        acc[:, a:b] += dot(gg, gate_w[i][...], NT) + dot(gu, up_w[i][...], NT)

    @pl.when(f == pl.num_programs(0) - 1)
    def _():
        own[...] = acc[rows_of(core, half), :].astype(bf16)
        oth[...] = acc[rows_of(1 - core, half), :].astype(bf16)
        gain_out[...] = jnp.sum(acc[...] * hat[...], 0, keepdims=True)


def down_kernel(np_, ids, act, *rest):
    weights, (own, oth) = rest[:np_], rest[-2:]
    t = pl.program_id(0)
    width = weights[0].shape[1]
    for i in range(np_):
        part = dot(act[...], weights[i][...]).astype(bf16)

        @pl.when(t == ids[1])
        def _():
            own[:, i * width : (i + 1) * width] = part

        @pl.when(t != ids[1])
        def _():
            oth[:, i * width : (i + 1) * width] = part


def picked(ids, own, oth, t):
    return jnp.where(ids[1] == t, own[...].astype(f32), oth[...].astype(f32))


def attend_back_kernel(cfg, out_at, ids, tok, b_own, b_oth, t_own, t_oth, valid, gain, grad, mixed, lse, q, start, pre, cos, sin, qg, *rest):
    heads, kv_heads, size, np_, back, block, scale2 = cfg
    chunks = rest[: back + 1]
    w_out = rest[back + 1 : back + 1 + np_]
    outs = rest[back + 1 + np_ :]
    resid_out, branch_out, gq_out, gain_out = outs[:4]
    far = outs[4 : 4 + back + 1]
    kv, dkv, dq, dout = outs[4 + back + 1 :]
    t = pl.program_id(0)
    rows = q.shape[0]
    length = chunks[0].shape[0]
    group = heads // kv_heads
    scale = size**-0.5

    @pl.when(t == 0)
    def _():
        for i in range(back + 1):
            kv[i * length : (i + 1) * length, :] = chunks[i][...]
        dkv[...] = jnp.zeros_like(dkv)
        gain_out[...] = jnp.zeros_like(gain_out)

    resid = ordered(tok, ids[0], np_).astype(f32) + valid[:, :1] * picked(ids, b_own, b_oth, t)
    resid_grad = ordered(grad, ids[0], np_).astype(f32) + norm_back(
        resid, inv_scale(resid), gain[...], picked(ids, t_own, t_oth, t)
    )
    resid_out[...] = resid_grad
    low = (valid[:, :1] * resid_grad).astype(bf16)
    branch_out[...] = low
    width = low.shape[1] // np_
    mixed_grad = dot(w_out[0][out_at:, :], low[:, :width], NT)
    for i in range(1, np_):
        mixed_grad = mixed_grad + dot(w_out[i][out_at:, :], low[:, i * width : (i + 1) * width], NT)
    dout[...] = mixed_grad.astype(bf16)
    delta = [
        jnp.sum(
            dout[h * size : (h + 1) * size, :].astype(f32) * mixed[h * size : (h + 1) * size, :].astype(f32),
            0,
            keepdims=True,
        )
        for h in range(heads)
    ]
    dq[...] = jnp.zeros_like(dq)
    row_base = back * length + t * rows
    start_row = start[...]

    def step(kb, carry):
        at = pl.ds(pl.multiple_of(kb * block, block), block)
        allow = allowed_block(kb * block, start_row, row_base, block, rows)
        for g in range(kv_heads):
            k = kv[at, g * size : (g + 1) * size]
            v = kv[at, (kv_heads + g) * size : (kv_heads + g + 1) * size]
            dk = dv = None
            for h in range(g * group, (g + 1) * group):
                qh = q[:, h * size : (h + 1) * size]
                do = dout[h * size : (h + 1) * size, :]
                s = dot(k, qh, NT)
                p = jnp.where(allow, jnp.exp2(s * scale2 - lse[h : h + 1, :]), 0.0)
                dp = dot(v, do)
                ds = (p * (dp - delta[h])).astype(bf16)
                one_v = dot(p.astype(bf16), do, NT)
                one_k = dot(ds, qh)
                dk, dv = (one_k, one_v) if dk is None else (dk + one_k, dv + one_v)
                dq[h * size : (h + 1) * size, :] += dot(k, ds, TN)
            dkv[at, g * size : (g + 1) * size] += dk * scale
            dkv[at, (kv_heads + g) * size : (kv_heads + g + 1) * size] += dv
        return carry

    lax.fori_loop(ids[2 + t], (row_base + rows) // block, step, 0)
    c, s_ = cos[...], sin[...]
    for h in range(heads):
        u = dq[h * size : (h + 1) * size, :].T * scale
        u = u * c - pltpu.roll(u, size // 2, 1) * s_
        v = pre[:, h * size : (h + 1) * size]
        r = inv_scale(v)
        gain_out[...] += jnp.sum(u * (v * r), 0, keepdims=True)
        gq_out[:, h * size : (h + 1) * size] = norm_back(v, r, qg[...], u).astype(bf16)

    @pl.when(t == pl.num_programs(0) - 1)
    def _():
        for i in range(back + 1):
            far[i][...] = dkv[i * length : (i + 1) * length, :].astype(far[i].dtype)


def input_back_kernel(cfg, ids, tok, gain, gq, near, came, pre, cos, sin, kg, *rest):
    heads, kv_heads, size, np_ = cfg
    weights = rest[: 2 * np_]
    gkv_out, own, oth, k_gain, a_gain = rest[-5:]
    t = pl.program_id(0)
    core = ids[1]

    @pl.when(t == 0)
    def _():
        k_gain[...] = jnp.zeros_like(k_gain)
        a_gain[...] = jnp.zeros_like(a_gain)

    dkv = near[...] + came[...].astype(f32)
    c, s_ = cos[...], sin[...]
    for h in range(kv_heads):
        u = dkv[:, h * size : (h + 1) * size]
        u = u * c - pltpu.roll(u, size // 2, 1) * s_
        v = pre[:, h * size : (h + 1) * size]
        r = inv_scale(v)
        k_gain[...] += jnp.sum(u * (v * r), 0, keepdims=True)
        gkv_out[:, h * size : (h + 1) * size] = norm_back(v, r, kg[...], u).astype(bf16)
    gkv_out[:, kv_heads * size :] = dkv[:, kv_heads * size :].astype(bf16)
    x = ordered(tok, ids[0], np_).astype(f32)
    normal = x * inv_scale(x)
    width = x.shape[1] // np_
    for i in range(np_):
        at = slice(i * width, (i + 1) * width)
        part = dot(gq[...], weights[i][...], NT)
        part = part + dot(gkv_out[...], weights[np_ + i][...], NT)
        a_gain[:, at] += jnp.sum(part * normal[:, at], 0, keepdims=True)
        low = part.astype(bf16)

        @pl.when(t == core)
        def _():
            own[:, at] = low

        @pl.when(t != core)
        def _():
            oth[:, at] = low


def place(out, values, fs, np_):
    width = values.shape[1] // np_
    if np_ == 1:
        out[...] = values
        return
    for i in range(2):
        at = pl.ds(pl.multiple_of((fs if i == 0 else 1 - fs) * width, 128), width)
        out[:, at] = values[:, i * width : (i + 1) * width]


def layer_kernel(np_, fine, ids, tok, b_own, b_oth, f_own, f_oth, valid, *rest):
    out = rest[-1]
    t = pl.program_id(0) // fine
    v = valid[:, :1]
    resid = ordered(tok, ids[0], np_).astype(f32) + v * picked(ids, b_own, b_oth, t)
    place(out, (resid + v * picked(ids, f_own, f_oth, t)).astype(bf16), ids[0], np_)


def input_kernel(np_, fine, ids, tok, resid_grad, g_own, g_oth, gain, *rest):
    out = rest[-1]
    t = pl.program_id(0) // fine
    x = ordered(tok, ids[0], np_).astype(f32)
    grad = resid_grad[...] + norm_back(x, inv_scale(x), gain[...], picked(ids, g_own, g_oth, t))
    place(out, grad, ids[0], np_)


def product_kernel(pairs, groups, tiles, split, left_t, tail, ids, *rest):
    count = 1 if split is None else 2
    outs = rest[-count:]
    m = pl.program_id(0)

    def low():
        columns = []
        for j in range(groups):
            total = None
            for i in range(pairs):
                one = dot(rest[i][...], rest[pairs * (1 + j) + i][...], NN if left_t else TN)
                total = one if total is None else total + one
            columns.append(total.astype(bf16))
        return columns[0] if groups == 1 else jnp.concatenate(columns, 1)

    if split is None:
        outs[0][...] = low()
    elif split == 1:
        value = low()
        width = value.shape[1] // 2
        outs[0][...] = value[:, :width]
        outs[1][...] = value[:, width:]
    else:

        @pl.when(m < tiles // 2)
        def _():
            outs[0][...] = low()

        @pl.when((m >= tiles // 2) & (m < tiles))
        def _():
            outs[1][...] = low()

    if tail:

        @pl.when(m == tiles)
        def _():
            at = pairs * (1 + groups)
            for i in range(2):
                outs[i][: rest[at + i].shape[0], :] = rest[at + i][...]


def product(name, ids, lefts, rights, split, tile, left_t=False, at=0, height=None, into=None, tail=None, waits=()):
    pairs, groups = len(lefts), len(rights)
    m = lefts[0].shape[0 if left_t else 1]
    k = lefts[0].shape[1 if left_t else 0]
    n = sum(r[0].shape[1] for r in rights)
    tiles = m // tile
    ins, args = [], []
    for left in lefts:
        if left_t:
            ins.append(pl.BlockSpec((tile, k), lambda i, *_: (jnp.minimum(i, tiles - 1), 0)))
        else:
            ins.append(pl.BlockSpec((k, tile), lambda i, *_: (0, jnp.minimum(i, tiles - 1))))
        args.append(left)
    for group in rights:
        for right in group:
            ins.append(whole(right.shape))
            args.append(right)
    if split is None:
        shape = jax.ShapeDtypeStruct((height or m, n), bf16)
        outs = [(shape, pl.BlockSpec((tile, n), lambda i, *_: (i + at, 0)))]
    elif split == 1:
        shape = jax.ShapeDtypeStruct((height or m, n // 2), bf16)
        outs = [(shape, pl.BlockSpec((tile, n // 2), lambda i, *_: (i + at, 0)))] * 2
    else:
        half = tiles // 2
        shape = jax.ShapeDtypeStruct((height or m // 2, n), bf16)
        last = at + half if tail is not None else at + half - 1

        def own(i, *_):
            return (jnp.where(i < half, i + at, jnp.where(i < tiles, half - 1 + at, last)), 0)

        def other(i, *_):
            return (jnp.where(i < tiles, jnp.maximum(i - half, 0) + at, last), 0)

        outs = [(shape, pl.BlockSpec((tile, n), own)), (shape, pl.BlockSpec((tile, n), other))]
    if tail is not None:
        ins += [whole(v.shape) for v in tail]
        args += list(tail)
    aliases = None
    if into is not None:
        aliases = {1 + len(ins) + i: i for i in range(len(into))}
        ins += [pl.BlockSpec(memory_space=pl.ANY)] * len(into)
        args += list(into)
    return call(
        functools.partial(product_kernel, pairs, groups, tiles, split, left_t, tail is not None),
        name, (tiles + (tail is not None),), ins, outs, [], ids, *args, aliases=aliases, waits=waits,
    )


def swap(values, axis, bit, size):
    return lax.ppermute(values, axis, [(i, i ^ bit) for i in range(size)])


def plus(a, b):
    return a + b


class Line:
    def __init__(self):
        self.last = None
        self.waited = ()

    def __call__(self, fn, *args):
        if self.last is not None:
            args, _ = lax.optimization_barrier((args, self.last))
        outs = fn(*args)
        self.last = jax.tree.leaves(outs)[0]
        return outs

    def wait(self, *values):
        self.waited += values

    def take(self):
        values, self.waited = self.waited, ()
        return values

    def after(self, value):
        return lax.optimization_barrier((value, self.last, self.waited))[0]


class Steps:
    def __init__(self, steps):
        self.steps, self.value = steps, None

    def __call__(self, count=1):
        for _ in range(count):
            self.value = next(self.steps)
        return self.value


def sum_tp(line, own, oth, size):
    total = line(plus, own, swap(line.after(oth), "tp", 1, size))
    yield total
    bit = 2
    while bit < size:
        total = line(plus, total, swap(total, "tp", bit, size))
        bit *= 2
        if bit < size:
            yield total
    yield total, swap(total, "tp", 1, size)


def sum_line(line, total, axis, size):
    index = lax.axis_index(axis)
    middle = size // 2
    for i in range(middle - 1):
        came = lax.ppermute(total, axis, [(i, i + 1), (size - 1 - i, size - 2 - i)])
        total = line(plus, total, came)
        yield total
    total = line(plus, total, lax.ppermute(total, axis, [(middle - 1, middle), (middle, middle - 1)]))
    yield total
    came, outer = total, index < 0
    for i in reversed(range(middle - 1)):
        total = jnp.where(outer, came, total)
        came = lax.ppermute(total, axis, [(i + 1, i), (size - 2 - i, size - 1 - i)])
        outer = (index == i) | (index == size - 1 - i)
    yield came, total, outer


def sum_small(values, axis, size):
    bit = 1
    while bit < size:
        values = values + swap(values, axis, bit, size)
        bit *= 2
    return values


def body(
    n_fs, n_ctx, n_tp,
    tokens, segment_ids, attn_gain, w_query, w_key, w_value, query_gain, key_gain,
    w_out, ffn_gain, w_gate, w_up, w_down, out_grad,
):
    seqs, length, model = tokens.shape
    paired = n_fs == 2
    np_ = 2 if paired else 1
    fs = lax.axis_index("fsdp")
    ctx = lax.axis_index("ctx")
    core = lax.axis_index("tp") % 2
    size = query_gain.shape[0] * n_fs
    heads = w_query.shape[1] // size
    kv_heads = w_key.shape[1] // size
    hidden = w_gate.shape[1]
    q_width, kv_width = heads * size, kv_heads * size
    rows = length // 2
    block = rows
    back = min(n_ctx - 1, -(-(longest_segment - 1) // length))
    scale2 = size**-0.5 * math.log2(math.e)

    def gather(weight, axis):
        if paired:
            return [weight, swap(weight, "fsdp", 1, 2)]
        return [lax.all_gather(weight, "fsdp", axis=axis, tiled=True)]

    kv_w = gather(jnp.concatenate([w_key, w_value], 1), 0)
    query_w = gather(w_query, 0)
    gate_w = gather(w_gate, 0)
    up_w = gather(w_up, 0)
    down_out = [jnp.concatenate([w_down, w_out], 0)] if paired else []
    out_at = hidden if paired else 0

    part, small = attn_gain.shape[0], query_gain.shape[0]
    padding = part - 2 * small
    gains = jnp.concatenate([query_gain, key_gain] + ([jnp.zeros((padding,), bf16)] if padding > 0 else []))
    gains = jnp.stack([attn_gain, ffn_gain, gains[:part]]) if padding >= 0 else None
    if paired:
        gains, kv_w[0] = lax.optimization_barrier((gains, kv_w[0]))
    both = [gains, swap(gains, "fsdp", 1, 2)] if paired else None
    if paired:
        wide = jnp.concatenate(both, 1).astype(f32)
        gain_one, gain_two = wide[:1], wide[1:2]

    def natural(first, values):
        if not paired:
            return lax.all_gather(values, "fsdp", axis=0, tiled=True)[None, :].astype(f32)
        own_first = jnp.concatenate([b[2:, first : first + small] for b in both], 1)
        return jnp.where(fs == 0, own_first, jnp.roll(own_first, small, 1)).astype(f32)

    if not paired:
        gain_one, gain_two = natural(0, attn_gain), natural(0, ffn_gain)
    qg, kg = natural(0, query_gain), natural(small, key_gain)

    def reorder(values):
        if not paired:
            return values
        half = model // 2
        return jnp.where(fs == 0, values, jnp.concatenate([values[..., half:], values[..., :half]], -1))

    index = ctx * length + jnp.arange(length, dtype=jnp.int32)
    row_seg = lax.dynamic_slice_in_dim(segment_ids, ctx * length, length, 1)
    first = jnp.sum((segment_ids[:, None, :] < row_seg[:, :, None]).astype(jnp.int32), -1)
    position = index[None, :] - first
    live = row_seg != 0
    valid = jnp.broadcast_to(live.astype(f32)[:, :, None], (seqs, length, 128))
    window = (back + 1) * length
    start = jnp.where(live, jnp.maximum(first - (ctx - back) * length, 0), window + 1)
    lowest = jnp.min(start.reshape(seqs, 2, rows), -1) // block
    frequency = rope_base ** (-(jnp.arange(size // 2, dtype=f32) * 2.0 / size))
    turned = position.astype(f32)[:, :, None] * frequency
    cosine, sine = jnp.cos(turned), jnp.sin(turned)
    cos = jnp.concatenate([cosine, cosine], -1)
    sin = jnp.concatenate([-sine, sine], -1)
    low_grad = jnp.where(live[:, :, None], reorder(out_grad), jnp.zeros((), bf16))
    start = start[:, None, :]

    def scalars(s):
        return jnp.concatenate([jnp.stack([fs, core]).astype(jnp.int32), lowest[s]])

    ids = [scalars(s) for s in range(seqs)]
    cfg = (heads, kv_heads, size, np_, back, block, scale2)
    cfg_forward = (heads, kv_heads, size, block, scale2)

    def tiled(width):
        return pl.BlockSpec((rows, width), lambda i, *_: (i, 0))

    def tiled_t(height):
        return pl.BlockSpec((height, rows), lambda i, *_: (0, i))

    def of(s, width, tile=rows):
        return pl.BlockSpec((None, tile, width), lambda i, *_: (s, i, 0))

    def all_of(s, width):
        return pl.BlockSpec((None, length, width), lambda *_: (s, 0, 0))

    def lanes(s):
        return pl.BlockSpec((None, 1, rows), lambda i, *_: (s, 0, i))

    def shape(*dims, dtype=bf16):
        return jax.ShapeDtypeStruct(dims, dtype)

    half_pair = [(shape(rows, model), whole((rows, model)))] * 2

    line = Line()
    up_perm = [(i, i + 1) for i in range(n_ctx - 1)]
    down_perm = [(i + 1, i) for i in range(n_ctx - 1)]
    kv_shape = (length, 2 * kv_width)
    sums = 8 * -(-heads // 8)

    def kernel(name, body_, grid, ins, outs, scratch, s, *args, aliases=None):
        count = len(args)

        def run(*all_args):
            return call(
                body_, name, grid, ins, outs, scratch, ids[s], *all_args[:count],
                aliases=aliases, waits=all_args[count:],
            )

        return line(run, *args, *line.take())

    normed, own_kv, pre_k, queries, pre_q = [], [], [], [], []

    def keys(s, through=()):
        first = 6 + len(kv_w)
        n, k, p, *through = kernel(
            "keys", functools.partial(kv_kernel, kv_heads, size, np_, len(through)), (2,),
            [of(s, model), whole((1, model)), of(s, size), of(s, size), whole((1, size))]
            + [whole(w.shape) for w in kv_w] + [pl.BlockSpec(memory_space=pl.ANY)] * len(through),
            [
                (shape(length, model), tiled(model)),
                (shape(*kv_shape), tiled(2 * kv_width)),
                (shape(length, kv_width, dtype=f32), tiled(kv_width)),
            ]
            + [(shape(*v.shape), pl.BlockSpec(memory_space=pl.ANY)) for v in through],
            [], s, tokens, gain_one, cos, sin, kg, *kv_w, *through,
            aliases={first + i: 3 + i for i in range(len(through))},
        )
        normed.append(n)
        own_kv.append(k)
        pre_k.append(p)
        return through

    def query(s):
        q, p = kernel(
            "query", functools.partial(query_kernel, heads, size, np_), (2,),
            [tiled(model), of(s, size), of(s, size), whole((1, size))] + [whole(w.shape) for w in query_w],
            [
                (shape(length, q_width), tiled(q_width)),
                (shape(length, q_width, dtype=f32), tiled(q_width)),
            ],
            [], s, normed[s], cos, sin, qg, *query_w,
        )
        queries.append(q)
        pre_q.append(p)

    kv = []

    def spread(s):
        chunks = [line.after(own_kv[s])]
        chunks.insert(0, lax.ppermute(chunks[0], "ctx", up_perm))
        kv.append(chunks)

    def forward(s):
        for _ in range(back - 1):
            kv[s].insert(0, lax.ppermute(line.after(kv[s][0]), "ctx", up_perm))

    sums_own, mixed, lse, branch = [], [], [], []

    def attend_own(s):
        sums_own.append(
            kernel(
                "attend_own", functools.partial(attend_own_kernel, cfg_forward, back), (2,),
                [tiled(q_width), lanes(s), whole(kv_shape)],
                [
                    (shape(q_width, length, dtype=f32), tiled_t(q_width)),
                    (shape(sums, length, dtype=f32), tiled_t(sums)),
                ],
                [], s, queries[s], start, own_kv[s],
            )
        )

    def attend(s):
        own, oth, m, l = kernel(
            "attend", functools.partial(attend_kernel, cfg_forward, np_, back, out_at), (2,),
            [tiled(q_width), lanes(s), tiled_t(q_width), tiled_t(sums)]
            + [whole(kv_shape)] * back + [whole(w.shape) for w in out_w],
            half_pair
            + [
                (shape(q_width, length), tiled_t(q_width)),
                (shape(sums, length, dtype=f32), tiled_t(sums)),
            ],
            [
                pltpu.VMEM((back * length, 2 * kv_width), bf16),
                pltpu.VMEM((q_width, rows), f32),
                pltpu.VMEM((sums, rows), f32),
            ],
            s, queries[s], start, *sums_own[s], *kv[s][:back], *out_w,
        )
        mixed.append(m)
        lse.append(l)
        branch.append(Steps(sum_tp(line, own, oth, n_tp)))

    tile = 256
    steps = hidden // tile
    normed_two, active, grad_gate, grad_up, grad_two, ffn_gains = [], [], [], [], [], []

    def ffn(s):
        col = pl.BlockSpec((length, tile), lambda i, *_: (0, i))
        w_in = [pl.BlockSpec((w.shape[0], tile), lambda i, *_: (0, i)) for w in gate_w]
        w_dn = [pl.BlockSpec((tile, w.shape[1]), lambda i, *_: (i, 0)) for w in down_w]
        n2, act, gg, gu, own, oth, fg = kernel(
            "ffn", functools.partial(ffn_kernel, np_), (steps,),
            [all_of(s, model), whole((rows, model)), whole((rows, model)), all_of(s, 128),
             whole((1, model)), all_of(s, model)] + w_in + w_in + w_dn,
            [
                (shape(length, model), whole((length, model))),
                (shape(length, hidden), col),
                (shape(length, hidden), col),
                (shape(length, hidden), col),
            ]
            + half_pair
            + [(shape(1, model, dtype=f32), whole((1, model)))],
            [pltpu.VMEM((length, model), f32), pltpu.VMEM((length, model), f32)],
            s, tokens, *branch[s].value, valid, gain_two, low_grad, *gate_w, *up_w, *down_w,
        )
        normed_two.append(n2)
        active.append(act)
        grad_gate.append(gg)
        grad_up.append(gu)
        grad_two.append(Steps(sum_tp(line, own, oth, n_tp)))
        ffn_gains.append(fg)

    both_pair = [
        (shape(seqs * rows, model), lambda s: pl.BlockSpec((rows, model), lambda *_: (s, 0))),
    ] * 2

    def pair_of(s):
        return [(one, spec(s)) for one, spec in both_pair]

    layers = []

    def down(s):
        first = 2 + len(down_w)
        into = list(layers)
        layers[:] = kernel(
            "down", functools.partial(down_kernel, np_), (2,),
            [tiled(hidden)] + [whole((hidden, w.shape[1])) for w in down_w] + [pl.BlockSpec(memory_space=pl.ANY)] * len(into),
            pair_of(s), [], s, active[s], *down_w, *into,
            aliases={first: 0, first + 1: 1} if into else None,
        )
        if s == seqs - 1:
            layers[:] = [Steps(sum_tp(line, *layers, n_tp))]

    fine = 1
    small_rows = rows // fine

    def halves(s):
        return [pl.BlockSpec((small_rows, model), lambda i, *_: (s * fine + i % fine, 0))] * 2

    finished = {}

    def output(name, body_, s, ins, dtype, *args):
        extra = [finished[name]] if name in finished else []
        finished[name] = kernel(
            name, functools.partial(body_, np_, fine), (2 * fine,),
            [of(s, model, small_rows)] + ins + [pl.BlockSpec(memory_space=pl.ANY)] * len(extra),
            [(shape(seqs, length, model, dtype=dtype), of(s, model, small_rows))],
            [], s, tokens, *args, *extra,
            aliases={2 + len(ins): 0} if extra else None,
        )[0]

    def layer_output(s):
        output(
            "layer_out", layer_kernel, s, halves(0) + halves(s) + [of(s, 128, small_rows)], bf16,
            *branch[s].value, *layers[0].value, valid,
        )

    resid_grad, grad_branch, grad_query, near, q_gains, came = [], [], [], [], [], []

    def bring(far):
        moving = None
        for one in far:
            one = line.after(one) if moving is None else line(plus, one, moving)
            moving = lax.ppermute(one, "ctx", down_perm)
            yield moving

    def attend_back(s):
        far_shapes = [(shape(*kv_shape), whole(kv_shape))] * back
        rg, gb, gq, qgain, *far, dkv = kernel(
            "attend_back", functools.partial(attend_back_kernel, cfg, out_at), (2,),
            [of(s, model)] + [whole((rows, model))] * 4 + [of(s, 128), whole((1, model)), of(s, model),
             tiled_t(q_width), tiled_t(sums), tiled(q_width), lanes(s),
             tiled(q_width), of(s, size), of(s, size), whole((1, size))]
            + [whole(kv_shape)] * (back + 1)
            + [whole(w.shape) for w in out_w],
            [
                (shape(length, model, dtype=f32), tiled(model)),
                (shape(length, model), tiled(model)),
                (shape(length, q_width), tiled(q_width)),
                (shape(1, size, dtype=f32), whole((1, size))),
            ]
            + far_shapes
            + [(shape(*kv_shape, dtype=f32), whole(kv_shape))],
            [
                pltpu.VMEM((window, 2 * kv_width), bf16),
                pltpu.VMEM((window, 2 * kv_width), f32),
                pltpu.VMEM((q_width, rows), f32),
                pltpu.VMEM((q_width, rows), bf16),
            ],
            s, tokens, *branch[s].value, *grad_two[s].value, valid, gain_two, out_grad, mixed[s], lse[s], queries[s],
            start, pre_q[s], cos, sin, qg, *kv[s], *out_w,
        )
        came.append(Steps(bring(far)))
        resid_grad.append(rg)
        grad_branch.append(gb)
        grad_query.append(gq)
        q_gains.append(qgain)
        near.append(dkv)

    grad_kv, k_gains, a_gains, grad_one = [], [], [], []
    qkv_w = query_w + kv_w

    def input_back(s):
        into = list(grad_one)
        first = 11 + len(qkv_w)
        gkv, own, oth, kgain, again = kernel(
            "input_back", functools.partial(input_back_kernel, (heads, kv_heads, size, np_)), (2,),
            [of(s, model), whole((1, model)), tiled(q_width), tiled(2 * kv_width), tiled(2 * kv_width),
             tiled(kv_width), of(s, size), of(s, size), whole((1, size))]
            + [whole(w.shape) for w in qkv_w] + [pl.BlockSpec(memory_space=pl.ANY)] * len(into),
            [(shape(*kv_shape), tiled(2 * kv_width))]
            + pair_of(s)
            + [(shape(1, size, dtype=f32), whole((1, size))), (shape(1, model, dtype=f32), whole((1, model)))],
            [], s, tokens, gain_one, grad_query[s], near[s], came[s].value, pre_k[s], cos, sin, kg, *qkv_w, *into,
            aliases={first - 1: 1, first: 2} if into else None,
        )
        grad_kv.append(gkv)
        k_gains.append(kgain)
        a_gains.append(again)
        grad_one[:] = [own, oth]
        if s == seqs - 1:
            grad_one[:] = [Steps(sum_tp(line, own, oth, n_tp))]

    def input_output(s):
        output(
            "input_grad", input_kernel, s, [pl.BlockSpec((small_rows, model), lambda i, *_: (i, 0))]
            + halves(s) + [whole((1, model))], f32,
            resid_grad[s], *grad_one[0].value, gain_one,
        )

    rows_split, cols_split = (0, 1) if paired else (None, None)

    def reduced(parts, axis):
        if paired:
            total = line(plus, parts[0], swap(parts[1], "fsdp", 1, 2))
        else:
            total = lax.psum_scatter(parts[0], "fsdp", scatter_dimension=axis, tiled=True)
        yield total
        yield from sum_line(line, total, "ctx", n_ctx)

    def weight(name, lefts, rights, split, left_t=False, **place_):
        def run(lefts, rights, place_):
            return product(name, ids[0], lefts, rights, split, 256, left_t, **place_)

        if not paired:
            place_ = {}
        numbers = {k: v for k, v in place_.items() if k in ("at", "height")}
        arrays = {k: v for k, v in place_.items() if k not in numbers and v is not None}
        arrays["waits"] = line.take()
        return line(lambda l, r, x: run(l, r, {**numbers, **x}), list(lefts), [list(r) for r in rights], arrays)

    gain_width = 2 * kv_width
    gain_rows = 16 * -(-(2 * part + 2 * small) // (16 * gain_width))

    def gain_sum():
        values = jnp.concatenate([sum(a_gains), sum(ffn_gains), sum(q_gains), sum(k_gains)], 1)
        bit = 1
        while bit < n_tp:
            values = line(jnp.add, values, swap(values, "tp", bit, n_tp))
            bit *= 2
            yield values
        yield values

    def gain_parts(values):
        def one(own):
            pieces = [values[:, (0 if own else part) :][:, :part], values[:, model + (0 if own else part) :][:, :part]]
            for at in (2 * model, 2 * model + size):
                low, high = values[:, at : at + small], values[:, at + small : at + size]
                pieces.append(jnp.where((fs == 0) == own, low, high))
            row = jnp.concatenate(pieces, 1)
            row = jnp.pad(row, ((0, 0), (0, gain_rows * gain_width - row.shape[1])))
            return row.reshape(gain_rows, gain_width).astype(bf16)

        return [one(True), one(False)]

    sums_of, parts_of = {}, {}

    def make(name):
        if name == "gate_up":
            parts_of[name] = weight("gate_up_grad", normed_two, [grad_gate, grad_up], rows_split)
        elif name == "down":
            parts_of[name] = weight(
                "down_grad", active, [[low_grad[s] for s in range(seqs)]], cols_split, height=hidden + q_width
            )
        elif name == "out":
            parts_of[name] = weight(
                "out_grad", mixed, [grad_branch], cols_split, True,
                at=hidden // 256, height=hidden + q_width, into=parts_of["down"],
            )
        elif name == "query":
            parts_of[name] = weight("query_grad", normed, [grad_query], rows_split)
        else:
            parts_of[name] = weight(
                "kv_grad", normed, [grad_kv], rows_split, height=model // 2 + gain_rows, tail=gain_parts(sums_of["gains"].value) if paired else None,
            )

    def send(*names):
        axis = 1 if names[0] in ("down", "out") else 0
        if paired:
            sums_of[names[0]] = Steps(reduced(parts_of[names[-1]], axis))
        else:
            steps = [reduced(parts_of[n], axis) for n in names]
            sums_of[names[0]] = Steps(zip(*steps))

    down_out = keys(0, down_out)
    if paired:
        down_w = out_w = gather(down_out[0], 1)
    else:
        down_w, out_w = gather(w_down, 1), gather(w_out, 1)
    line.wait(query_w[-1])
    spread(0)
    keys(1)
    spread(1)
    forward(0)
    query(0)
    query(1)
    attend_own(0)
    attend_own(1)
    forward(1)
    attend(0)
    line.wait(gate_w[-1])
    branch[0]()
    attend(1)
    branch[0]()
    line.wait(up_w[-1])
    branch[1]()
    ffn(0)
    branch[1]()
    grad_two[0]()
    ffn(1)
    grad_two[0]()
    grad_two[1]()
    attend_back(0)
    came[0]()
    make("gate_up")
    send("gate_up")
    grad_two[1]()
    down(0)
    came[0]()
    attend_back(1)
    line.wait(came[0].value)
    came[1]()
    make("down")
    make("out")
    send("down", "out")
    make("query")
    send("query")
    came[1]()
    down(1)
    input_back(0)
    sums_of["gate_up"]()
    input_back(1)
    sums_of["down"]()
    sums_of["query"]()
    sums_of["gains"] = Steps(gain_sum())
    sums_of["gains"]()
    sums_of["gains"]()
    make("kv")
    send("kv")
    grad_one[0]()
    sums_of["gate_up"]()
    layers[0]()
    grad_one[0]()
    input_output(0)
    sums_of["down"]()
    sums_of["gate_up"]()
    sums_of["query"]()
    sums_of["kv"]()
    layers[0]()
    input_output(1)
    sums_of["down"]()
    sums_of["kv"]()
    layer_output(0)
    sums_of["query"]()
    sums_of["kv"]()
    half = model // 2

    def wide_type(value):
        return (value.astype(f32),)

    def columns_of(width):
        return lambda value: (value[:, :width].astype(f32), value[:, width:].astype(f32))

    def rows_at(height):
        return lambda value: (value[:height].astype(f32), value[height:].astype(f32))

    def keys_values(value):
        return columns_of(kv_width)(value[:half]) + (value[half:].astype(f32),)

    def finish(name, *after):
        steps_ = sums_of[name]()
        outs = []
        for (came_, total, outer), to in zip([steps_] if paired else steps_, after):
            outs += line(lambda c, v: to(jnp.where(outer, c, v)), came_, total)
        return outs

    if paired:
        gate_sum, up_sum = finish("gate_up", columns_of(hidden))
        layer_output(1)
        down_sum, out_sum = finish("down", rows_at(hidden))
        (query_sum,) = finish("query", wide_type)
        key_sum, value_sum, gain_total = finish("kv", keys_values)
    else:
        layer_output(1)
        gate_sum, up_sum = finish("gate_up", columns_of(hidden))
        down_sum, out_sum = finish("down", wide_type, wide_type)
        (query_sum,) = finish("query", wide_type)
        key_sum, value_sum = finish("kv", columns_of(kv_width))
    if paired:
        mine_all = gain_total.reshape(1, -1)[0]
        gain_out = []
        at = 0
        for width in (part, part, small, small):
            gain_out.append(mine_all[at : at + width])
            at += width
    else:
        values = sums_of["gains"].value
        for axis, count in (("fsdp", n_fs), ("ctx", n_ctx)):
            values = sum_small(values, axis, count)
        gain_out = []
        for at, width in ((0, model), (model, model), (2 * model, size), (2 * model + size, size)):
            gain_out.append(lax.dynamic_slice_in_dim(values[0], at + fs * (width // n_fs), width // n_fs, 0))
    attn_out, ffn_out, query_out, key_out = gain_out

    return (
        finished["layer_out"],
        finished["input_grad"],
        attn_out,
        query_sum,
        key_sum,
        value_sum,
        query_out,
        key_out,
        out_sum,
        ffn_out,
        gate_sum,
        up_sum,
        down_sum,
    )


def solution(mesh):
    n_fs, n_ctx, n_tp = mesh.shape["fsdp"], mesh.shape["ctx"], mesh.shape["tp"]
    placed = (
        P("fsdp", "ctx", None),
        P("fsdp", None),
        P("fsdp"),
        P("fsdp", "tp"),
        P("fsdp", "tp"),
        P("fsdp", "tp"),
        P("fsdp"),
        P("fsdp"),
        P("tp", "fsdp"),
        P("fsdp"),
        P("fsdp", "tp"),
        P("fsdp", "tp"),
        P("tp", "fsdp"),
        P("fsdp", "ctx", None),
    )
    return jax.shard_map(
        functools.partial(body, n_fs, n_ctx, n_tp),
        mesh=mesh,
        in_specs=placed,
        out_specs=(
            P("fsdp", "ctx", None),
            P("fsdp", "ctx", None),
            P("fsdp"),
            P("fsdp", "tp"),
            P("fsdp", "tp"),
            P("fsdp", "tp"),
            P("fsdp"),
            P("fsdp"),
            P("tp", "fsdp"),
            P("fsdp"),
            P("fsdp", "tp"),
            P("fsdp", "tp"),
            P("tp", "fsdp"),
        ),
        check_vma=False,
    )
```

```python
import functools
import math

import jax
import jax.numpy as jnp
from jax import lax
from jax.experimental import pallas as pl
from jax.experimental.pallas import tpu as pltpu
from jax.sharding import PartitionSpec as P

epsilon = 1e-06
rope_base = 1000000.0
longest_segment = 1024
f32 = jnp.float32
bf16 = jnp.bfloat16

NN = (((1,), (0,)), ((), ()))
NT = (((1,), (1,)), ((), ()))
TN = (((0,), (0,)), ((), ()))


def dot(left, right, dims=NN):
    return lax.dot_general(left, right, dims, preferred_element_type=f32)


def inv_scale(values):
    return lax.rsqrt(jnp.mean(values * values, -1, keepdims=True) + epsilon)


def norm_back(values, scale, gain, grad):
    scaled = grad * gain
    return scale * scaled - values * (scale * scale * scale) * jnp.mean(
        scaled * values, -1, keepdims=True
    )


def rows_of(index, size):
    return pl.ds(pl.multiple_of(index * size, size), size)


def ordered(ref, fs, np_):
    if np_ == 1:
        return ref[...]
    half = ref.shape[-1] // 2
    first = ref[:, pl.ds(pl.multiple_of(fs * half, 128), half)]
    other = ref[:, pl.ds(pl.multiple_of((1 - fs) * half, 128), half)]
    return jnp.concatenate([first, other], 1)


def whole(shape):
    return pl.BlockSpec(shape, lambda *_: (0,) * len(shape))


def columns(parts):
    width = parts[0]
    return [(i * width, (i + 1) * width) for i in range(len(parts))]


def call(kernel, name, grid, ins, outs, scratch, scalars, *args, aliases=None, waits=()):
    skip = len(waits)

    def body_(ids, *refs):
        kernel(ids, *refs[skip:])

    return pl.pallas_call(
        body_,
        name=name,
        out_shape=[o[0] for o in outs],
        grid_spec=pltpu.PrefetchScalarGridSpec(
            num_scalar_prefetch=1,
            grid=grid,
            in_specs=[pl.BlockSpec(memory_space=pl.ANY)] * skip + ins,
            out_specs=[o[1] for o in outs],
            scratch_shapes=scratch,
        ),
        input_output_aliases={k + skip: v for k, v in (aliases or {}).items()},
        compiler_params=pltpu.CompilerParams(dimension_semantics=("arbitrary",) * len(grid)),
        cost_estimate=pl.CostEstimate(flops=1, bytes_accessed=1, transcendentals=0),
    )(scalars, *waits, *args)


def project(low, weights, np_):
    width = low.shape[1] // np_
    acc = None
    for i in range(np_):
        one = dot(low[:, i * width : (i + 1) * width], weights[i][...])
        acc = one if acc is None else acc + one
    return acc


def turn(acc, count, size, g, c, s, out):
    for h in range(count):
        u = acc[:, h * size : (h + 1) * size]
        u = u * inv_scale(u) * g
        out[:, h * size : (h + 1) * size] = (u * c + pltpu.roll(u, size // 2, 1) * s).astype(bf16)


def kv_kernel(kv_heads, size, np_, passed, ids, tok, gain, cos, sin, kg, *rest):
    weights, (normed, kv_out, pre_out) = rest[:np_], rest[np_ + passed : np_ + passed + 3]
    x = ordered(tok, ids[0], np_).astype(f32)
    low = (x * inv_scale(x) * gain[...]).astype(bf16)
    normed[...] = low
    acc = project(low, weights, np_)
    pre_out[...] = acc[:, : kv_heads * size]
    turn(acc, kv_heads, size, kg[...], cos[...], sin[...], kv_out)
    kv_out[:, kv_heads * size :] = acc[:, kv_heads * size :].astype(bf16)


def query_kernel(heads, size, np_, ids, normed, cos, sin, qg, *rest):
    weights, (q_out, pre_out) = rest[:np_], rest[np_:]
    acc = project(normed[...], weights, np_)
    pre_out[...] = acc
    turn(acc, heads, size, qg[...], cos[...], sin[...], q_out)


def allowed_block(key_base, start, row_base, block, rows):
    key_index = key_base + lax.broadcasted_iota(jnp.int32, (block, rows), 0)
    row_index = row_base + lax.broadcasted_iota(jnp.int32, (block, rows), 1)
    return (key_index >= start) & (key_index <= row_index)


def attend_blocks(cfg, low, high, base, kv, q, start_row, row_base, acc, total):
    heads, kv_heads, size, block, scale2 = cfg
    group = heads // kv_heads
    rows = q.shape[0]

    def step(kb, carry):
        at = pl.ds(pl.multiple_of((kb - base) * block, block), block)
        allow = allowed_block(kb * block, start_row, row_base, block, rows)
        for g in range(kv_heads):
            k = kv[at, g * size : (g + 1) * size]
            v = kv[at, (kv_heads + g) * size : (kv_heads + g + 1) * size]
            for h in range(g * group, (g + 1) * group):
                s = dot(k, q[:, h * size : (h + 1) * size], NT)
                e = jnp.where(allow, jnp.exp2(s * scale2), 0.0)
                total[h : h + 1, :] += jnp.sum(e, 0, keepdims=True)
                acc[h * size : (h + 1) * size, :] += dot(v, e.astype(bf16), TN)
        return carry

    lax.fori_loop(low, high, step, 0)


def attend_own_kernel(cfg, back, ids, q, start, kv, acc, total):
    t = pl.program_id(0)
    rows = q.shape[0]
    base = back * kv.shape[0]
    acc[...] = jnp.zeros_like(acc)
    total[...] = jnp.zeros_like(total)
    first = base // cfg[3]
    attend_blocks(
        cfg, jnp.maximum(ids[2 + t], first), (base + (t + 1) * rows) // cfg[3], first,
        kv, q, start[...], base + t * rows, acc, total,
    )


def attend_kernel(cfg, np_, back, out_at, ids, q, start, acc_in, total_in, *rest):
    heads, _, size, block, _ = cfg
    chunks = rest[:back]
    w_out = rest[back : back + np_]
    own, oth, mixed_out, lse_out, kv, acc, total = rest[back + np_ :]
    t = pl.program_id(0)
    core = ids[1]
    rows = q.shape[0]
    length = chunks[0].shape[0]

    @pl.when(t == 0)
    def _():
        for i in range(back):
            kv[i * length : (i + 1) * length, :] = chunks[i][...]

    acc[...] = acc_in[...]
    total[...] = total_in[...]
    attend_blocks(
        cfg, ids[2 + t], back * length // block, 0, kv, q, start[...], back * length + t * rows, acc, total
    )
    sums = total[...]
    sums = jnp.where(sums > 0.0, sums, 1.0)
    lse_out[...] = jnp.log2(sums)
    inverse = 1.0 / sums
    for h in range(heads):
        part = (acc[h * size : (h + 1) * size, :] * inverse[h : h + 1, :]).astype(bf16)
        mixed_out[h * size : (h + 1) * size, :] = part
    mixed = mixed_out[...]
    width = w_out[0].shape[1]
    for i in range(np_):
        part = dot(mixed, w_out[i][out_at:, :], TN).astype(bf16)

        @pl.when(t == core)
        def _():
            own[:, i * width : (i + 1) * width] = part

        @pl.when(t != core)
        def _():
            oth[:, i * width : (i + 1) * width] = part


def ffn_kernel(np_, ids, tok, b_own, b_oth, valid, gain, grad, *rest):
    gate_w, up_w, down_w = rest[:np_], rest[np_ : 2 * np_], rest[2 * np_ : 3 * np_]
    n2_out, act_out, gg_out, gu_out, own, oth, gain_out, hat, acc = rest[3 * np_ :]
    f = pl.program_id(0)
    core = ids[1]
    half = b_own.shape[0]

    @pl.when(f == 0)
    def _():
        for ref, tile in ((b_own, core), (b_oth, 1 - core)):
            at = rows_of(tile, half)
            tokens = ordered(tok.at[at], ids[0], np_).astype(f32)
            resid = tokens + valid[at, :1] * ref[...].astype(f32)
            normal = resid * inv_scale(resid)
            hat[at, :] = normal
            n2_out[at, :] = (normal * gain[...]).astype(bf16)
        acc[...] = jnp.zeros_like(acc)

    width = tok.shape[1] // np_
    parts = [(i * width, (i + 1) * width) for i in range(np_)]
    gate = up = active_grad = None
    for i, (a, b) in enumerate(parts):
        x = n2_out[:, a:b]
        g, u, d = dot(x, gate_w[i][...]), dot(x, up_w[i][...]), dot(grad[:, a:b], down_w[i][...], NT)
        gate, up, active_grad = (g, u, d) if i == 0 else (gate + g, up + u, active_grad + d)
    sigma = jax.nn.sigmoid(gate)
    silu = gate * sigma
    act_out[...] = (silu * up).astype(bf16)
    gg = (active_grad * up * sigma * (1.0 + gate * (1.0 - sigma))).astype(bf16)
    gu = (active_grad * silu).astype(bf16)
    gg_out[...] = gg
    gu_out[...] = gu
    for i, (a, b) in enumerate(parts):
        acc[:, a:b] += dot(gg, gate_w[i][...], NT) + dot(gu, up_w[i][...], NT)

    @pl.when(f == pl.num_programs(0) - 1)
    def _():
        own[...] = acc[rows_of(core, half), :].astype(bf16)
        oth[...] = acc[rows_of(1 - core, half), :].astype(bf16)
        gain_out[...] = jnp.sum(acc[...] * hat[...], 0, keepdims=True)


def down_kernel(np_, ids, act, *rest):
    weights, (own, oth) = rest[:np_], rest[-2:]
    t = pl.program_id(0)
    width = weights[0].shape[1]
    for i in range(np_):
        part = dot(act[...], weights[i][...]).astype(bf16)

        @pl.when(t == ids[1])
        def _():
            own[:, i * width : (i + 1) * width] = part

        @pl.when(t != ids[1])
        def _():
            oth[:, i * width : (i + 1) * width] = part


def picked(ids, own, oth, t):
    return jnp.where(ids[1] == t, own[...].astype(f32), oth[...].astype(f32))


def attend_back_kernel(cfg, out_at, ids, tok, b_own, b_oth, t_own, t_oth, valid, gain, grad, mixed, lse, q, start, pre, cos, sin, qg, *rest):
    heads, kv_heads, size, np_, back, block, scale2 = cfg
    chunks = rest[: back + 1]
    w_out = rest[back + 1 : back + 1 + np_]
    outs = rest[back + 1 + np_ :]
    resid_out, branch_out, gq_out, gain_out = outs[:4]
    far = outs[4 : 4 + back + 1]
    kv, dkv, dq, dout = outs[4 + back + 1 :]
    t = pl.program_id(0)
    rows = q.shape[0]
    length = chunks[0].shape[0]
    group = heads // kv_heads
    scale = size**-0.5

    @pl.when(t == 0)
    def _():
        for i in range(back + 1):
            kv[i * length : (i + 1) * length, :] = chunks[i][...]
        dkv[...] = jnp.zeros_like(dkv)
        gain_out[...] = jnp.zeros_like(gain_out)

    resid = ordered(tok, ids[0], np_).astype(f32) + valid[:, :1] * picked(ids, b_own, b_oth, t)
    resid_grad = ordered(grad, ids[0], np_).astype(f32) + norm_back(
        resid, inv_scale(resid), gain[...], picked(ids, t_own, t_oth, t)
    )
    resid_out[...] = resid_grad
    low = (valid[:, :1] * resid_grad).astype(bf16)
    branch_out[...] = low
    width = low.shape[1] // np_
    mixed_grad = dot(w_out[0][out_at:, :], low[:, :width], NT)
    for i in range(1, np_):
        mixed_grad = mixed_grad + dot(w_out[i][out_at:, :], low[:, i * width : (i + 1) * width], NT)
    dout[...] = mixed_grad.astype(bf16)
    delta = [
        jnp.sum(
            dout[h * size : (h + 1) * size, :].astype(f32) * mixed[h * size : (h + 1) * size, :].astype(f32),
            0,
            keepdims=True,
        )
        for h in range(heads)
    ]
    dq[...] = jnp.zeros_like(dq)
    row_base = back * length + t * rows
    start_row = start[...]

    def step(kb, carry):
        at = pl.ds(pl.multiple_of(kb * block, block), block)
        allow = allowed_block(kb * block, start_row, row_base, block, rows)
        for g in range(kv_heads):
            k = kv[at, g * size : (g + 1) * size]
            v = kv[at, (kv_heads + g) * size : (kv_heads + g + 1) * size]
            dk = dv = None
            for h in range(g * group, (g + 1) * group):
                qh = q[:, h * size : (h + 1) * size]
                do = dout[h * size : (h + 1) * size, :]
                s = dot(k, qh, NT)
                p = jnp.where(allow, jnp.exp2(s * scale2 - lse[h : h + 1, :]), 0.0)
                dp = dot(v, do)
                ds = (p * (dp - delta[h])).astype(bf16)
                one_v = dot(p.astype(bf16), do, NT)
                one_k = dot(ds, qh)
                dk, dv = (one_k, one_v) if dk is None else (dk + one_k, dv + one_v)
                dq[h * size : (h + 1) * size, :] += dot(k, ds, TN)
            dkv[at, g * size : (g + 1) * size] += dk * scale
            dkv[at, (kv_heads + g) * size : (kv_heads + g + 1) * size] += dv
        return carry

    lax.fori_loop(ids[2 + t], (row_base + rows) // block, step, 0)
    c, s_ = cos[...], sin[...]
    for h in range(heads):
        u = dq[h * size : (h + 1) * size, :].T * scale
        u = u * c - pltpu.roll(u, size // 2, 1) * s_
        v = pre[:, h * size : (h + 1) * size]
        r = inv_scale(v)
        gain_out[...] += jnp.sum(u * (v * r), 0, keepdims=True)
        gq_out[:, h * size : (h + 1) * size] = norm_back(v, r, qg[...], u).astype(bf16)

    @pl.when(t == pl.num_programs(0) - 1)
    def _():
        for i in range(back + 1):
            far[i][...] = dkv[i * length : (i + 1) * length, :].astype(far[i].dtype)


def input_back_kernel(cfg, ids, tok, gain, gq, near, came, pre, cos, sin, kg, *rest):
    heads, kv_heads, size, np_ = cfg
    weights = rest[: 2 * np_]
    gkv_out, own, oth, k_gain, a_gain = rest[-5:]
    t = pl.program_id(0)
    core = ids[1]

    @pl.when(t == 0)
    def _():
        k_gain[...] = jnp.zeros_like(k_gain)
        a_gain[...] = jnp.zeros_like(a_gain)

    dkv = near[...] + came[...].astype(f32)
    c, s_ = cos[...], sin[...]
    for h in range(kv_heads):
        u = dkv[:, h * size : (h + 1) * size]
        u = u * c - pltpu.roll(u, size // 2, 1) * s_
        v = pre[:, h * size : (h + 1) * size]
        r = inv_scale(v)
        k_gain[...] += jnp.sum(u * (v * r), 0, keepdims=True)
        gkv_out[:, h * size : (h + 1) * size] = norm_back(v, r, kg[...], u).astype(bf16)
    gkv_out[:, kv_heads * size :] = dkv[:, kv_heads * size :].astype(bf16)
    x = ordered(tok, ids[0], np_).astype(f32)
    normal = x * inv_scale(x)
    width = x.shape[1] // np_
    for i in range(np_):
        at = slice(i * width, (i + 1) * width)
        part = dot(gq[...], weights[i][...], NT)
        part = part + dot(gkv_out[...], weights[np_ + i][...], NT)
        a_gain[:, at] += jnp.sum(part * normal[:, at], 0, keepdims=True)
        low = part.astype(bf16)

        @pl.when(t == core)
        def _():
            own[:, at] = low

        @pl.when(t != core)
        def _():
            oth[:, at] = low


def place(out, values, fs, np_):
    width = values.shape[1] // np_
    if np_ == 1:
        out[...] = values
        return
    for i in range(2):
        at = pl.ds(pl.multiple_of((fs if i == 0 else 1 - fs) * width, 128), width)
        out[:, at] = values[:, i * width : (i + 1) * width]


def layer_kernel(np_, fine, ids, tok, b_own, b_oth, f_own, f_oth, valid, *rest):
    out = rest[-1]
    t = pl.program_id(0) // fine
    v = valid[:, :1]
    resid = ordered(tok, ids[0], np_).astype(f32) + v * picked(ids, b_own, b_oth, t)
    place(out, (resid + v * picked(ids, f_own, f_oth, t)).astype(bf16), ids[0], np_)


def input_kernel(np_, fine, ids, tok, resid_grad, g_own, g_oth, gain, *rest):
    out = rest[-1]
    t = pl.program_id(0) // fine
    x = ordered(tok, ids[0], np_).astype(f32)
    grad = resid_grad[...] + norm_back(x, inv_scale(x), gain[...], picked(ids, g_own, g_oth, t))
    place(out, grad, ids[0], np_)


def product_kernel(pairs, groups, tiles, split, left_t, tail, ids, *rest):
    count = 1 if split is None else 2
    outs = rest[-count:]
    m = pl.program_id(0)

    def low():
        columns = []
        for j in range(groups):
            total = None
            for i in range(pairs):
                one = dot(rest[i][...], rest[pairs * (1 + j) + i][...], NN if left_t else TN)
                total = one if total is None else total + one
            columns.append(total.astype(bf16))
        return columns[0] if groups == 1 else jnp.concatenate(columns, 1)

    if split is None:
        outs[0][...] = low()
    elif split == 1:
        value = low()
        width = value.shape[1] // 2
        outs[0][...] = value[:, :width]
        outs[1][...] = value[:, width:]
    else:

        @pl.when(m < tiles // 2)
        def _():
            outs[0][...] = low()

        @pl.when((m >= tiles // 2) & (m < tiles))
        def _():
            outs[1][...] = low()

    if tail:

        @pl.when(m == tiles)
        def _():
            at = pairs * (1 + groups)
            for i in range(2):
                outs[i][: rest[at + i].shape[0], :] = rest[at + i][...]


def product(name, ids, lefts, rights, split, tile, left_t=False, at=0, height=None, into=None, tail=None, waits=()):
    pairs, groups = len(lefts), len(rights)
    m = lefts[0].shape[0 if left_t else 1]
    k = lefts[0].shape[1 if left_t else 0]
    n = sum(r[0].shape[1] for r in rights)
    tiles = m // tile
    ins, args = [], []
    for left in lefts:
        if left_t:
            ins.append(pl.BlockSpec((tile, k), lambda i, *_: (jnp.minimum(i, tiles - 1), 0)))
        else:
            ins.append(pl.BlockSpec((k, tile), lambda i, *_: (0, jnp.minimum(i, tiles - 1))))
        args.append(left)
    for group in rights:
        for right in group:
            ins.append(whole(right.shape))
            args.append(right)
    if split is None:
        shape = jax.ShapeDtypeStruct((height or m, n), bf16)
        outs = [(shape, pl.BlockSpec((tile, n), lambda i, *_: (i + at, 0)))]
    elif split == 1:
        shape = jax.ShapeDtypeStruct((height or m, n // 2), bf16)
        outs = [(shape, pl.BlockSpec((tile, n // 2), lambda i, *_: (i + at, 0)))] * 2
    else:
        half = tiles // 2
        shape = jax.ShapeDtypeStruct((height or m // 2, n), bf16)
        last = at + half if tail is not None else at + half - 1

        def own(i, *_):
            return (jnp.where(i < half, i + at, jnp.where(i < tiles, half - 1 + at, last)), 0)

        def other(i, *_):
            return (jnp.where(i < tiles, jnp.maximum(i - half, 0) + at, last), 0)

        outs = [(shape, pl.BlockSpec((tile, n), own)), (shape, pl.BlockSpec((tile, n), other))]
    if tail is not None:
        ins += [whole(v.shape) for v in tail]
        args += list(tail)
    aliases = None
    if into is not None:
        aliases = {1 + len(ins) + i: i for i in range(len(into))}
        ins += [pl.BlockSpec(memory_space=pl.ANY)] * len(into)
        args += list(into)
    return call(
        functools.partial(product_kernel, pairs, groups, tiles, split, left_t, tail is not None),
        name, (tiles + (tail is not None),), ins, outs, [], ids, *args, aliases=aliases, waits=waits,
    )


def swap(values, axis, bit, size):
    return lax.ppermute(values, axis, [(i, i ^ bit) for i in range(size)])


def plus(a, b):
    return a + b


class Line:
    def __init__(self):
        self.last = None
        self.waited = ()

    def __call__(self, fn, *args):
        if self.last is not None:
            args, _ = lax.optimization_barrier((args, self.last))
        outs = fn(*args)
        self.last = jax.tree.leaves(outs)[0]
        return outs

    def wait(self, *values):
        self.waited += values

    def take(self):
        values, self.waited = self.waited, ()
        return values

    def after(self, value):
        return lax.optimization_barrier((value, self.last, self.waited))[0]


class Steps:
    def __init__(self, steps):
        self.steps, self.value = steps, None

    def __call__(self, count=1):
        for _ in range(count):
            self.value = next(self.steps)
        return self.value


def sum_tp(line, own, oth, size):
    total = line(plus, own, swap(line.after(oth), "tp", 1, size))
    yield total
    bit = 2
    while bit < size:
        total = line(plus, total, swap(total, "tp", bit, size))
        bit *= 2
        if bit < size:
            yield total
    yield total, swap(total, "tp", 1, size)


def sum_line(line, total, axis, size):
    index = lax.axis_index(axis)
    middle = size // 2
    for i in range(middle - 1):
        came = lax.ppermute(total, axis, [(i, i + 1), (size - 1 - i, size - 2 - i)])
        total = line(plus, total, came)
        yield total
    total = line(plus, total, lax.ppermute(total, axis, [(middle - 1, middle), (middle, middle - 1)]))
    yield total
    came, outer = total, index < 0
    for i in reversed(range(middle - 1)):
        total = jnp.where(outer, came, total)
        came = lax.ppermute(total, axis, [(i + 1, i), (size - 2 - i, size - 1 - i)])
        outer = (index == i) | (index == size - 1 - i)
    yield came, total, outer


def sum_small(values, axis, size):
    bit = 1
    while bit < size:
        values = values + swap(values, axis, bit, size)
        bit *= 2
    return values


def body(
    n_fs, n_ctx, n_tp,
    tokens, segment_ids, attn_gain, w_query, w_key, w_value, query_gain, key_gain,
    w_out, ffn_gain, w_gate, w_up, w_down, out_grad,
):
    seqs, length, model = tokens.shape
    paired = n_fs == 2
    np_ = 2 if paired else 1
    fs = lax.axis_index("fsdp")
    ctx = lax.axis_index("ctx")
    core = lax.axis_index("tp") % 2
    size = query_gain.shape[0] * n_fs
    heads = w_query.shape[1] // size
    kv_heads = w_key.shape[1] // size
    hidden = w_gate.shape[1]
    q_width, kv_width = heads * size, kv_heads * size
    rows = length // 2
    block = rows
    back = min(n_ctx - 1, -(-(longest_segment - 1) // length))
    scale2 = size**-0.5 * math.log2(math.e)

    def gather(weight, axis):
        if paired:
            return [weight, swap(weight, "fsdp", 1, 2)]
        return [lax.all_gather(weight, "fsdp", axis=axis, tiled=True)]

    kv_w = gather(jnp.concatenate([w_key, w_value], 1), 0)
    query_w = gather(w_query, 0)
    gate_w = gather(w_gate, 0)
    up_w = gather(w_up, 0)
    down_out = [jnp.concatenate([w_down, w_out], 0)] if paired else []
    out_at = hidden if paired else 0

    part, small = attn_gain.shape[0], query_gain.shape[0]
    padding = part - 2 * small
    gains = jnp.concatenate([query_gain, key_gain] + ([jnp.zeros((padding,), bf16)] if padding > 0 else []))
    gains = jnp.stack([attn_gain, ffn_gain, gains[:part]]) if padding >= 0 else None
    if paired:
        gains, kv_w[0] = lax.optimization_barrier((gains, kv_w[0]))
    both = [gains, swap(gains, "fsdp", 1, 2)] if paired else None
    if paired:
        wide = jnp.concatenate(both, 1).astype(f32)
        gain_one, gain_two = wide[:1], wide[1:2]

    def natural(first, values):
        if not paired:
            return lax.all_gather(values, "fsdp", axis=0, tiled=True)[None, :].astype(f32)
        own_first = jnp.concatenate([b[2:, first : first + small] for b in both], 1)
        return jnp.where(fs == 0, own_first, jnp.roll(own_first, small, 1)).astype(f32)

    if not paired:
        gain_one, gain_two = natural(0, attn_gain), natural(0, ffn_gain)
    qg, kg = natural(0, query_gain), natural(small, key_gain)

    def reorder(values):
        if not paired:
            return values
        half = model // 2
        return jnp.where(fs == 0, values, jnp.concatenate([values[..., half:], values[..., :half]], -1))

    index = ctx * length + jnp.arange(length, dtype=jnp.int32)
    row_seg = lax.dynamic_slice_in_dim(segment_ids, ctx * length, length, 1)
    first = jnp.sum((segment_ids[:, None, :] < row_seg[:, :, None]).astype(jnp.int32), -1)
    position = index[None, :] - first
    live = row_seg != 0
    valid = jnp.broadcast_to(live.astype(f32)[:, :, None], (seqs, length, 128))
    window = (back + 1) * length
    start = jnp.where(live, jnp.maximum(first - (ctx - back) * length, 0), window + 1)
    lowest = jnp.min(start.reshape(seqs, 2, rows), -1) // block
    frequency = rope_base ** (-(jnp.arange(size // 2, dtype=f32) * 2.0 / size))
    turned = position.astype(f32)[:, :, None] * frequency
    cosine, sine = jnp.cos(turned), jnp.sin(turned)
    cos = jnp.concatenate([cosine, cosine], -1)
    sin = jnp.concatenate([-sine, sine], -1)
    low_grad = jnp.where(live[:, :, None], reorder(out_grad), jnp.zeros((), bf16))
    start = start[:, None, :]

    def scalars(s):
        return jnp.concatenate([jnp.stack([fs, core]).astype(jnp.int32), lowest[s]])

    ids = [scalars(s) for s in range(seqs)]
    cfg = (heads, kv_heads, size, np_, back, block, scale2)
    cfg_forward = (heads, kv_heads, size, block, scale2)

    def tiled(width):
        return pl.BlockSpec((rows, width), lambda i, *_: (i, 0))

    def tiled_t(height):
        return pl.BlockSpec((height, rows), lambda i, *_: (0, i))

    def of(s, width, tile=rows):
        return pl.BlockSpec((None, tile, width), lambda i, *_: (s, i, 0))

    def all_of(s, width):
        return pl.BlockSpec((None, length, width), lambda *_: (s, 0, 0))

    def lanes(s):
        return pl.BlockSpec((None, 1, rows), lambda i, *_: (s, 0, i))

    def shape(*dims, dtype=bf16):
        return jax.ShapeDtypeStruct(dims, dtype)

    half_pair = [(shape(rows, model), whole((rows, model)))] * 2

    line = Line()
    up_perm = [(i, i + 1) for i in range(n_ctx - 1)]
    down_perm = [(i + 1, i) for i in range(n_ctx - 1)]
    kv_shape = (length, 2 * kv_width)
    sums = 8 * -(-heads // 8)

    def kernel(name, body_, grid, ins, outs, scratch, s, *args, aliases=None):
        count = len(args)

        def run(*all_args):
            return call(
                body_, name, grid, ins, outs, scratch, ids[s], *all_args[:count],
                aliases=aliases, waits=all_args[count:],
            )

        return line(run, *args, *line.take())

    normed, own_kv, pre_k, queries, pre_q = [], [], [], [], []

    def keys(s, through=()):
        first = 6 + len(kv_w)
        n, k, p, *through = kernel(
            "keys", functools.partial(kv_kernel, kv_heads, size, np_, len(through)), (2,),
            [of(s, model), whole((1, model)), of(s, size), of(s, size), whole((1, size))]
            + [whole(w.shape) for w in kv_w] + [pl.BlockSpec(memory_space=pl.ANY)] * len(through),
            [
                (shape(length, model), tiled(model)),
                (shape(*kv_shape), tiled(2 * kv_width)),
                (shape(length, kv_width, dtype=f32), tiled(kv_width)),
            ]
            + [(shape(*v.shape), pl.BlockSpec(memory_space=pl.ANY)) for v in through],
            [], s, tokens, gain_one, cos, sin, kg, *kv_w, *through,
            aliases={first + i: 3 + i for i in range(len(through))},
        )
        normed.append(n)
        own_kv.append(k)
        pre_k.append(p)
        return through

    def query(s):
        q, p = kernel(
            "query", functools.partial(query_kernel, heads, size, np_), (2,),
            [tiled(model), of(s, size), of(s, size), whole((1, size))] + [whole(w.shape) for w in query_w],
            [
                (shape(length, q_width), tiled(q_width)),
                (shape(length, q_width, dtype=f32), tiled(q_width)),
            ],
            [], s, normed[s], cos, sin, qg, *query_w,
        )
        queries.append(q)
        pre_q.append(p)

    kv = []

    def spread(s):
        chunks = [line.after(own_kv[s])]
        chunks.insert(0, lax.ppermute(chunks[0], "ctx", up_perm))
        kv.append(chunks)

    def forward(s):
        for _ in range(back - 1):
            kv[s].insert(0, lax.ppermute(line.after(kv[s][0]), "ctx", up_perm))

    sums_own, mixed, lse, branch = [], [], [], []

    def attend_own(s):
        sums_own.append(
            kernel(
                "attend_own", functools.partial(attend_own_kernel, cfg_forward, back), (2,),
                [tiled(q_width), lanes(s), whole(kv_shape)],
                [
                    (shape(q_width, length, dtype=f32), tiled_t(q_width)),
                    (shape(sums, length, dtype=f32), tiled_t(sums)),
                ],
                [], s, queries[s], start, own_kv[s],
            )
        )

    def attend(s):
        own, oth, m, l = kernel(
            "attend", functools.partial(attend_kernel, cfg_forward, np_, back, out_at), (2,),
            [tiled(q_width), lanes(s), tiled_t(q_width), tiled_t(sums)]
            + [whole(kv_shape)] * back + [whole(w.shape) for w in out_w],
            half_pair
            + [
                (shape(q_width, length), tiled_t(q_width)),
                (shape(sums, length, dtype=f32), tiled_t(sums)),
            ],
            [
                pltpu.VMEM((back * length, 2 * kv_width), bf16),
                pltpu.VMEM((q_width, rows), f32),
                pltpu.VMEM((sums, rows), f32),
            ],
            s, queries[s], start, *sums_own[s], *kv[s][:back], *out_w,
        )
        mixed.append(m)
        lse.append(l)
        branch.append(Steps(sum_tp(line, own, oth, n_tp)))

    tile = 256
    steps = hidden // tile
    normed_two, active, grad_gate, grad_up, grad_two, ffn_gains = [], [], [], [], [], []

    def ffn(s):
        col = pl.BlockSpec((length, tile), lambda i, *_: (0, i))
        w_in = [pl.BlockSpec((w.shape[0], tile), lambda i, *_: (0, i)) for w in gate_w]
        w_dn = [pl.BlockSpec((tile, w.shape[1]), lambda i, *_: (i, 0)) for w in down_w]
        n2, act, gg, gu, own, oth, fg = kernel(
            "ffn", functools.partial(ffn_kernel, np_), (steps,),
            [all_of(s, model), whole((rows, model)), whole((rows, model)), all_of(s, 128),
             whole((1, model)), all_of(s, model)] + w_in + w_in + w_dn,
            [
                (shape(length, model), whole((length, model))),
                (shape(length, hidden), col),
                (shape(length, hidden), col),
                (shape(length, hidden), col),
            ]
            + half_pair
            + [(shape(1, model, dtype=f32), whole((1, model)))],
            [pltpu.VMEM((length, model), f32), pltpu.VMEM((length, model), f32)],
            s, tokens, *branch[s].value, valid, gain_two, low_grad, *gate_w, *up_w, *down_w,
        )
        normed_two.append(n2)
        active.append(act)
        grad_gate.append(gg)
        grad_up.append(gu)
        grad_two.append(Steps(sum_tp(line, own, oth, n_tp)))
        ffn_gains.append(fg)

    both_pair = [
        (shape(seqs * rows, model), lambda s: pl.BlockSpec((rows, model), lambda *_: (s, 0))),
    ] * 2

    def pair_of(s):
        return [(one, spec(s)) for one, spec in both_pair]

    layers = []

    def down(s):
        first = 2 + len(down_w)
        into = list(layers)
        layers[:] = kernel(
            "down", functools.partial(down_kernel, np_), (2,),
            [tiled(hidden)] + [whole((hidden, w.shape[1])) for w in down_w] + [pl.BlockSpec(memory_space=pl.ANY)] * len(into),
            pair_of(s), [], s, active[s], *down_w, *into,
            aliases={first: 0, first + 1: 1} if into else None,
        )
        if s == seqs - 1:
            layers[:] = [Steps(sum_tp(line, *layers, n_tp))]

    fine = 1
    small_rows = rows // fine

    def halves(s):
        return [pl.BlockSpec((small_rows, model), lambda i, *_: (s * fine + i % fine, 0))] * 2

    finished = {}

    def output(name, body_, s, ins, dtype, *args):
        extra = [finished[name]] if name in finished else []
        finished[name] = kernel(
            name, functools.partial(body_, np_, fine), (2 * fine,),
            [of(s, model, small_rows)] + ins + [pl.BlockSpec(memory_space=pl.ANY)] * len(extra),
            [(shape(seqs, length, model, dtype=dtype), of(s, model, small_rows))],
            [], s, tokens, *args, *extra,
            aliases={2 + len(ins): 0} if extra else None,
        )[0]

    def layer_output(s):
        output(
            "layer_out", layer_kernel, s, halves(0) + halves(s) + [of(s, 128, small_rows)], bf16,
            *branch[s].value, *layers[0].value, valid,
        )

    resid_grad, grad_branch, grad_query, near, q_gains, came = [], [], [], [], [], []

    def bring(far):
        moving = None
        for one in far:
            one = line.after(one) if moving is None else line(plus, one, moving)
            moving = lax.ppermute(one, "ctx", down_perm)
            yield moving

    def attend_back(s):
        far_shapes = [(shape(*kv_shape), whole(kv_shape))] * back
        rg, gb, gq, qgain, *far, dkv = kernel(
            "attend_back", functools.partial(attend_back_kernel, cfg, out_at), (2,),
            [of(s, model)] + [whole((rows, model))] * 4 + [of(s, 128), whole((1, model)), of(s, model),
             tiled_t(q_width), tiled_t(sums), tiled(q_width), lanes(s),
             tiled(q_width), of(s, size), of(s, size), whole((1, size))]
            + [whole(kv_shape)] * (back + 1)
            + [whole(w.shape) for w in out_w],
            [
                (shape(length, model, dtype=f32), tiled(model)),
                (shape(length, model), tiled(model)),
                (shape(length, q_width), tiled(q_width)),
                (shape(1, size, dtype=f32), whole((1, size))),
            ]
            + far_shapes
            + [(shape(*kv_shape, dtype=f32), whole(kv_shape))],
            [
                pltpu.VMEM((window, 2 * kv_width), bf16),
                pltpu.VMEM((window, 2 * kv_width), f32),
                pltpu.VMEM((q_width, rows), f32),
                pltpu.VMEM((q_width, rows), bf16),
            ],
            s, tokens, *branch[s].value, *grad_two[s].value, valid, gain_two, out_grad, mixed[s], lse[s], queries[s],
            start, pre_q[s], cos, sin, qg, *kv[s], *out_w,
        )
        came.append(Steps(bring(far)))
        resid_grad.append(rg)
        grad_branch.append(gb)
        grad_query.append(gq)
        q_gains.append(qgain)
        near.append(dkv)

    grad_kv, k_gains, a_gains, grad_one = [], [], [], []
    qkv_w = query_w + kv_w

    def input_back(s):
        into = list(grad_one)
        first = 11 + len(qkv_w)
        gkv, own, oth, kgain, again = kernel(
            "input_back", functools.partial(input_back_kernel, (heads, kv_heads, size, np_)), (2,),
            [of(s, model), whole((1, model)), tiled(q_width), tiled(2 * kv_width), tiled(2 * kv_width),
             tiled(kv_width), of(s, size), of(s, size), whole((1, size))]
            + [whole(w.shape) for w in qkv_w] + [pl.BlockSpec(memory_space=pl.ANY)] * len(into),
            [(shape(*kv_shape), tiled(2 * kv_width))]
            + pair_of(s)
            + [(shape(1, size, dtype=f32), whole((1, size))), (shape(1, model, dtype=f32), whole((1, model)))],
            [], s, tokens, gain_one, grad_query[s], near[s], came[s].value, pre_k[s], cos, sin, kg, *qkv_w, *into,
            aliases={first - 1: 1, first: 2} if into else None,
        )
        grad_kv.append(gkv)
        k_gains.append(kgain)
        a_gains.append(again)
        grad_one[:] = [own, oth]
        if s == seqs - 1:
            grad_one[:] = [Steps(sum_tp(line, own, oth, n_tp))]

    def input_output(s):
        output(
            "input_grad", input_kernel, s, [pl.BlockSpec((small_rows, model), lambda i, *_: (i, 0))]
            + halves(s) + [whole((1, model))], f32,
            resid_grad[s], *grad_one[0].value, gain_one,
        )

    rows_split, cols_split = (0, 1) if paired else (None, None)

    def reduced(parts, axis):
        if paired:
            total = line(plus, parts[0], swap(parts[1], "fsdp", 1, 2))
        else:
            total = lax.psum_scatter(parts[0], "fsdp", scatter_dimension=axis, tiled=True)
        yield total
        yield from sum_line(line, total, "ctx", n_ctx)

    def weight(name, lefts, rights, split, left_t=False, **place_):
        def run(lefts, rights, place_):
            return product(name, ids[0], lefts, rights, split, 256, left_t, **place_)

        if not paired:
            place_ = {}
        numbers = {k: v for k, v in place_.items() if k in ("at", "height")}
        arrays = {k: v for k, v in place_.items() if k not in numbers and v is not None}
        arrays["waits"] = line.take()
        return line(lambda l, r, x: run(l, r, {**numbers, **x}), list(lefts), [list(r) for r in rights], arrays)

    gain_width = 2 * kv_width
    gain_rows = 16 * -(-(2 * part + 2 * small) // (16 * gain_width))

    def gain_sum():
        values = jnp.concatenate([sum(a_gains), sum(ffn_gains), sum(q_gains), sum(k_gains)], 1)
        bit = 1
        while bit < n_tp:
            values = line(jnp.add, values, swap(values, "tp", bit, n_tp))
            bit *= 2
            yield values
        yield values

    def gain_parts(values):
        def one(own):
            pieces = [values[:, (0 if own else part) :][:, :part], values[:, model + (0 if own else part) :][:, :part]]
            for at in (2 * model, 2 * model + size):
                low, high = values[:, at : at + small], values[:, at + small : at + size]
                pieces.append(jnp.where((fs == 0) == own, low, high))
            row = jnp.concatenate(pieces, 1)
            row = jnp.pad(row, ((0, 0), (0, gain_rows * gain_width - row.shape[1])))
            return row.reshape(gain_rows, gain_width).astype(bf16)

        return [one(True), one(False)]

    sums_of, parts_of = {}, {}

    def make(name):
        if name == "gate_up":
            parts_of[name] = weight("gate_up_grad", normed_two, [grad_gate, grad_up], rows_split)
        elif name == "down":
            parts_of[name] = weight(
                "down_grad", active, [[low_grad[s] for s in range(seqs)]], cols_split, height=hidden + q_width
            )
        elif name == "out":
            parts_of[name] = weight(
                "out_grad", mixed, [grad_branch], cols_split, True,
                at=hidden // 256, height=hidden + q_width, into=parts_of["down"],
            )
        elif name == "query":
            parts_of[name] = weight("query_grad", normed, [grad_query], rows_split)
        else:
            parts_of[name] = weight(
                "kv_grad", normed, [grad_kv], rows_split, height=model // 2 + gain_rows, tail=gain_parts(sums_of["gains"].value) if paired else None,
            )

    def send(*names):
        axis = 1 if names[0] in ("down", "out") else 0
        if paired:
            sums_of[names[0]] = Steps(reduced(parts_of[names[-1]], axis))
        else:
            steps = [reduced(parts_of[n], axis) for n in names]
            sums_of[names[0]] = Steps(zip(*steps))

    down_out = keys(0, down_out)
    if paired:
        down_w = out_w = gather(down_out[0], 1)
    else:
        down_w, out_w = gather(w_down, 1), gather(w_out, 1)
    line.wait(query_w[-1])
    spread(0)
    keys(1)
    spread(1)
    forward(0)
    query(0)
    query(1)
    attend_own(0)
    attend_own(1)
    forward(1)
    attend(0)
    line.wait(gate_w[-1])
    branch[0]()
    line.wait(low_grad, valid)
    attend(1)
    branch[0]()
    line.wait(up_w[-1])
    branch[1]()
    ffn(0)
    branch[1]()
    grad_two[0]()
    ffn(1)
    grad_two[0]()
    grad_two[1]()
    attend_back(0)
    came[0]()
    make("gate_up")
    send("gate_up")
    grad_two[1]()
    down(0)
    came[0]()
    attend_back(1)
    line.wait(came[0].value)
    came[1]()
    make("down")
    make("out")
    send("down", "out")
    make("query")
    send("query")
    came[1]()
    down(1)
    input_back(0)
    sums_of["gate_up"]()
    input_back(1)
    sums_of["down"]()
    sums_of["query"]()
    sums_of["gains"] = Steps(gain_sum())
    sums_of["gains"]()
    sums_of["gains"]()
    make("kv")
    send("kv")
    grad_one[0]()
    sums_of["gate_up"]()
    layers[0]()
    grad_one[0]()
    input_output(0)
    sums_of["down"]()
    sums_of["gate_up"]()
    sums_of["query"]()
    sums_of["kv"]()
    layers[0]()
    input_output(1)
    sums_of["down"]()
    sums_of["kv"]()
    layer_output(0)
    sums_of["query"]()
    sums_of["kv"]()
    half = model // 2

    def wide_type(value):
        return (value.astype(f32),)

    def columns_of(width):
        return lambda value: (value[:, :width].astype(f32), value[:, width:].astype(f32))

    def rows_at(height):
        return lambda value: (value[:height].astype(f32), value[height:].astype(f32))

    def keys_values(value):
        return columns_of(kv_width)(value[:half]) + (value[half:].astype(f32),)

    def finish(name, *after):
        steps_ = sums_of[name]()
        outs = []
        for (came_, total, outer), to in zip([steps_] if paired else steps_, after):
            outs += line(lambda c, v: to(jnp.where(outer, c, v)), came_, total)
        return outs

    if paired:
        gate_sum, up_sum = finish("gate_up", columns_of(hidden))
        layer_output(1)
        down_sum, out_sum = finish("down", rows_at(hidden))
        (query_sum,) = finish("query", wide_type)
        key_sum, value_sum, gain_total = finish("kv", keys_values)
    else:
        layer_output(1)
        gate_sum, up_sum = finish("gate_up", columns_of(hidden))
        down_sum, out_sum = finish("down", wide_type, wide_type)
        (query_sum,) = finish("query", wide_type)
        key_sum, value_sum = finish("kv", columns_of(kv_width))
    if paired:
        mine_all = gain_total.reshape(1, -1)[0]
        gain_out = []
        at = 0
        for width in (part, part, small, small):
            gain_out.append(mine_all[at : at + width])
            at += width
    else:
        values = sums_of["gains"].value
        for axis, count in (("fsdp", n_fs), ("ctx", n_ctx)):
            values = sum_small(values, axis, count)
        gain_out = []
        for at, width in ((0, model), (model, model), (2 * model, size), (2 * model + size, size)):
            gain_out.append(lax.dynamic_slice_in_dim(values[0], at + fs * (width // n_fs), width // n_fs, 0))
    attn_out, ffn_out, query_out, key_out = gain_out

    return (
        finished["layer_out"],
        finished["input_grad"],
        attn_out,
        query_sum,
        key_sum,
        value_sum,
        query_out,
        key_out,
        out_sum,
        ffn_out,
        gate_sum,
        up_sum,
        down_sum,
    )


def solution(mesh):
    n_fs, n_ctx, n_tp = mesh.shape["fsdp"], mesh.shape["ctx"], mesh.shape["tp"]
    placed = (
        P("fsdp", "ctx", None),
        P("fsdp", None),
        P("fsdp"),
        P("fsdp", "tp"),
        P("fsdp", "tp"),
        P("fsdp", "tp"),
        P("fsdp"),
        P("fsdp"),
        P("tp", "fsdp"),
        P("fsdp"),
        P("fsdp", "tp"),
        P("fsdp", "tp"),
        P("tp", "fsdp"),
        P("fsdp", "ctx", None),
    )
    return jax.shard_map(
        functools.partial(body, n_fs, n_ctx, n_tp),
        mesh=mesh,
        in_specs=placed,
        out_specs=(
            P("fsdp", "ctx", None),
            P("fsdp", "ctx", None),
            P("fsdp"),
            P("fsdp", "tp"),
            P("fsdp", "tp"),
            P("fsdp", "tp"),
            P("fsdp"),
            P("fsdp"),
            P("tp", "fsdp"),
            P("fsdp"),
            P("fsdp", "tp"),
            P("fsdp", "tp"),
            P("tp", "fsdp"),
        ),
        check_vma=False,
    )
```
